32 devices in a mesh: seq: 4 (over y, x), batch: 8 (over z, core).
Axes of the slice: x: 2, y: 2, z: 4, core: 2. Of those that a mesh axis runs over, the one named last changes fastest.
Arguments:
- attn_out: bfloat16 [16384, 2560], P(('seq', 'batch')), may hold values from -200 to 200
- out_grad: bfloat16 [16384, 2560], P(('seq', 'batch')), may hold values from -6 to 6
- master: float32 [2560, 2560], P(('seq', 'batch')), may hold values from -0.125 to 0.125
- moment_one: float32 [2560, 2560], P(('seq', 'batch')), may hold values from -4 to 4
- moment_two: float32 [2560, 2560], P(('seq', 'batch')), may hold values from 0.002 to 0.05
Outputs:
- input_grad: bfloat16 [16384, 2560], P(('seq', 'batch'))
- new_master: float32 [2560, 2560], P(('seq', 'batch'))
- new_moment_one: float32 [2560, 2560], P(('seq', 'batch'))
- new_moment_two: float32 [2560, 2560], P(('seq', 'batch'))
The draws below stay inside these ranges and needn't reach their ends.
All inputs are finite; a program needn't handle non-finite values.
Results may differ from the reference program's by a relative error of at most 0.01.
Values may be sent and summed in bfloat16 or wider, within the bound.
A program may use at most 128 MiB of HBM per device.

```python
import math
import jax
import jax.numpy as jnp
from jax import lax

DIN = 2560
DOUT = 2560
TOK_DEV = 512
STEP = 10
TOKENS = 16384


def draw_attn_out(key, part):
    blocks = TOKENS // TOK_DEV
    feature_width = DIN // blocks
    first_key, second_key = jax.random.split(jax.random.fold_in(key, 11), 2)
    ramp = jnp.arange(DIN, dtype=jnp.float32) / jnp.float32(DIN)
    values = jax.random.normal(first_key, (TOKENS, DIN), jnp.float32)
    column = 10.0 ** ramp
    pairing = jax.random.permutation(second_key, blocks)
    token_block = jnp.arange(TOKENS) // TOK_DEV
    feature_block = jnp.arange(DIN) // feature_width
    spike = jnp.where(pairing[token_block][:, None] == feature_block[None, :], 6.0, 1.0)
    result = jnp.clip(values * column[None, :] * spike, -200.0, 200.0)
    return result.astype(jnp.bfloat16)


def steps_of(rng, shape, pieces, least, largest):
    factor_of, own = 1.0, jax.random.fold_in(rng, 6)
    for dim, parts in pieces:
        heights = jnp.exp(jax.random.uniform(jax.random.fold_in(own, dim), (parts,), jnp.float32, least / len(pieces), largest / len(pieces)))
        factor_of = factor_of * jnp.repeat(heights, shape[dim] // parts).reshape([-1 if axis == dim else 1 for axis in range(len(shape))])
    return factor_of


def noise(stream_key, extent, spread, most, shards=(), kind=jnp.bfloat16):
    drawn = jax.random.normal(stream_key, extent, jnp.float32) * spread
    if len(shards) > 0:
        drawn = steps_of(stream_key, extent, shards, -0.22, 0.18) * drawn
    return jnp.clip(drawn, min=-most, max=most).astype(kind)


def setup_inputs(seed: int = 0) -> dict:
    key_list = jax.random.split(jax.random.key(seed), 6)
    attn_out = draw_attn_out(jax.random.fold_in(key_list[5], 71), 0)
    out_grad = noise(key_list[1], (TOKENS, DOUT), 1.0, 6.0, ((0, 32),))
    master = noise(key_list[2], (DIN, DOUT), DIN ** -0.5, 0.125, ((0, 32),), jnp.float32)
    moment_one = noise(key_list[3], (DIN, DOUT), 0.3, 4.0, ((0, 32),), jnp.float32)
    moment_two = jnp.clip(jnp.exp(math.log(0.05) - 3.218876 * jax.random.uniform(key_list[4], (DIN, DOUT), jnp.float32) ** steps_of(key_list[4], (DIN, DOUT), ((0, 32),), -0.2, 0.2)), 0.002, 0.05)
    return dict(attn_out=attn_out, out_grad=out_grad, master=master, moment_one=moment_one, moment_two=moment_two)


def reference(attn_out, out_grad, master, moment_one, moment_two):
    weight = master.astype(jnp.bfloat16)
    input_grad = lax.dot_general(out_grad, weight, (((1,), (1,)), ((), ())), preferred_element_type=jnp.float32).astype(jnp.bfloat16)
    weight_grad = lax.dot_general(attn_out, out_grad, (((0,), (0,)), ((), ())), preferred_element_type=jnp.float32)
    grad_norm = jnp.sqrt(jnp.sum(weight_grad * weight_grad)) + 1e-06
    limit = jnp.sqrt(jnp.float32(DIN * DOUT))
    clipped = weight_grad * jnp.minimum(jnp.float32(1.0), limit / grad_norm)
    new_one = 0.9 * moment_one + 0.1 * clipped
    new_two = 0.999 * moment_two + 0.001 * clipped * clipped
    first_hat = new_one / (1.0 - 0.9 ** STEP)
    second_hat = new_two / (1.0 - 0.999 ** STEP)
    new_master = master - 0.01 * (first_hat / (jnp.sqrt(second_hat) + 1e-08) + 0.1 * master)
    return (input_grad, new_master, new_one, new_two)
```

```python
import functools
import jax
import jax.numpy as jnp
from jax import lax
from jax.experimental import pallas as pl
from jax.experimental.pallas import tpu as pltpu
from jax.sharding import PartitionSpec as P

GRAD_BLOCKS = 4
STEP = 10
MESH = pl.DeviceIdType.MESH
F32 = jnp.float32
BF16 = jnp.bfloat16


def kernel(nb, attn_hbm, og_hbm, master_hbm, ig_hbm, gw_ref, sq_ref,
           attn_ref, og_ref, mst, rx_og, tbuf, tx, at_own, at_rx, wg, g, rx1, rzb, rx3, fbuf, ig, sqs,
           l_s, o_s, x_s, x_r, p_s, p_r, z_s, z_r, e_s, e_r, c_s, c_r, r_s, r_r, y_s, y_r, f_s, f_r, q_s, q_r):
    ns = 4
    nz = nb // 2
    tok, din = attn_ref.shape
    dout = og_ref.shape[1]
    r = gw_ref.shape[0]
    half = dout // 2
    block = nb * r
    seq = lax.axis_index("seq")
    batch = lax.axis_index("batch")
    z = batch // 2
    core = batch % 2
    hi = seq // 2
    lo = seq % 2
    sh = (1 - hi) * 2 + lo
    sl = hi * 2 + (1 - lo)
    sd = (1 - hi) * 2 + (1 - lo)
    first = (sl, sh)
    last = (sh, sl)
    cols = (pl.ds(0, half), pl.ds(half, half))
    core_dev = (seq, z * 2 + 1 - core)
    edge = jnp.logical_or(z == 0, z == nz - 1)

    def other(i):
        f = lax.rem(seq * nb + batch + i, ns * nb)
        return (f // nb, lax.rem(f, nb))

    lm = pltpu.make_async_copy(master_hbm, mst, l_s.at[2])
    lm.start()
    la = pltpu.make_async_copy(attn_hbm, attn_ref, l_s.at[0])
    la.start()
    lg = pltpu.make_async_copy(og_hbm, og_ref, l_s.at[1])
    lg.start()
    barrier = pltpu.get_barrier_semaphore()

    def greet(i, carry):
        pl.semaphore_signal(barrier, inc=1, device_id=other(i), device_id_type=MESH)
        return carry

    lax.fori_loop(1, ns * nb, greet, 0)

    near = jnp.minimum(z, nz - 1 - z)

    def zk(t):
        if t == 0:
            return z
        both = t <= 2 * near
        dist = jnp.where(both, (t + 1) // 2, t - near)
        above = jnp.where(both, t % 2, jnp.where(z < nz - 1 - z, 1, 0))
        return z + dist * (2 * above - 1)

    def wrows(s, zz):
        return pl.ds(pl.multiple_of((s * nb + zz * 2 + core) * r, 16), r)

    def grows(s, zz):
        return pl.ds(pl.multiple_of((zz * ns + s) * r, 16), r)

    def remote(s, d, ssem, rsem, dev):
        return pltpu.make_async_remote_copy(
            src_ref=s, dst_ref=d, send_sem=ssem, recv_sem=rsem,
            device_id=dev, device_id_type=MESH)

    def shard(s, zz, h):
        return wg.at[wrows(s, zz), cols[h]]

    def p_copy(h):
        v = shard(seq, z, h)
        return remote(v, v, p_s.at[h], p_r.at[h], (first[h], batch))

    def z_copy(h, i, t, up):
        zz = zk(t)
        to = jnp.minimum(z + 1, nz - 1) if up else jnp.maximum(z - 1, 0)
        v = shard((seq, first[h])[i], zz, h)
        k = (h * 2 + i) * nz + zz
        return remote(v, v, z_s.at[4 * nz * up + k], z_r.at[k], (seq, to * 2 + core))

    def z_each(h, i, t, act):
        zz = zk(t)
        for up in (0, 1):
            ok = jnp.logical_and(zz <= z, z < nz - 1) if up else jnp.logical_and(zz >= z, z > 0)

            @pl.when(ok)
            def _():
                act(z_copy(h, i, t, up))

    def e_copy(h, i, t):
        v = shard((seq, first[h])[i], zk(t), h)
        k = (h * 2 + i) * nz + t
        return remote(v, v, e_s.at[k], e_r.at[k], (last[h], batch))

    def c_copy(k, t):
        s, h = ((seq, None), (sl, 0), (sh, 1), (sh, 0), (sd, 0), (sl, 1), (sd, 1))[k]
        v = wg.at[wrows(s, zk(t))] if h is None else shard(s, zk(t), h)
        return remote(v, v, c_s.at[7 * t + k], c_r.at[7 * t + k], core_dev)

    def r_copy(h, i, j):
        k = (h * 2 + i) * nz + j
        v = g.at[grows((last[h], sd)[i], zk(nz - 1 - j)), cols[h]]
        return remote(v, rx1.at[k], r_s.at[k], r_r.at[k], (last[h], batch))

    def y_copy(h, i, j):
        t = zk(nz - 1 - j)
        up = t > z
        to = jnp.where(up, jnp.minimum(z + 1, nz - 1), jnp.maximum(z - 1, 0))
        k = (h * 2 + i) * (nz + 1) + jnp.where(jnp.logical_and(jnp.logical_not(up), t == z - 1), nz, t)
        v = g.at[grows((seq, first[h])[i], t), cols[h]]
        return remote(v, rzb.at[k], y_s.at[(h * 2 + i) * nz + j], y_r.at[k], (seq, to * 2 + core))

    def y_slot(h, i, t):
        k = (h * 2 + i) * (nz + 1) + t
        v = g.at[grows(seq, z), cols[h]]
        return remote(v, rzb.at[k], y_s.at[0], y_r.at[k], core_dev), rzb.at[k]

    def f_copy(h):
        v = g.at[grows(first[h], z), cols[h]]
        return remote(v, rx3.at[h], f_s.at[h], f_r.at[h], (first[h], batch))

    def az(t, h, i):
        z_copy(h, i, t, 0).wait_recv()
        z_each(h, i, t, lambda c: c.start())
        e_copy(h, i, t).start()
        if i == 1:
            c_copy(1 + h, t).start()
        elif h == 1:
            c_copy(0, t).start()

    def ae(t, h, i):
        e_copy(h, i, t).wait_recv()
        c_copy(3 + 2 * h + i, t).start()

    def rs(j):
        for i in (1, 0):
            for h in (0, 1):
                r_copy(h, i, j).start()

    def rr(j, h, i):
        k = (h * 2 + i) * nz + j
        t = zk(nz - 1 - j)
        rows = grows((seq, first[h])[i], t)
        r_copy(h, i, j).wait_recv()
        more = jnp.logical_or(jnp.logical_and(t > z, z > 0), jnp.logical_and(t < z, z < nz - 1))

        @pl.when(more)
        def _():
            c, buf = y_slot(h, i, t)
            c.wait_recv()
            g[rows, cols[h]] = (g[rows, cols[h]].astype(F32) + rx1[k].astype(F32) + buf[...].astype(F32)).astype(BF16)

        @pl.when(jnp.logical_not(more))
        def _():
            g[rows, cols[h]] = (g[rows, cols[h]].astype(F32) + rx1[k].astype(F32)).astype(BF16)
        y_copy(h, i, j).start()

    def rl(h, i):
        j = nz - 1
        k = (h * 2 + i) * nz + j
        rows = grows((seq, first[h])[i], z)
        dst = gw_ref.at[:, cols[h]] if i == 0 else fbuf.at[h]
        r_copy(h, i, j).wait_recv()
        dst[...] = g[rows, cols[h]].astype(F32) + rx1[k].astype(F32)
        for ok, t in ((z > 0, z), (z < nz - 1, nz)):
            @pl.when(ok)
            def _():
                c, buf = y_slot(h, i, t)
                c.wait_recv()
                dst[...] += buf[...].astype(F32)
        if i == 1:
            g[rows, cols[h]] = dst[...].astype(BF16)
            f_copy(h).start()

    tile = 256

    def grad(j):
        rows = pl.ds(pl.multiple_of(zk(nz - 1 - j) * (ns * r), 16), ns * r)

        def body(i, carry):
            c = pl.ds(pl.multiple_of(i * tile, tile), tile)
            acc = jnp.dot(at_own[rows, :], og_ref[:, c], preferred_element_type=F32)
            acc += jnp.dot(at_rx[rows, :], rx_og[:, c], preferred_element_type=F32)
            g[rows, c] = acc.astype(BF16)
            return carry
        lax.fori_loop(0, dout // tile, body, 0)

    def input_cols(q, s):
        def part(c):
            v = lax.dot_general(og_ref[...], wg[c, :], (((1,), (1,)), ((), ())), preferred_element_type=F32)
            ig[:, c] = v.astype(BF16)

        def body(i, carry):
            part(pl.ds(pl.multiple_of(s * block + i * tile, 128), tile))
            return carry
        lax.fori_loop(0, block // tile, body, 0)
        if block % tile:
            part(pl.ds(pl.multiple_of(s * block + block // tile * tile, 128), block % tile))
        o_copy(q, s).start()

    def o_copy(q, s):
        c = pl.ds(pl.multiple_of(s * block, 128), block)
        return pltpu.make_async_copy(ig.at[:, c], ig_hbm.at[:, c], o_s.at[q])

    xo = remote(og_hbm, rx_og, x_s.at[0], x_r.at[0], core_dev)
    xt = remote(tx, at_rx, x_s.at[1], x_r.at[1], core_dev)

    lm.wait()
    wg[wrows(seq, z), :] = mst[...].astype(BF16)
    pl.semaphore_wait(barrier, ns * nb - 1)
    for h in (0, 1):
        p_copy(h).start()
    for h in (0, 1):
        z_each(h, 0, 0, lambda c: c.start())
    for h in (1, 0):
        e_copy(h, 0, 0).start()
    xo.start()
    la.wait()
    for s in range(ns):
        tbuf[...] = attn_ref[:, s * block:(s + 1) * block].T
        for zz in range(nz):
            rows = pl.ds((zz * ns + s) * r, r)
            at_own[rows, :] = tbuf[pl.ds(pl.multiple_of((zz * 2 + core) * r, 16), r), :]
            tx[rows, :] = tbuf[pl.ds(pl.multiple_of((zz * 2 + 1 - core) * r, 16), r), :]
    xt.start()
    c_copy(0, 0).start()
    for h in (0, 1):
        p_copy(h).wait_recv()
        z_each(h, 1, 0, lambda c: c.start())
        e_copy(h, 1, 0).start()
        c_copy(1 + h, 0).start()
    lg.wait()
    xo.wait_recv()
    xt.wait_recv()

    def do(on_edge, inside):
        for ok, events in ((edge, on_edge), (jnp.logical_not(edge), inside)):
            if events:
                @pl.when(ok)
                def _():
                    for f, *a in events:
                        f(*a)

    hs = (0, 1)
    ih = [(h, i) for i in (1, 0) for h in hs]
    grad(0)
    rs(0)
    do([(az, 1, h, 0) for h in hs],
       [(az, t, h, 0) for h in hs for t in (1, 2)])
    grad(1)
    do([(az, 1, 0, 1)],
       [(az, t, 0, 1) for t in (1, 2)])
    grad(2)
    do([(az, 1, 1, 1), (rs, 1)],
       [(az, t, 1, 1) for t in (1, 2)] + [(rs, 1), (rs, 2)])
    do([(rr, 0, h, i) for h, i in ih[:2]], [])
    grad(3)
    do([(rr, 0, h, i) for h, i in ih[2:]]
       + [(az, 2, h, i) for i in hs for h in hs]
       + [(rs, 2)]
       + [(rr, 1, h, i) for h, i in ih]
       + [(ae, t, h, i) for t in (0, 1) for i in hs for h in hs]
       + [(az, 3, h, i) for i in hs for h in hs]
       + [(rs, 3)]
       + [(ae, 2, h, i) for i in hs for h in hs],
       [e for n, (h, i) in enumerate(ih) for e in ((az, 3, n % 2, n // 2), (rr, 0, h, i))]
       + [(rs, 3)]
       + [(ae, t, h, i) for t in (0, 1, 2) for i in hs for h in hs]
       + [(rr, j, h, i) for h, i in ih[:2] for j in (1, 2)])
    for t in range(nz):
        c_copy(0, t).wait_recv()
    do([], [(rr, j, h, i) for h, i in ih[2:] for j in (1, 2)])
    input_cols(0, seq)
    do([(rr, 2, h, i) for h, i in ih], [])
    for i in hs:
        for h in hs:
            ae(3, h, i)
    for k in range(1, 7):
        for t in range(nz):
            c_copy(k, t).wait_recv()
    input_cols(1, sl)
    input_cols(2, sh)
    rl(0, 1)
    rl(1, 1)
    input_cols(3, sd)
    rl(0, 0)
    rl(1, 0)
    for h in hs:
        f_copy(h).wait_recv()
        gw_ref[:, cols[h]] += rx3[h].astype(F32)

    v = gw_ref[...]
    part = jnp.sum((v * v).reshape(r // 8, 8, dout), axis=0)
    acc = part[:, :128]
    for i in range(1, dout // 128):
        acc += part[:, i * 128:(i + 1) * 128]
    sqs[0] = jnp.sum(acc, axis=0, keepdims=True)

    def q_copy(i):
        return remote(sqs.at[0], sqs.at[i], q_s.at[i], q_r.at[i], other(i))

    def q_start(i, carry):
        q_copy(i).start()
        return carry

    def q_wait(i, carry):
        q_copy(i).wait()
        return carry

    lax.fori_loop(1, ns * nb, q_start, 0)
    for h in hs:
        p_copy(h).wait_send()
        f_copy(h).wait_send()
        for i in hs:
            for t in range(nz):
                z_each(h, i, t, lambda c: c.wait_send())
                e_copy(h, i, t).wait_send()
                r_copy(h, i, t).wait_send()
                if t < nz - 1:
                    y_copy(h, i, t).wait_send()
    for t in range(nz):
        for k in range(7):
            c_copy(k, t).wait_send()
    xo.wait_send()
    xt.wait_send()
    for q, s in enumerate((seq, sl, sh, sd)):
        o_copy(q, s).wait()
    lax.fori_loop(1, ns * nb, q_wait, 0)
    total = sqs[0]
    for i in range(1, ns * nb):
        total += sqs[i]
    sq_ref[...] = total


def fused(attn_out, out_grad, master, ns, nb):
    tok, din = attn_out.shape
    dout = out_grad.shape[1]
    r = master.shape[0]
    half = dout // 2
    nz = nb // 2
    n = ns * nb
    dma = lambda k: pltpu.SemaphoreType.DMA((k,))
    vm = pl.BlockSpec(memory_space=pltpu.VMEM)
    hbm = pl.BlockSpec(memory_space=pl.ANY)
    sems = [3, 4, 2, 2, 2, 2, 8 * nz, 4 * nz, 4 * nz, 4 * nz, 7 * nz, 7 * nz,
            4 * nz, 4 * nz, 4 * nz, 4 * (nz + 1), 2, 2, n, n]
    return pl.pallas_call(
        functools.partial(kernel, nb),
        out_shape=(
            jax.ShapeDtypeStruct((tok, din), BF16),
            jax.ShapeDtypeStruct((r, dout), F32),
            jax.ShapeDtypeStruct((1, 128), F32),
        ),
        in_specs=[hbm] * 3,
        out_specs=(hbm, vm, vm),
        scratch_shapes=[
            pltpu.VMEM((tok, din), BF16),
            pltpu.VMEM((tok, dout), BF16),
            pltpu.VMEM((r, dout), F32),
            pltpu.VMEM((tok, dout), BF16),
            pltpu.VMEM((nb * r, tok), BF16),
            pltpu.VMEM((din // 2, tok), BF16),
            pltpu.VMEM((din // 2, tok), BF16),
            pltpu.VMEM((din // 2, tok), BF16),
            pltpu.VMEM((din, dout), BF16),
            pltpu.VMEM((din // 2, dout), BF16),
            pltpu.VMEM((4 * nz, r, half), BF16),
            pltpu.VMEM((4 * (nz + 1), r, half), BF16),
            pltpu.VMEM((2, r, half), BF16),
            pltpu.VMEM((2, r, half), F32),
            pltpu.VMEM((tok, din), BF16),
            pltpu.VMEM((n, 1, 128), F32),
        ] + [dma(k) for k in sems],
        compiler_params=pltpu.CompilerParams(
            collective_id=0, has_side_effects=True, vmem_limit_bytes=62_000_000),
    )(attn_out, out_grad, master)


def plain(attn_out, out_grad, shard_weight):
    projected = lax.dot_general(
        out_grad,
        lax.all_gather(shard_weight, ("seq", "batch"), axis=0, tiled=True),
        (((1,), (1,)), ((), ())),
        preferred_element_type=F32,
    )
    width = out_grad.shape[1] // GRAD_BLOCKS
    parts = []
    for b in range(GRAD_BLOCKS):
        d = lax.dot_general(
            attn_out, out_grad[:, b * width:(b + 1) * width],
            (((0,), (0,)), ((), ())), preferred_element_type=F32).astype(BF16)
        d = lax.psum_scatter(d, "seq", scatter_dimension=0, tiled=True)
        parts.append(lax.psum_scatter(d, "batch", scatter_dimension=0, tiled=True).astype(F32))
    weight_grad = jnp.concatenate(parts, axis=1)
    squares = lax.psum(jnp.sum(weight_grad * weight_grad), ("seq", "batch"))
    return projected.astype(BF16), weight_grad, squares


def on_device(ns, nb, attn_out, out_grad, master, moment_one, moment_two):
    r, dout = master.shape
    din = attn_out.shape[1]
    if ns == 4 and nb == 8 and r % 16 == 0 and (nb * r) % 128 == 0 and dout % 256 == 0:
        input_grad, weight_grad, sq = fused(attn_out, out_grad, master, ns, nb)
        squares = jnp.sum(sq)
    else:
        input_grad, weight_grad, squares = plain(attn_out, out_grad, master.astype(BF16))
    grad_norm = jnp.sqrt(squares) + 1e-06
    limit = jnp.sqrt(jnp.float32(din * dout))
    clipped = weight_grad * jnp.minimum(jnp.float32(1.0), limit / grad_norm)
    new_one = 0.9 * moment_one + 0.1 * clipped
    new_two = 0.999 * moment_two + 0.001 * clipped * clipped
    first_hat = new_one / (1.0 - 0.9**STEP)
    second_hat = new_two / (1.0 - 0.999**STEP)
    new_master = master - 0.01 * (first_hat / (jnp.sqrt(second_hat) + 1e-08) + 0.1 * master)
    return (input_grad, new_master, new_one, new_two)


def solution(mesh):
    spec = P(("seq", "batch"), None)
    return jax.shard_map(
        functools.partial(on_device, mesh.shape["seq"], mesh.shape["batch"]),
        mesh=mesh,
        in_specs=(spec,) * 5,
        out_specs=(spec,) * 4,
        check_vma=False,
    )
```

```python
import functools
import jax
import jax.numpy as jnp
from jax import lax
from jax.experimental import pallas as pl
from jax.experimental.pallas import tpu as pltpu
from jax.sharding import PartitionSpec as P

GRAD_BLOCKS = 4
STEP = 10
MESH = pl.DeviceIdType.MESH
F32 = jnp.float32
BF16 = jnp.bfloat16


def update(weight_grad, squares, master, moment_one, moment_two, size):
    grad_norm = jnp.sqrt(squares) + 1e-06
    limit = jnp.sqrt(jnp.float32(size))
    clipped = weight_grad * jnp.minimum(jnp.float32(1.0), limit / grad_norm)
    new_one = 0.9 * moment_one + 0.1 * clipped
    new_two = 0.999 * moment_two + 0.001 * clipped * clipped
    first_hat = new_one * (1.0 / (1.0 - 0.9**STEP))
    second_hat = new_two * (1.0 / (1.0 - 0.999**STEP))
    new_master = master - 0.01 * (first_hat / (jnp.sqrt(second_hat) + 1e-08) + 0.1 * master)
    return new_master, new_one, new_two


def kernel(nb, attn_hbm, og_hbm, master_hbm, m1_hbm, m2_hbm, ig, gw_ref, sq_ref, mst, m1, m2,
           attn_ref, og_ref, rx_og, tbuf, tx, at_own, at_rx, wg, g, rx1, rzb, rx3, fbuf, sqs,
           l_s, x_s, x_r, p_s, p_r, z_s, z_r, e_s, e_r, c_s, c_r, r_s, r_r, y_s, y_r, f_s, f_r, q_s, q_r):
    ns = 4
    nz = nb // 2
    tok, din = attn_ref.shape
    dout = og_ref.shape[1]
    r = gw_ref.shape[0]
    half = dout // 2
    block = nb * r
    seq = lax.axis_index("seq")
    batch = lax.axis_index("batch")
    z = batch // 2
    core = batch % 2
    hi = seq // 2
    lo = seq % 2
    sh = (1 - hi) * 2 + lo
    sl = hi * 2 + (1 - lo)
    sd = (1 - hi) * 2 + (1 - lo)
    first = (sl, sh)
    last = (sh, sl)
    cols = (pl.ds(0, half), pl.ds(half, half))
    core_dev = (seq, z * 2 + 1 - core)
    edge = jnp.logical_or(z == 0, z == nz - 1)

    def other(i):
        f = lax.rem(seq * nb + batch + i, ns * nb)
        return (f // nb, lax.rem(f, nb))

    lm = pltpu.make_async_copy(master_hbm, mst, l_s.at[2])
    lm.start()
    la = pltpu.make_async_copy(attn_hbm, attn_ref, l_s.at[0])
    la.start()
    lg = pltpu.make_async_copy(og_hbm, og_ref, l_s.at[1])
    lg.start()
    l1 = pltpu.make_async_copy(m1_hbm, m1, l_s.at[3])
    l1.start()
    l2 = pltpu.make_async_copy(m2_hbm, m2, l_s.at[4])
    l2.start()
    barrier = pltpu.get_barrier_semaphore()

    def greet(s, b):
        pl.semaphore_signal(barrier, inc=1, device_id=(s, b), device_id_type=MESH)

    greet(sl, batch)
    greet(sh, batch)
    greet(*core_dev)
    for step, ok in ((-2, z > 0), (2, z < nz - 1)):
        @pl.when(ok)
        def _():
            greet(seq, batch + step)

    near = jnp.minimum(z, nz - 1 - z)

    def zk(t):
        if t == 0:
            return z
        both = t <= 2 * near
        dist = jnp.where(both, (t + 1) // 2, t - near)
        above = jnp.where(both, t % 2, jnp.where(z < nz - 1 - z, 1, 0))
        return z + dist * (2 * above - 1)

    def wrows(s, zz):
        return pl.ds(pl.multiple_of((s * nb + zz * 2 + core) * r, 16), r)

    def grows(s, zz):
        return pl.ds(pl.multiple_of((zz * ns + s) * r, 16), r)

    def remote(s, d, ssem, rsem, dev):
        return pltpu.make_async_remote_copy(
            src_ref=s, dst_ref=d, send_sem=ssem, recv_sem=rsem,
            device_id=dev, device_id_type=MESH)

    def shard(s, zz, h):
        return wg.at[wrows(s, zz), cols[h]]

    def p_copy(h):
        v = shard(seq, z, h)
        return remote(v, v, p_s.at[h], p_r.at[h], (first[h], batch))

    def z_copy(h, i, t, up):
        zz = zk(t)
        to = jnp.minimum(z + 1, nz - 1) if up else jnp.maximum(z - 1, 0)
        v = shard((seq, first[h])[i], zz, h)
        k = (h * 2 + i) * nz + zz
        return remote(v, v, z_s.at[4 * nz * up + k], z_r.at[k], (seq, to * 2 + core))

    def z_each(h, i, t, act):
        zz = zk(t)
        for up in (0, 1):
            ok = jnp.logical_and(zz <= z, z < nz - 1) if up else jnp.logical_and(zz >= z, z > 0)

            @pl.when(ok)
            def _():
                act(z_copy(h, i, t, up))

    def e_copy(h, i, t):
        v = shard((seq, first[h])[i], zk(t), h)
        k = (h * 2 + i) * nz + t
        return remote(v, v, e_s.at[k], e_r.at[k], (last[h], batch))

    def c_copy(k, t):
        s, h = ((seq, None), (sl, 0), (sh, 1), (sh, 0), (sd, 0), (sl, 1), (sd, 1))[k]
        v = wg.at[wrows(s, zk(t))] if h is None else shard(s, zk(t), h)
        return remote(v, v, c_s.at[7 * t + k], c_r.at[7 * t + k], core_dev)

    def r_copy(h, i, j):
        k = (h * 2 + i) * nz + j
        v = g.at[grows((last[h], sd)[i], zk(nz - 1 - j)), cols[h]]
        return remote(v, rx1.at[k], r_s.at[k], r_r.at[k], (last[h], batch))

    def y_copy(h, i, j):
        t = zk(nz - 1 - j)
        up = t > z
        to = jnp.where(up, jnp.minimum(z + 1, nz - 1), jnp.maximum(z - 1, 0))
        k = (h * 2 + i) * (nz + 1) + jnp.where(jnp.logical_and(jnp.logical_not(up), t == z - 1), nz, t)
        v = g.at[grows((seq, first[h])[i], t), cols[h]]
        return remote(v, rzb.at[k], y_s.at[(h * 2 + i) * nz + j], y_r.at[k], (seq, to * 2 + core))

    def y_slot(h, i, t):
        k = (h * 2 + i) * (nz + 1) + t
        v = g.at[grows(seq, z), cols[h]]
        return remote(v, rzb.at[k], y_s.at[0], y_r.at[k], core_dev), rzb.at[k]

    def f_copy(h):
        v = g.at[grows(first[h], z), cols[h]]
        return remote(v, rx3.at[h], f_s.at[h], f_r.at[h], (first[h], batch))

    def az(t, h, i):
        z_copy(h, i, t, 0).wait_recv()
        z_each(h, i, t, lambda c: c.start())
        if t < nz - 1 or i == 0:
            e_copy(h, i, t).start()
        if i == 1:
            c_copy(1 + h, t).start()
        elif h == 1:
            c_copy(0, t).start()

    def ae(t, h, i):
        e_copy(h, i, t).wait_recv()
        c_copy(3 + 2 * h + i, t).start()

    def rs(j):
        for i in (1, 0):
            for h in (0, 1):
                r_copy(h, i, j).start()

    def rr(j, h, i):
        k = (h * 2 + i) * nz + j
        t = zk(nz - 1 - j)
        rows = grows((seq, first[h])[i], t)
        r_copy(h, i, j).wait_recv()
        more = jnp.logical_or(jnp.logical_and(t > z, z > 0), jnp.logical_and(t < z, z < nz - 1))

        @pl.when(more)
        def _():
            c, buf = y_slot(h, i, t)
            c.wait_recv()
            g[rows, cols[h]] = (g[rows, cols[h]].astype(F32) + rx1[k].astype(F32) + buf[...].astype(F32)).astype(BF16)

        @pl.when(jnp.logical_not(more))
        def _():
            g[rows, cols[h]] = (g[rows, cols[h]].astype(F32) + rx1[k].astype(F32)).astype(BF16)
        y_copy(h, i, j).start()

    def rl(h, i):
        j = nz - 1
        k = (h * 2 + i) * nz + j
        rows = grows((seq, first[h])[i], z)
        dst = gw_ref.at[:, cols[h]] if i == 0 else fbuf.at[h]
        r_copy(h, i, j).wait_recv()
        dst[...] = g[rows, cols[h]].astype(F32) + rx1[k].astype(F32)
        for ok, t in ((z > 0, z), (z < nz - 1, nz)):
            @pl.when(ok)
            def _():
                c, buf = y_slot(h, i, t)
                c.wait_recv()
                dst[...] += buf[...].astype(F32)
        if i == 1:
            g[rows, cols[h]] = dst[...].astype(BF16)
            f_copy(h).start()

    tile = 256
    far_cols = (nz - 1) * 2 * r // 128 * 128
    near_cols = far_cols // (nz - 1)

    def grad(j):
        rows = pl.ds(pl.multiple_of(zk(nz - 1 - j) * (ns * r), 16), ns * r)

        def body(i, carry):
            c = pl.ds(pl.multiple_of(i * tile, tile), tile)
            acc = jnp.dot(at_own[rows, :], og_ref[:, c], preferred_element_type=F32)
            acc += jnp.dot(at_rx[rows, :], rx_og[:, c], preferred_element_type=F32)
            g[rows, c] = acc.astype(BF16)
            return carry
        lax.fori_loop(0, dout // tile, body, 0)

    def part(c):
        v = lax.dot_general(og_ref[...], wg[c, :], (((1,), (1,)), ((), ())), preferred_element_type=F32)
        ig[:, c] = v.astype(BF16)

    def input_cols(s):

        def body(i, carry):
            part(pl.ds(pl.multiple_of(s * block + i * tile, 128), tile))
            return carry
        lax.fori_loop(0, block // tile, body, 0)
        if block % tile:
            part(pl.ds(pl.multiple_of(s * block + block // tile * tile, 128), block % tile))

    xo = remote(og_hbm, rx_og, x_s.at[0], x_r.at[0], core_dev)
    xt = remote(tx, at_rx, x_s.at[1], x_r.at[1], core_dev)

    lm.wait()
    wg[wrows(seq, z), :] = mst[...].astype(BF16)
    pl.semaphore_wait(barrier, 5 - edge.astype(jnp.int32))
    for h in (0, 1):
        p_copy(h).start()
    for h in (0, 1):
        z_each(h, 0, 0, lambda c: c.start())
    for h in (1, 0):
        e_copy(h, 0, 0).start()
    xo.start()
    la.wait()
    for s in range(ns):
        tbuf[...] = attn_ref[:, s * block:(s + 1) * block].T
        for zz in range(nz):
            rows = pl.ds((zz * ns + s) * r, r)
            at_own[rows, :] = tbuf[pl.ds(pl.multiple_of((zz * 2 + core) * r, 16), r), :]
            tx[rows, :] = tbuf[pl.ds(pl.multiple_of((zz * 2 + 1 - core) * r, 16), r), :]
    xt.start()
    c_copy(0, 0).start()
    for h in (0, 1):
        p_copy(h).wait_recv()
        z_each(h, 1, 0, lambda c: c.start())
        e_copy(h, 1, 0).start()
        c_copy(1 + h, 0).start()
    lg.wait()
    xo.wait_recv()
    xt.wait_recv()

    def do(on_edge, inside):
        for ok, events in ((edge, on_edge), (jnp.logical_not(edge), inside)):
            if events:
                @pl.when(ok)
                def _():
                    for f, *a in events:
                        f(*a)

    hs = (0, 1)
    ih = [(h, i) for i in (1, 0) for h in hs]
    grad(0)
    rs(0)
    do([(az, 1, h, 0) for h in hs],
       [(az, t, h, 0) for h in hs for t in (1, 2)])
    grad(1)
    do([(az, 1, 0, 1)],
       [(az, t, 0, 1) for t in (1, 2)])
    grad(2)
    do([(az, 1, 1, 1), (rs, 1)],
       [(az, t, 1, 1) for t in (1, 2)] + [(rs, 1), (rs, 2)])
    do([(rr, 0, h, i) for h, i in ih[:2]], [])
    grad(3)
    do([(rr, 0, h, i) for h, i in ih[2:]]
       + [(az, 2, h, i) for i in hs for h in hs]
       + [(rs, 2)]
       + [(rr, 1, h, i) for h, i in ih]
       + [(ae, t, h, i) for t in (0, 1) for i in hs for h in hs]
       + [(az, 3, h, i) for i in hs for h in hs]
       + [(rs, 3)]
       + [(ae, 2, h, i) for i in hs for h in hs],
       [e for n, (h, i) in enumerate(ih) for e in ((az, 3, n % 2, n // 2), (rr, 0, h, i))]
       + [(rs, 3)]
       + [(ae, t, h, i) for t in (0, 1, 2) for i in hs for h in hs]
       + [(rr, j, h, i) for h, i in ih[:2] for j in (1, 2)])
    for t in range(nz):
        c_copy(0, t).wait_recv()
    do([], [(rr, j, h, i) for h, i in ih[2:] for j in (1, 2)])
    input_cols(seq)
    do([(rr, 2, h, i) for h, i in ih], [])
    for h in hs:
        ae(3, h, 0)
    for h in hs:
        rl(h, 1)
    for h in hs:
        e_copy(h, 1, nz - 1).start()
    for k in (1, 2, 3, 5):
        for t in range(nz):
            c_copy(k, t).wait_recv()
    input_cols(sl)
    input_cols(sh)
    for k in (4, 6):
        for t in range(nz - 1):
            c_copy(k, t).wait_recv()
    for h in hs:
        rl(h, 0)
    part(pl.ds(pl.multiple_of(sd * block + jnp.where(zk(nz - 1) == 0, block - far_cols, 0), 128), far_cols))
    for h in hs:
        f_copy(h).wait_recv()
        gw_ref[:, cols[h]] += rx3[h].astype(F32)

    v = gw_ref[...]
    fold = jnp.sum((v * v).reshape(r // 8, 8, dout), axis=0)
    acc = fold[:, :128]
    for i in range(1, dout // 128):
        acc += fold[:, i * 128:(i + 1) * 128]
    sqs[0] = jnp.sum(acc, axis=0, keepdims=True)

    def q_copy(i):
        return remote(sqs.at[0], sqs.at[i], q_s.at[i], q_r.at[i], other(i))

    def q_start(i, carry):
        q_copy(i).start()
        return carry

    def q_wait(i, carry):
        q_copy(i).wait()
        return carry

    lax.fori_loop(1, ns * nb, q_start, 0)
    for h in hs:
        ae(3, h, 1)
    for h in hs:
        p_copy(h).wait_send()
        f_copy(h).wait_send()
        for i in hs:
            for t in range(nz):
                z_each(h, i, t, lambda c: c.wait_send())
                e_copy(h, i, t).wait_send()
                r_copy(h, i, t).wait_send()
                if t < nz - 1:
                    y_copy(h, i, t).wait_send()
    xo.wait_send()
    xt.wait_send()
    for k in (4, 6):
        c_copy(k, nz - 1).wait_recv()
    part(pl.ds(pl.multiple_of(sd * block + zk(nz - 1) * near_cols, 128), block - far_cols))
    for t in range(nz):
        for k in range(7):
            c_copy(k, t).wait_send()
    l1.wait()
    l2.wait()
    lax.fori_loop(1, ns * nb, q_wait, 0)
    total = sqs[0]
    for i in range(1, ns * nb):
        total += sqs[i]
    sq_ref[...] = total


def finish(size, ig, gw, sq, mst, m1, m2, ig_hbm, nm_hbm, n1_hbm, n2_hbm, nm, n1, n2, i_s, o_s):
    ci = pltpu.make_async_copy(ig, ig_hbm, i_s.at[0])
    ci.start()
    steps = gw.shape[0] // 8
    squares = jnp.sum(sq[...], axis=1, keepdims=True)

    def copies(i):
        rows = pl.ds(pl.multiple_of(i * 8, 8), 8)
        return [pltpu.make_async_copy(a.at[rows], b.at[rows], o_s.at[k, i])
                for k, (a, b) in enumerate(((nm, nm_hbm), (n1, n1_hbm), (n2, n2_hbm)))]

    def body(i, carry):
        rows = pl.ds(pl.multiple_of(i * 8, 8), 8)
        nm[rows, :], n1[rows, :], n2[rows, :] = update(
            gw[rows, :], squares, mst[rows, :], m1[rows, :], m2[rows, :], size)
        for c in copies(i):
            c.start()
        return carry

    def drain(i, carry):
        for c in copies(i):
            c.wait()
        return carry

    lax.fori_loop(0, steps, body, 0)
    lax.fori_loop(0, steps, drain, 0)
    ci.wait()


def fused(attn_out, out_grad, master, moment_one, moment_two, ns, nb):
    tok, din = attn_out.shape
    dout = out_grad.shape[1]
    r = master.shape[0]
    half = dout // 2
    nz = nb // 2
    n = ns * nb
    dma = lambda k: pltpu.SemaphoreType.DMA((k,))
    vm = pl.BlockSpec(memory_space=pltpu.VMEM)
    hbm = pl.BlockSpec(memory_space=pl.ANY)
    sems = [5, 2, 2, 2, 2, 8 * nz, 4 * nz, 4 * nz, 4 * nz, 7 * nz, 7 * nz,
            4 * nz, 4 * nz, 4 * nz, 4 * (nz + 1), 2, 2, n, n]
    flat = (r, dout), F32
    held = pl.pallas_call(
        functools.partial(kernel, nb),
        out_shape=tuple(pltpu.VMEM(*o) for o in (((tok, din), BF16), flat, ((1, 128), F32), flat, flat, flat)),
        in_specs=[hbm] * 5,
        out_specs=(vm,) * 6,
        scratch_shapes=[
            pltpu.VMEM((tok, din), BF16),
            pltpu.VMEM((tok, dout), BF16),
            pltpu.VMEM((tok, dout), BF16),
            pltpu.VMEM((nb * r, tok), BF16),
            pltpu.VMEM((din // 2, tok), BF16),
            pltpu.VMEM((din // 2, tok), BF16),
            pltpu.VMEM((din // 2, tok), BF16),
            pltpu.VMEM((din, dout), BF16),
            pltpu.VMEM((din // 2, dout), BF16),
            pltpu.VMEM((4 * nz, r, half), BF16),
            pltpu.VMEM((4 * (nz + 1), r, half), BF16),
            pltpu.VMEM((2, r, half), BF16),
            pltpu.VMEM((2, r, half), F32),
            pltpu.VMEM((n, 1, 128), F32),
        ] + [dma(k) for k in sems],
        compiler_params=pltpu.CompilerParams(
            collective_id=0, has_side_effects=True, vmem_limit_bytes=52_000_000),
    )(attn_out, out_grad, master, moment_one, moment_two)
    return pl.pallas_call(
        functools.partial(finish, din * dout),
        out_shape=(jax.ShapeDtypeStruct((tok, din), BF16),) + (jax.ShapeDtypeStruct(*flat),) * 3,
        in_specs=[vm] * 6,
        out_specs=(hbm,) * 4,
        scratch_shapes=[pltpu.VMEM(*flat)] * 3 + [dma(1), pltpu.SemaphoreType.DMA((3, r // 8))],
        compiler_params=pltpu.CompilerParams(vmem_limit_bytes=6_000_000),
    )(*(pltpu.with_memory_space_constraint(v, pltpu.VMEM) for v in held))


def plain(attn_out, out_grad, shard_weight):
    projected = lax.dot_general(
        out_grad,
        lax.all_gather(shard_weight, ("seq", "batch"), axis=0, tiled=True),
        (((1,), (1,)), ((), ())),
        preferred_element_type=F32,
    )
    width = out_grad.shape[1] // GRAD_BLOCKS
    parts = []
    for b in range(GRAD_BLOCKS):
        d = lax.dot_general(
            attn_out, out_grad[:, b * width:(b + 1) * width],
            (((0,), (0,)), ((), ())), preferred_element_type=F32).astype(BF16)
        d = lax.psum_scatter(d, "seq", scatter_dimension=0, tiled=True)
        parts.append(lax.psum_scatter(d, "batch", scatter_dimension=0, tiled=True).astype(F32))
    weight_grad = jnp.concatenate(parts, axis=1)
    squares = lax.psum(jnp.sum(weight_grad * weight_grad), ("seq", "batch"))
    return projected.astype(BF16), weight_grad, squares


def on_device(ns, nb, attn_out, out_grad, master, moment_one, moment_two):
    r, dout = master.shape
    din = attn_out.shape[1]
    if ns == 4 and nb == 8 and r % 16 == 0 and (nb * r) % 128 == 0 and dout % 256 == 0:
        return fused(attn_out, out_grad, master, moment_one, moment_two, ns, nb)
    input_grad, weight_grad, squares = plain(attn_out, out_grad, master.astype(BF16))
    return (input_grad,) + update(weight_grad, squares, master, moment_one, moment_two, din * dout)


def solution(mesh):
    spec = P(("seq", "batch"), None)
    return jax.shard_map(
        functools.partial(on_device, mesh.shape["seq"], mesh.shape["batch"]),
        mesh=mesh,
        in_specs=(spec,) * 5,
        out_specs=(spec,) * 4,
        check_vma=False,
    )
```

```python
import functools
import jax
import jax.numpy as jnp
from jax import lax
from jax.experimental import pallas as pl
from jax.experimental.pallas import tpu as pltpu
from jax.sharding import PartitionSpec as P

GRAD_BLOCKS = 4
STEP = 10
MESH = pl.DeviceIdType.MESH
F32 = jnp.float32
BF16 = jnp.bfloat16


def update(weight_grad, squares, master, moment_one, moment_two, size):
    grad_norm = jnp.sqrt(squares) + 1e-06
    limit = jnp.sqrt(jnp.float32(size))
    clipped = weight_grad * jnp.minimum(jnp.float32(1.0), limit / grad_norm)
    new_one = 0.9 * moment_one + 0.1 * clipped
    new_two = 0.999 * moment_two + 0.001 * clipped * clipped
    first_hat = new_one * (1.0 / (1.0 - 0.9**STEP))
    second_hat = new_two * (1.0 / (1.0 - 0.999**STEP))
    new_master = master - 0.01 * (first_hat / (jnp.sqrt(second_hat) + 1e-08) + 0.1 * master)
    return new_master, new_one, new_two


def kernel(nb, attn_hbm, og_hbm, master_hbm, m1_hbm, m2_hbm, ig, gw_ref, sq_ref, mst, m1, m2,
           attn_ref, og_ref, rx_og, tbuf, tx, at_own, at_rx, wg, g, rx1, rzb, rx3, fbuf, sqs,
           l_s, x_s, x_r, p_s, p_r, z_s, z_r, e_s, e_r, c_s, c_r, r_s, r_r, y_s, y_r, f_s, f_r, q_s, q_r):
    ns = 4
    nz = nb // 2
    tok, din = attn_ref.shape
    dout = og_ref.shape[1]
    r = gw_ref.shape[0]
    half = dout // 2
    block = nb * r
    seq = lax.axis_index("seq")
    batch = lax.axis_index("batch")
    z = batch // 2
    core = batch % 2
    hi = seq // 2
    lo = seq % 2
    sh = (1 - hi) * 2 + lo
    sl = hi * 2 + (1 - lo)
    sd = (1 - hi) * 2 + (1 - lo)
    first = (sl, sh)
    last = (sh, sl)
    cols = (pl.ds(0, half), pl.ds(half, half))
    core_dev = (seq, z * 2 + 1 - core)
    edge = jnp.logical_or(z == 0, z == nz - 1)

    def other(i):
        f = lax.rem(seq * nb + batch + i, ns * nb)
        return (f // nb, lax.rem(f, nb))

    lm = pltpu.make_async_copy(master_hbm, mst, l_s.at[2])
    lm.start()
    la = pltpu.make_async_copy(attn_hbm, attn_ref, l_s.at[0])
    la.start()
    lg = pltpu.make_async_copy(og_hbm, og_ref, l_s.at[1])
    lg.start()
    l1 = pltpu.make_async_copy(m1_hbm, m1, l_s.at[3])
    l1.start()
    l2 = pltpu.make_async_copy(m2_hbm, m2, l_s.at[4])
    l2.start()
    barrier = pltpu.get_barrier_semaphore()

    def greet(s, b):
        pl.semaphore_signal(barrier, inc=1, device_id=(s, b), device_id_type=MESH)

    greet(sl, batch)
    greet(sh, batch)
    greet(*core_dev)
    for step, ok in ((-2, z > 0), (2, z < nz - 1)):
        @pl.when(ok)
        def _():
            greet(seq, batch + step)

    near = jnp.minimum(z, nz - 1 - z)

    def zk(t):
        if t == 0:
            return z
        both = t <= 2 * near
        dist = jnp.where(both, (t + 1) // 2, t - near)
        above = jnp.where(both, t % 2, jnp.where(z < nz - 1 - z, 1, 0))
        return z + dist * (2 * above - 1)

    def wrows(s, zz):
        return pl.ds(pl.multiple_of((s * nb + zz * 2 + core) * r, 16), r)

    def grows(s, zz):
        return pl.ds(pl.multiple_of((zz * ns + s) * r, 16), r)

    def remote(s, d, ssem, rsem, dev):
        return pltpu.make_async_remote_copy(
            src_ref=s, dst_ref=d, send_sem=ssem, recv_sem=rsem,
            device_id=dev, device_id_type=MESH)

    def shard(s, zz, h):
        return wg.at[wrows(s, zz), cols[h]]

    def p_copy(h):
        v = shard(seq, z, h)
        return remote(v, v, p_s.at[0], p_r.at[h], (first[h], batch))

    def z_copy(h, i, t, up):
        zz = zk(t)
        to = jnp.minimum(z + 1, nz - 1) if up else jnp.maximum(z - 1, 0)
        v = shard((seq, first[h])[i], zz, h)
        k = (h * 2 + i) * nz + zz
        return remote(v, v, z_s.at[up], z_r.at[k], (seq, to * 2 + core))

    def z_each(h, i, t, act):
        zz = zk(t)
        for up in (0, 1):
            ok = jnp.logical_and(zz <= z, z < nz - 1) if up else jnp.logical_and(zz >= z, z > 0)

            @pl.when(ok)
            def _():
                act(z_copy(h, i, t, up))

    def e_copy(h, i, t):
        v = shard((seq, first[h])[i], zk(t), h)
        k = (h * 2 + i) * nz + t
        return remote(v, v, e_s.at[0], e_r.at[k], (last[h], batch))

    def c_copy(k, t):
        s, h = ((seq, None), (sl, 0), (sh, 1), (sh, 0), (sd, 0), (sl, 1), (sd, 1))[k]
        v = wg.at[wrows(s, zk(t))] if h is None else shard(s, zk(t), h)
        return remote(v, v, c_s.at[0], c_r.at[c_group(k, t)], core_dev)

    def c_group(k, t):
        if k in (4, 6):
            return 3 if t == nz - 1 else 2
        return 1 if k else 0

    def r_copy(h, i, j):
        k = (h * 2 + i) * nz + j
        v = g.at[grows((last[h], sd)[i], zk(nz - 1 - j)), cols[h]]
        return remote(v, rx1.at[k], r_s.at[0], r_r.at[k], (last[h], batch))

    def y_copy(h, i, j):
        t = zk(nz - 1 - j)
        up = t > z
        to = jnp.where(up, jnp.minimum(z + 1, nz - 1), jnp.maximum(z - 1, 0))
        k = (h * 2 + i) * (nz + 1) + jnp.where(jnp.logical_and(jnp.logical_not(up), t == z - 1), nz, t)
        v = g.at[grows((seq, first[h])[i], t), cols[h]]
        return remote(v, rzb.at[k], y_s.at[0], y_r.at[k], (seq, to * 2 + core))

    def y_slot(h, i, t):
        k = (h * 2 + i) * (nz + 1) + t
        v = g.at[grows(seq, z), cols[h]]
        return remote(v, rzb.at[k], y_s.at[0], y_r.at[k], core_dev), rzb.at[k]

    def f_copy(h):
        v = g.at[grows(first[h], z), cols[h]]
        return remote(v, rx3.at[h], f_s.at[0], f_r.at[h], (first[h], batch))

    def all_of(ref, ssem, rsem):
        return remote(ref, ref, ssem, rsem, core_dev)

    def c_wait(group):
        rows = (nz * r, 4 * nz * r // 2, 6 * (nz - 1) * r // 6, r)[group]
        all_of(wg.at[pl.ds(0, rows)], c_s.at[0], c_r.at[group]).wait_recv()

    def az(t, h, i):
        z_copy(h, i, t, 0).wait_recv()
        z_each(h, i, t, lambda c: c.start())
        if t < nz - 1 or i == 0:
            e_copy(h, i, t).start()
        if i == 1:
            c_copy(1 + h, t).start()
        elif h == 1:
            c_copy(0, t).start()

    def ae(t, h, i):
        e_copy(h, i, t).wait_recv()
        c_copy(3 + 2 * h + i, t).start()

    def rs(j):
        for i in (1, 0):
            for h in (0, 1):
                r_copy(h, i, j).start()

    def rr(j, h, i):
        k = (h * 2 + i) * nz + j
        t = zk(nz - 1 - j)
        rows = grows((seq, first[h])[i], t)
        r_copy(h, i, j).wait_recv()
        more = jnp.logical_or(jnp.logical_and(t > z, z > 0), jnp.logical_and(t < z, z < nz - 1))

        @pl.when(more)
        def _():
            c, buf = y_slot(h, i, t)
            c.wait_recv()
            g[rows, cols[h]] = (g[rows, cols[h]].astype(F32) + rx1[k].astype(F32) + buf[...].astype(F32)).astype(BF16)

        @pl.when(jnp.logical_not(more))
        def _():
            g[rows, cols[h]] = (g[rows, cols[h]].astype(F32) + rx1[k].astype(F32)).astype(BF16)
        y_copy(h, i, j).start()

    def rl(h, i):
        j = nz - 1
        k = (h * 2 + i) * nz + j
        rows = grows((seq, first[h])[i], z)
        dst = gw_ref.at[:, cols[h]] if i == 0 else fbuf.at[h]
        r_copy(h, i, j).wait_recv()
        dst[...] = g[rows, cols[h]].astype(F32) + rx1[k].astype(F32)
        for ok, t in ((z > 0, z), (z < nz - 1, nz)):
            @pl.when(ok)
            def _():
                c, buf = y_slot(h, i, t)
                c.wait_recv()
                dst[...] += buf[...].astype(F32)
        if i == 1:
            g[rows, cols[h]] = dst[...].astype(BF16)
            f_copy(h).start()

    tile = 256
    far_cols = (nz - 1) * 2 * r // 128 * 128
    near_cols = far_cols // (nz - 1)

    def grad(j):
        rows = pl.ds(pl.multiple_of(zk(nz - 1 - j) * (ns * r), 16), ns * r)

        def body(i, carry):
            c = pl.ds(pl.multiple_of(i * tile, tile), tile)
            acc = jnp.dot(at_own[rows, :], og_ref[:, c], preferred_element_type=F32)
            acc += jnp.dot(at_rx[rows, :], rx_og[:, c], preferred_element_type=F32)
            g[rows, c] = acc.astype(BF16)
            return carry
        lax.fori_loop(0, dout // tile, body, 0)

    def part(c):
        v = lax.dot_general(og_ref[...], wg[c, :], (((1,), (1,)), ((), ())), preferred_element_type=F32)
        ig[:, c] = v.astype(BF16)

    def input_cols(s):

        def body(i, carry):
            part(pl.ds(pl.multiple_of(s * block + i * tile, 128), tile))
            return carry
        lax.fori_loop(0, block // tile, body, 0)
        if block % tile:
            part(pl.ds(pl.multiple_of(s * block + block // tile * tile, 128), block % tile))

    xo = remote(og_hbm, rx_og, x_s.at[0], x_r.at[0], core_dev)
    xt = remote(tx, at_rx, x_s.at[1], x_r.at[1], core_dev)

    lm.wait()
    wg[wrows(seq, z), :] = mst[...].astype(BF16)
    pl.semaphore_wait(barrier, 5 - edge.astype(jnp.int32))
    for h in (0, 1):
        p_copy(h).start()
    for h in (0, 1):
        z_each(h, 0, 0, lambda c: c.start())
    for h in (1, 0):
        e_copy(h, 0, 0).start()
    xo.start()
    la.wait()
    for s in range(ns):
        tbuf[...] = attn_ref[:, s * block:(s + 1) * block].T
        for zz in range(nz):
            rows = pl.ds((zz * ns + s) * r, r)
            at_own[rows, :] = tbuf[pl.ds(pl.multiple_of((zz * 2 + core) * r, 16), r), :]
            tx[rows, :] = tbuf[pl.ds(pl.multiple_of((zz * 2 + 1 - core) * r, 16), r), :]
    xt.start()
    c_copy(0, 0).start()
    for h in (0, 1):
        p_copy(h).wait_recv()
        z_each(h, 1, 0, lambda c: c.start())
        e_copy(h, 1, 0).start()
        c_copy(1 + h, 0).start()
    lg.wait()
    xo.wait_recv()
    xt.wait_recv()

    def do(on_edge, inside):
        for ok, events in ((edge, on_edge), (jnp.logical_not(edge), inside)):
            if events:
                @pl.when(ok)
                def _():
                    for f, *a in events:
                        f(*a)

    hs = (0, 1)
    ih = [(h, i) for i in (1, 0) for h in hs]
    grad(0)
    rs(0)
    do([(az, 1, h, 0) for h in hs],
       [(az, t, h, 0) for h in hs for t in (1, 2)])
    grad(1)
    do([(az, 1, 0, 1)],
       [(az, t, 0, 1) for t in (1, 2)])
    grad(2)
    do([(az, 1, 1, 1), (rs, 1)],
       [(az, t, 1, 1) for t in (1, 2)] + [(rs, 1), (rs, 2)])
    do([(rr, 0, h, i) for h, i in ih[:2]], [])
    grad(3)
    do([(rr, 0, h, i) for h, i in ih[2:]]
       + [(az, 2, h, i) for i in hs for h in hs]
       + [(rs, 2)]
       + [(rr, 1, h, i) for h, i in ih]
       + [(ae, t, h, i) for t in (0, 1) for i in hs for h in hs]
       + [(az, 3, h, i) for i in hs for h in hs]
       + [(rs, 3)]
       + [(ae, 2, h, i) for i in hs for h in hs],
       [e for n, (h, i) in enumerate(ih) for e in ((az, 3, n % 2, n // 2), (rr, 0, h, i))]
       + [(rs, 3)]
       + [(ae, t, h, i) for t in (0, 1, 2) for i in hs for h in hs]
       + [(rr, j, h, i) for h, i in ih[:2] for j in (1, 2)])
    c_wait(0)
    do([], [(rr, j, h, i) for h, i in ih[2:] for j in (1, 2)])
    input_cols(seq)
    do([(rr, 2, h, i) for h, i in ih], [])
    for h in hs:
        ae(3, h, 0)
    for h in hs:
        rl(h, 1)
    for h in hs:
        e_copy(h, 1, nz - 1).start()
    c_wait(1)
    input_cols(sl)
    input_cols(sh)
    c_wait(2)
    for h in hs:
        rl(h, 0)
    part(pl.ds(pl.multiple_of(sd * block + jnp.where(zk(nz - 1) == 0, block - far_cols, 0), 128), far_cols))
    for h in hs:
        f_copy(h).wait_recv()
        gw_ref[:, cols[h]] += rx3[h].astype(F32)

    v = gw_ref[...]
    fold = jnp.sum((v * v).reshape(r // 8, 8, dout), axis=0)
    acc = fold[:, :128]
    for i in range(1, dout // 128):
        acc += fold[:, i * 128:(i + 1) * 128]
    sqs[0] = jnp.sum(acc, axis=0, keepdims=True)

    def q_copy(i):
        return remote(sqs.at[0], sqs.at[i], q_s.at[0], q_r.at[0], other(i))

    def q_start(i, carry):
        q_copy(i).start()
        return carry

    lax.fori_loop(1, ns * nb, q_start, 0)
    for h in hs:
        ae(3, h, 1)
    xo.wait_send()
    xt.wait_send()
    c_wait(3)
    part(pl.ds(pl.multiple_of(sd * block + zk(nz - 1) * near_cols, 128), block - far_cols))
    for n, sem in ((2, p_s), (2, f_s), (4 * nz, e_s), (4 * nz, r_s), (4 * (nz - 1), y_s)):
        all_of(rx1.at[pl.ds(0, n)], sem.at[0], q_r.at[0]).wait_send()
    for k in range(nz):
        @pl.when(z == k)
        def _():
            if k < nz - 1:
                all_of(rx1.at[pl.ds(0, 4 * (k + 1))], z_s.at[1], q_r.at[0]).wait_send()
            if k:
                all_of(rx1.at[pl.ds(0, 4 * (nz - k))], z_s.at[0], q_r.at[0]).wait_send()
    all_of(wg.at[pl.ds(0, 4 * nz * r)], c_s.at[0], q_r.at[0]).wait_send()
    l1.wait()
    l2.wait()
    all_of(sqs.at[pl.ds(1, ns * nb - 1)], q_s.at[0], q_r.at[0]).wait()
    total = sqs[0]
    for i in range(1, ns * nb):
        total += sqs[i]
    sq_ref[...] = total


def finish(size, ig, gw, sq, mst, m1, m2, ig_hbm, nm_hbm, n1_hbm, n2_hbm, nm, n1, n2, i_s, o_s):
    ci = pltpu.make_async_copy(ig, ig_hbm, i_s.at[0])
    ci.start()
    steps = gw.shape[0] // 8
    squares = jnp.sum(sq[...], axis=1, keepdims=True)

    def copies(i):
        rows = pl.ds(pl.multiple_of(i * 8, 8), 8)
        return [pltpu.make_async_copy(a.at[rows], b.at[rows], o_s.at[k, i])
                for k, (a, b) in enumerate(((nm, nm_hbm), (n1, n1_hbm), (n2, n2_hbm)))]

    def body(i, carry):
        rows = pl.ds(pl.multiple_of(i * 8, 8), 8)
        nm[rows, :], n1[rows, :], n2[rows, :] = update(
            gw[rows, :], squares, mst[rows, :], m1[rows, :], m2[rows, :], size)
        for c in copies(i):
            c.start()
        return carry

    def drain(i, carry):
        for c in copies(i):
            c.wait()
        return carry

    lax.fori_loop(0, steps, body, 0)
    lax.fori_loop(0, steps, drain, 0)
    ci.wait()


def fused(attn_out, out_grad, master, moment_one, moment_two, ns, nb):
    tok, din = attn_out.shape
    dout = out_grad.shape[1]
    r = master.shape[0]
    half = dout // 2
    nz = nb // 2
    n = ns * nb
    dma = lambda k: pltpu.SemaphoreType.DMA((k,))
    vm = pl.BlockSpec(memory_space=pltpu.VMEM)
    hbm = pl.BlockSpec(memory_space=pl.ANY)
    sems = [5, 2, 2, 1, 2, 2, 4 * nz, 1, 4 * nz, 1, 4, 1, 4 * nz, 1, 4 * (nz + 1), 1, 2, 1, 1]
    flat = (r, dout), F32
    held = pl.pallas_call(
        functools.partial(kernel, nb),
        out_shape=tuple(pltpu.VMEM(*o) for o in (((tok, din), BF16), flat, ((1, 128), F32), flat, flat, flat)),
        in_specs=[hbm] * 5,
        out_specs=(vm,) * 6,
        scratch_shapes=[
            pltpu.VMEM((tok, din), BF16),
            pltpu.VMEM((tok, dout), BF16),
            pltpu.VMEM((tok, dout), BF16),
            pltpu.VMEM((nb * r, tok), BF16),
            pltpu.VMEM((din // 2, tok), BF16),
            pltpu.VMEM((din // 2, tok), BF16),
            pltpu.VMEM((din // 2, tok), BF16),
            pltpu.VMEM((din, dout), BF16),
            pltpu.VMEM((din // 2, dout), BF16),
            pltpu.VMEM((4 * nz, r, half), BF16),
            pltpu.VMEM((4 * (nz + 1), r, half), BF16),
            pltpu.VMEM((2, r, half), BF16),
            pltpu.VMEM((2, r, half), F32),
            pltpu.VMEM((n, 1, 128), F32),
        ] + [dma(k) for k in sems],
        compiler_params=pltpu.CompilerParams(
            collective_id=0, has_side_effects=True, vmem_limit_bytes=52_000_000),
    )(attn_out, out_grad, master, moment_one, moment_two)
    return pl.pallas_call(
        functools.partial(finish, din * dout),
        out_shape=(jax.ShapeDtypeStruct((tok, din), BF16),) + (jax.ShapeDtypeStruct(*flat),) * 3,
        in_specs=[vm] * 6,
        out_specs=(hbm,) * 4,
        scratch_shapes=[pltpu.VMEM(*flat)] * 3 + [dma(1), pltpu.SemaphoreType.DMA((3, r // 8))],
        compiler_params=pltpu.CompilerParams(vmem_limit_bytes=6_000_000),
    )(*(pltpu.with_memory_space_constraint(v, pltpu.VMEM) for v in held))


def plain(attn_out, out_grad, shard_weight):
    projected = lax.dot_general(
        out_grad,
        lax.all_gather(shard_weight, ("seq", "batch"), axis=0, tiled=True),
        (((1,), (1,)), ((), ())),
        preferred_element_type=F32,
    )
    width = out_grad.shape[1] // GRAD_BLOCKS
    parts = []
    for b in range(GRAD_BLOCKS):
        d = lax.dot_general(
            attn_out, out_grad[:, b * width:(b + 1) * width],
            (((0,), (0,)), ((), ())), preferred_element_type=F32).astype(BF16)
        d = lax.psum_scatter(d, "seq", scatter_dimension=0, tiled=True)
        parts.append(lax.psum_scatter(d, "batch", scatter_dimension=0, tiled=True).astype(F32))
    weight_grad = jnp.concatenate(parts, axis=1)
    squares = lax.psum(jnp.sum(weight_grad * weight_grad), ("seq", "batch"))
    return projected.astype(BF16), weight_grad, squares


def on_device(ns, nb, attn_out, out_grad, master, moment_one, moment_two):
    r, dout = master.shape
    din = attn_out.shape[1]
    if ns == 4 and nb == 8 and r % 16 == 0 and (nb * r) % 128 == 0 and dout % 256 == 0:
        return fused(attn_out, out_grad, master, moment_one, moment_two, ns, nb)
    input_grad, weight_grad, squares = plain(attn_out, out_grad, master.astype(BF16))
    return (input_grad,) + update(weight_grad, squares, master, moment_one, moment_two, din * dout)


def solution(mesh):
    spec = P(("seq", "batch"), None)
    return jax.shard_map(
        functools.partial(on_device, mesh.shape["seq"], mesh.shape["batch"]),
        mesh=mesh,
        in_specs=(spec,) * 5,
        out_specs=(spec,) * 4,
        check_vma=False,
    )
```

```python
import functools
import jax
import jax.numpy as jnp
from jax import lax
from jax.experimental import pallas as pl
from jax.experimental.pallas import tpu as pltpu
from jax.sharding import PartitionSpec as P

GRAD_BLOCKS = 4
STEP = 10
MESH = pl.DeviceIdType.MESH
F32 = jnp.float32
BF16 = jnp.bfloat16


def update(weight_grad, squares, master, moment_one, moment_two, size):
    grad_norm = jnp.sqrt(squares) + 1e-06
    limit = jnp.sqrt(jnp.float32(size))
    clipped = weight_grad * jnp.minimum(jnp.float32(1.0), limit / grad_norm)
    new_one = 0.9 * moment_one + 0.1 * clipped
    new_two = 0.999 * moment_two + 0.001 * clipped * clipped
    first_hat = new_one * (1.0 / (1.0 - 0.9**STEP))
    second_hat = new_two * (1.0 / (1.0 - 0.999**STEP))
    new_master = master - 0.01 * (first_hat / (jnp.sqrt(second_hat) + 1e-08) + 0.1 * master)
    return new_master, new_one, new_two


def widths(dout):
    tiles = dout // 128 - 1
    wide = (tiles + 1) // 2 * 128
    return wide, tiles * 128 - wide, tiles * 128


def kernel(nb, attn_hbm, og_hbm, master_hbm, m1_hbm, m2_hbm, ig, gw_ref, sq_ref, mst, m1, m2,
           attn_ref, og_ref, rx_og, tbuf, tx, at_own, at_rx, wg, g, rx1, rzb, rx3, fbuf, sqs,
           tz, ty, tl, tsum,
           l_s, x_s, x_r, p_s, p_r, z_s, z_r, e_s, e_r, c_s, c_r, r_s, r_r, y_s, y_r, f_s, f_r, q_s, q_r,
           a_s, a_r, b_s, b_r, d_s, d_r, t_s, t_r, u_s, u_r):
    ns = 4
    nz = nb // 2
    tok, din = attn_ref.shape
    dout = og_ref.shape[1]
    r = gw_ref.shape[0]
    block = nb * r
    seq = lax.axis_index("seq")
    batch = lax.axis_index("batch")
    z = batch // 2
    core = batch % 2
    hi = seq // 2
    lo = seq % 2
    sh = (1 - hi) * 2 + lo
    sl = hi * 2 + (1 - lo)
    sd = (1 - hi) * 2 + (1 - lo)
    first = (sl, sh)
    last = (sh, sl)
    wide, slim, both = widths(dout)
    gcols = (pl.ds(0, wide), pl.ds(wide, slim))
    rcols = (pl.ds(0, slim), pl.ds(slim, wide))
    rw = (pl.ds(0, slim), pl.ds(0, wide))
    bcols = pl.ds(0, both)
    tcols = pl.ds(both, dout - both)
    core_dev = (seq, z * 2 + 1 - core)
    edge = jnp.logical_or(z == 0, z == nz - 1)

    def other(i):
        f = lax.rem(seq * nb + batch + i, ns * nb)
        return (f // nb, lax.rem(f, nb))

    lm = pltpu.make_async_copy(master_hbm, mst, l_s.at[2])
    lm.start()
    la = pltpu.make_async_copy(attn_hbm, attn_ref, l_s.at[0])
    la.start()
    lg = pltpu.make_async_copy(og_hbm, og_ref, l_s.at[1])
    lg.start()
    l1 = pltpu.make_async_copy(m1_hbm, m1, l_s.at[3])
    l1.start()
    l2 = pltpu.make_async_copy(m2_hbm, m2, l_s.at[4])
    l2.start()
    barrier = pltpu.get_barrier_semaphore()

    def greet(s, b):
        pl.semaphore_signal(barrier, inc=1, device_id=(s, b), device_id_type=MESH)

    greet(sl, batch)
    greet(sh, batch)
    greet(*core_dev)
    for step, ok in ((-2, z > 0), (2, z < nz - 1)):
        @pl.when(ok)
        def _():
            greet(seq, batch + step)

    near = jnp.minimum(z, nz - 1 - z)

    def zk(t):
        if t == 0:
            return z
        both = t <= 2 * near
        dist = jnp.where(both, (t + 1) // 2, t - near)
        above = jnp.where(both, t % 2, jnp.where(z < nz - 1 - z, 1, 0))
        return z + dist * (2 * above - 1)

    def wrows(zz):
        return pl.ds(pl.multiple_of((zz * 2 + core) * r, 16), r)

    def grows(s, zz):
        return pl.ds(pl.multiple_of((zz * ns + s) * r, 16), r)

    def remote(s, d, ssem, rsem, dev):
        return pltpu.make_async_remote_copy(
            src_ref=s, dst_ref=d, send_sem=ssem, recv_sem=rsem,
            device_id=dev, device_id_type=MESH)

    def shard(s, zz, h):
        return wg.at[s, wrows(zz), gcols[h]]

    def p_copy(h):
        v = shard(seq, z, h)
        return remote(v, v, p_s.at[0], p_r.at[h], (first[h], batch))

    def z_copy(h, i, t, up):
        zz = zk(t)
        to = jnp.minimum(z + 1, nz - 1) if up else jnp.maximum(z - 1, 0)
        v = shard((seq, first[h])[i], zz, h)
        k = (h * 2 + i) * nz + zz
        return remote(v, v, z_s.at[up], z_r.at[k], (seq, to * 2 + core))

    def z_each(h, i, t, act):
        zz = zk(t)
        for up in (0, 1):
            ok = jnp.logical_and(zz <= z, z < nz - 1) if up else jnp.logical_and(zz >= z, z > 0)

            @pl.when(ok)
            def _():
                act(z_copy(h, i, t, up))

    def e_copy(h, i, t):
        v = shard((seq, first[h])[i], zk(t), h)
        k = (h * 2 + i) * nz + t
        return remote(v, v, e_s.at[0], e_r.at[k], (last[h], batch))

    def c_copy(k, t):
        s, h = ((seq, None), (sl, 0), (sh, 1), (sh, 0), (sd, 0), (sl, 1), (sd, 1))[k]
        v = wg.at[s, wrows(zk(t)), bcols] if h is None else shard(s, zk(t), h)
        return remote(v, v, c_s.at[0], c_r.at[c_group(k, t)], core_dev)

    def c_group(k, t):
        if t < nz - 1:
            return 0
        return 3 if k in (4, 6) else 2 if k else 1

    def r_copy(h, i, j):
        k = (h * 2 + i) * nz + j
        v = g.at[grows((last[h], sd)[i], zk(nz - 1 - j)), rcols[h]]
        return remote(v, rx1.at[k, :, rw[h]], r_s.at[0], r_r.at[k], (last[h], batch))

    def y_copy(h, i, j):
        t = zk(nz - 1 - j)
        up = t > z
        to = jnp.where(up, jnp.minimum(z + 1, nz - 1), jnp.maximum(z - 1, 0))
        k = (h * 2 + i) * (nz + 1) + jnp.where(jnp.logical_and(jnp.logical_not(up), t == z - 1), nz, t)
        v = g.at[grows((seq, first[h])[i], t), rcols[h]]
        return remote(v, rzb.at[k, :, rw[h]], y_s.at[0], y_r.at[k], (seq, to * 2 + core))

    def y_slot(h, i, t):
        k = (h * 2 + i) * (nz + 1) + t
        v = rzb.at[k, :, rw[h]]
        return remote(v, v, y_s.at[0], y_r.at[k], core_dev), v

    def f_copy(h):
        v = g.at[grows(first[h], z), rcols[h]]
        return remote(v, rx3.at[h, :, rw[h]], f_s.at[0], f_r.at[h], (first[h], batch))

    def all_of(ref, ssem, rsem):
        return remote(ref, ref, ssem, rsem, core_dev)

    def c_wait(group):
        v = (wg.at[pl.ds(0, nz - 1), pl.ds(0, ns * r), bcols] if group == 0
             else wg.at[0, pl.ds(0, (1, 2, 1)[group - 1] * r), bcols])
        all_of(v, c_s.at[0], c_r.at[group]).wait_recv()

    def d_wait(group):
        v = wg.at[:, pl.ds(0, (nz - 1, 1)[group] * r), tcols]
        all_of(v, d_s.at[0], d_r.at[group]).wait_recv()

    def a_copy(k):
        s, to = ((seq, sh), (seq, sl), (sh, sl))[k]
        v = wg.at[s, wrows(z), tcols]
        return remote(v, v, a_s.at[0], a_r.at[k], (to, batch))

    def b_copy(t, up):
        to = jnp.minimum(z + 1, nz - 1) if up else jnp.maximum(z - 1, 0)
        v = wg.at[:, wrows(zk(t)), tcols]
        return remote(v, v, b_s.at[up], b_r.at[zk(t)], (seq, to * 2 + core))

    def b_each(t, act):
        zz = zk(t)
        for up in (0, 1):
            ok = jnp.logical_and(zz <= z, z < nz - 1) if up else jnp.logical_and(zz >= z, z > 0)

            @pl.when(ok)
            def _():
                act(b_copy(t, up))

    def d_copy(t):
        v = wg.at[:, wrows(zk(t)), tcols]
        return remote(v, v, d_s.at[0], d_r.at[t // (nz - 1)], core_dev)

    def ab(t):
        b_copy(t, 0).wait_recv()
        b_each(t, lambda c: c.start())
        d_copy(t).start()

    def trows(t):
        return pl.ds(pl.multiple_of(t * (ns * r), 16), ns * r)

    def t_copy(j):
        t = zk(nz - 1 - j)
        up = t > z
        to = jnp.where(up, jnp.minimum(z + 1, nz - 1), jnp.maximum(z - 1, 0))
        k = jnp.where(jnp.logical_and(jnp.logical_not(up), t == z - 1), nz, t)
        return remote(g.at[trows(t), tcols], tz.at[k], t_s.at[0], t_r.at[k], (seq, to * 2 + core))

    def tr(j):
        t = zk(nz - 1 - j)
        more = jnp.logical_or(jnp.logical_and(t > z, z > 0), jnp.logical_and(t < z, z < nz - 1))

        @pl.when(more)
        def _():
            all_of(tz.at[t], t_s.at[0], t_r.at[t]).wait_recv()
            g[trows(t), tcols] = (g[trows(t), tcols].astype(F32) + tz[t].astype(F32)).astype(BF16)
        t_copy(j).start()

    def u_copy(k):
        if k == 0:
            v = g.at[pl.ds(pl.multiple_of(z * (ns * r) + (1 - hi) * (2 * r), 16), 2 * r), tcols]
            return remote(v, ty, u_s.at[0], u_r.at[0], (sh, batch))
        return remote(g.at[grows(sl, z), tcols], tl, u_s.at[1], u_r.at[1], (sl, batch))

    def tl1():
        tsum[...] = g[trows(z), tcols].astype(F32)
        for ok, k in ((z > 0, z), (z < nz - 1, nz)):
            @pl.when(ok)
            def _():
                all_of(tz.at[k], t_s.at[0], t_r.at[k]).wait_recv()
                tsum[...] += tz[k].astype(F32)
        away = pl.ds(pl.multiple_of((1 - hi) * (2 * r), 16), 2 * r)
        g[pl.ds(pl.multiple_of(z * (ns * r) + (1 - hi) * (2 * r), 16), 2 * r), tcols] = tsum[away, :].astype(BF16)
        u_copy(0).start()

    def tl2():
        u_copy(0).wait_recv()
        mine = pl.ds(pl.multiple_of((hi * 2 + lo) * r, 16), r)
        his = pl.ds(pl.multiple_of((hi * 2 + 1 - lo) * r, 16), r)
        gw_ref[:, tcols] = tsum[mine, :] + ty[pl.ds(pl.multiple_of(lo * r, 16), r), :].astype(F32)
        v = tsum[his, :] + ty[pl.ds(pl.multiple_of((1 - lo) * r, 16), r), :].astype(F32)
        g[grows(sl, z), tcols] = v.astype(BF16)
        u_copy(1).start()

    def az(t, h, i):
        z_copy(h, i, t, 0).wait_recv()
        z_each(h, i, t, lambda c: c.start())
        if t < nz - 1 or i == 0:
            e_copy(h, i, t).start()
        if i == 1:
            c_copy(1 + h, t).start()
        elif h == 1:
            c_copy(0, t).start()

    def ae(t, h, i):
        e_copy(h, i, t).wait_recv()
        c_copy(3 + 2 * h + i, t).start()

    def rs(j):
        for i in (1, 0):
            for h in (0, 1):
                r_copy(h, i, j).start()

    def rr(j, h, i):
        k = (h * 2 + i) * nz + j
        t = zk(nz - 1 - j)
        rows = grows((seq, first[h])[i], t)
        r_copy(h, i, j).wait_recv()
        more = jnp.logical_or(jnp.logical_and(t > z, z > 0), jnp.logical_and(t < z, z < nz - 1))

        @pl.when(more)
        def _():
            c, buf = y_slot(h, i, t)
            c.wait_recv()
            g[rows, rcols[h]] = (g[rows, rcols[h]].astype(F32) + rx1[k, :, rw[h]].astype(F32)
                                 + buf[...].astype(F32)).astype(BF16)

        @pl.when(jnp.logical_not(more))
        def _():
            g[rows, rcols[h]] = (g[rows, rcols[h]].astype(F32) + rx1[k, :, rw[h]].astype(F32)).astype(BF16)
        y_copy(h, i, j).start()

    def rl(h, i):
        j = nz - 1
        k = (h * 2 + i) * nz + j
        rows = grows((seq, first[h])[i], z)
        dst = gw_ref.at[:, rcols[h]] if i == 0 else fbuf.at[h, :, rw[h]]
        r_copy(h, i, j).wait_recv()
        dst[...] = g[rows, rcols[h]].astype(F32) + rx1[k, :, rw[h]].astype(F32)
        for ok, t in ((z > 0, z), (z < nz - 1, nz)):
            @pl.when(ok)
            def _():
                c, buf = y_slot(h, i, t)
                c.wait_recv()
                dst[...] += buf[...].astype(F32)
        if i == 1:
            g[rows, rcols[h]] = dst[...].astype(BF16)
            f_copy(h).start()

    tile = 256
    far_cols = (nz - 1) * 2 * r // 128 * 128
    near_cols = far_cols // (nz - 1)

    def grad(j):
        rows = pl.ds(pl.multiple_of(zk(nz - 1 - j) * (ns * r), 16), ns * r)

        def body(i, carry):
            c = pl.ds(pl.multiple_of(i * tile, tile), tile)
            acc = jnp.dot(at_own[rows, :], og_ref[:, c], preferred_element_type=F32)
            acc += jnp.dot(at_rx[rows, :], rx_og[:, c], preferred_element_type=F32)
            g[rows, c] = acc.astype(BF16)
            return carry
        lax.fori_loop(0, dout // tile, body, 0)

    def part(s, c, n):
        v = lax.dot_general(og_ref[...], wg[s, pl.ds(pl.multiple_of(c, 128), n), :], (((1,), (1,)), ((), ())),
                            preferred_element_type=F32)
        ig[:, pl.ds(pl.multiple_of(s * block + c, 128), n)] = v.astype(BF16)

    def early(s):
        part(s, jnp.where(zk(nz - 1) == 0, block - far_cols, 0), far_cols)

    def late(s):
        part(s, zk(nz - 1) * near_cols, block - far_cols)

    xo = remote(og_hbm, rx_og, x_s.at[0], x_r.at[0], core_dev)
    xt = remote(tx, at_rx, x_s.at[1], x_r.at[1], core_dev)

    lm.wait()
    wg[seq, wrows(z), :] = mst[...].astype(BF16)
    pl.semaphore_wait(barrier, 5 - edge.astype(jnp.int32))
    for k in (0, 1):
        a_copy(k).start()
    for h in (0, 1):
        p_copy(h).start()
    for h in (0, 1):
        z_each(h, 0, 0, lambda c: c.start())
    xo.start()
    la.wait()
    for s in range(ns):
        tbuf[...] = attn_ref[:, s * block:(s + 1) * block].T
        for zz in range(nz):
            rows = pl.ds((zz * ns + s) * r, r)
            at_own[rows, :] = tbuf[pl.ds(pl.multiple_of((zz * 2 + core) * r, 16), r), :]
            tx[rows, :] = tbuf[pl.ds(pl.multiple_of((zz * 2 + 1 - core) * r, 16), r), :]
    xt.start()
    a_copy(0).wait_recv()
    a_copy(2).start()
    for h in (1, 0):
        e_copy(h, 0, 0).start()
    c_copy(0, 0).start()
    for h in (0, 1):
        p_copy(h).wait_recv()
        z_each(h, 1, 0, lambda c: c.start())
        e_copy(h, 1, 0).start()
        c_copy(1 + h, 0).start()
    for k in (1, 2):
        a_copy(k).wait_recv()
    b_each(0, lambda c: c.start())
    d_copy(0).start()
    lg.wait()
    xo.wait_recv()
    xt.wait_recv()

    def do(on_edge, inside):
        for ok, events in ((edge, on_edge), (jnp.logical_not(edge), inside)):
            if events:
                @pl.when(ok)
                def _():
                    for f, *a in events:
                        f(*a)

    hs = (0, 1)
    ih = [(h, i) for i in (1, 0) for h in hs]
    grad(0)
    rs(0)
    do([(tr, 0)] + [(az, 1, h, 0) for h in hs],
       [(az, t, h, 0) for h in hs for t in (1, 2)])
    grad(1)
    do([(tr, 1), (az, 1, 0, 1)],
       [(az, t, 0, 1) for t in (1, 2)])
    grad(2)
    do([(tr, 2), (az, 1, 1, 1), (rs, 1)],
       [(az, t, 1, 1) for t in (1, 2)] + [(rs, 1), (rs, 2)])
    do([(rr, 0, h, i) for h, i in ih[:2]], [])
    grad(3)
    do([(rr, 0, h, i) for h, i in ih[2:]] + [(ab, 1)]
       + [(az, 2, h, 0) for h in hs] + [(rs, 2)] + [(az, 2, h, 1) for h in hs]
       + [(rr, 1, h, i) for h, i in ih] + [(ab, 2)]
       + [(ae, t, h, i) for t in (0, 1) for i in hs for h in hs]
       + [(az, 3, h, i) for i in hs for h in hs]
       + [(rs, 3)] + [(rr, 2, h, i) for h, i in ih]
       + [(ae, 2, h, i) for i in hs for h in hs],
       [(ab, 1), (ab, 2), (tr, 0)]
       + [e for n, (h, i) in enumerate(ih) for e in ((az, 3, n % 2, n // 2), (rr, 0, h, i))]
       + [(tr, 1), (tr, 2), (rs, 3)]
       + [(ae, t, h, i) for t in (0, 1, 2) for i in hs for h in hs]
       + [(ab, 3)]
       + [(rr, j, h, i) for h, i in ih[:2] for j in (1, 2)])
    do([], [(rr, j, h, i) for h, i in ih[2:] for j in (1, 2)])
    c_wait(0)
    d_wait(0)
    early(seq)
    early(sl)
    early(sh)
    early(sd)
    do([(ab, 3)], [])
    tl1()
    for h in hs:
        ae(3, h, 0)
    c_wait(1)
    d_wait(1)
    late(seq)
    for h in hs:
        rl(h, 1)
    e_copy(0, 1, nz - 1).start()
    tl2()
    e_copy(1, 1, nz - 1).start()
    c_wait(2)
    late(sl)
    late(sh)
    for h in hs:
        rl(h, 0)
    for h in hs:
        f_copy(h).wait_recv()
        gw_ref[:, rcols[h]] += rx3[h, :, rw[h]].astype(F32)
    u_copy(1).wait_recv()
    gw_ref[:, tcols] += tl[...].astype(F32)

    v = gw_ref[...]
    fold = jnp.sum((v * v).reshape(r // 8, 8, dout), axis=0)
    acc = fold[:, :128]
    for i in range(1, dout // 128):
        acc += fold[:, i * 128:(i + 1) * 128]
    sqs[0] = jnp.sum(acc, axis=0, keepdims=True)

    def q_copy(i):
        return remote(sqs.at[0], sqs.at[i], q_s.at[0], q_r.at[0], other(i))

    def q_start(i, carry):
        q_copy(i).start()
        return carry

    lax.fori_loop(1, ns * nb, q_start, 0)
    for h in hs:
        ae(3, h, 1)
    xo.wait_send()
    xt.wait_send()
    c_wait(3)
    late(sd)
    for n, sem in ((1, p_s), (1, f_s), (2 * nz, e_s), (2 * nz, r_s), (2 * (nz - 1), y_s)):
        all_of(wg.at[0, pl.ds(0, n * r), bcols], sem.at[0], q_r.at[0]).wait_send()
    for k in range(nz):
        @pl.when(z == k)
        def _():
            for up, n in ((1, k + 1 if k < nz - 1 else 0), (0, nz - k if k else 0)):
                if n:
                    all_of(wg.at[0, pl.ds(0, 2 * n * r), bcols], z_s.at[up], q_r.at[0]).wait_send()
                    all_of(wg.at[:, pl.ds(0, n * r), tcols], b_s.at[up], q_r.at[0]).wait_send()
    all_of(wg.at[pl.ds(0, 2), :, bcols], c_s.at[0], q_r.at[0]).wait_send()
    all_of(wg.at[:, pl.ds(0, nz * r), tcols], d_s.at[0], q_r.at[0]).wait_send()
    all_of(tz.at[pl.ds(0, nz - 1)], t_s.at[0], q_r.at[0]).wait_send()
    all_of(wg.at[pl.ds(0, 3), pl.ds(0, r), tcols], a_s.at[0], q_r.at[0]).wait_send()
    for k in (0, 1):
        u_copy(k).wait_send()
    l1.wait()
    l2.wait()
    all_of(sqs.at[pl.ds(1, ns * nb - 1)], q_s.at[0], q_r.at[0]).wait()
    total = sqs[0]
    for i in range(1, ns * nb):
        total += sqs[i]
    sq_ref[...] = total


def finish(size, ig, gw, sq, mst, m1, m2, ig_hbm, nm_hbm, n1_hbm, n2_hbm, nm, n1, n2, i_s, o_s):
    ci = pltpu.make_async_copy(ig, ig_hbm, i_s.at[0])
    ci.start()
    steps = gw.shape[0] // 8
    squares = jnp.sum(sq[...], axis=1, keepdims=True)

    def copies(i):
        rows = pl.ds(pl.multiple_of(i * 8, 8), 8)
        return [pltpu.make_async_copy(a.at[rows], b.at[rows], o_s.at[k, i])
                for k, (a, b) in enumerate(((nm, nm_hbm), (n1, n1_hbm), (n2, n2_hbm)))]

    def body(i, carry):
        rows = pl.ds(pl.multiple_of(i * 8, 8), 8)
        nm[rows, :], n1[rows, :], n2[rows, :] = update(
            gw[rows, :], squares, mst[rows, :], m1[rows, :], m2[rows, :], size)
        for c in copies(i):
            c.start()
        return carry

    def drain(i, carry):
        for c in copies(i):
            c.wait()
        return carry

    lax.fori_loop(0, steps, body, 0)
    lax.fori_loop(0, steps, drain, 0)
    ci.wait()


def fused(attn_out, out_grad, master, moment_one, moment_two, ns, nb):
    tok, din = attn_out.shape
    dout = out_grad.shape[1]
    r = master.shape[0]
    wide, _, both = widths(dout)
    rest = dout - both
    nz = nb // 2
    n = ns * nb
    dma = lambda k: pltpu.SemaphoreType.DMA((k,))
    vm = pl.BlockSpec(memory_space=pltpu.VMEM)
    hbm = pl.BlockSpec(memory_space=pl.ANY)
    sems = [5, 2, 2, 1, 2, 2, 4 * nz, 1, 4 * nz, 1, 4, 1, 4 * nz, 1, 4 * (nz + 1), 1, 2, 1, 1,
            1, 3, 2, nz, 1, 2, 1, nz + 1, 2, 2]
    flat = (r, dout), F32
    held = pl.pallas_call(
        functools.partial(kernel, nb),
        out_shape=tuple(pltpu.VMEM(*o) for o in (((tok, din), BF16), flat, ((1, 128), F32), flat, flat, flat)),
        in_specs=[hbm] * 5,
        out_specs=(vm,) * 6,
        scratch_shapes=[
            pltpu.VMEM((tok, din), BF16),
            pltpu.VMEM((tok, dout), BF16),
            pltpu.VMEM((tok, dout), BF16),
            pltpu.VMEM((nb * r, tok), BF16),
            pltpu.VMEM((din // 2, tok), BF16),
            pltpu.VMEM((din // 2, tok), BF16),
            pltpu.VMEM((din // 2, tok), BF16),
            pltpu.VMEM((ns, nb * r, dout), BF16),
            pltpu.VMEM((din // 2, dout), BF16),
            pltpu.VMEM((4 * nz, r, wide), BF16),
            pltpu.VMEM((4 * (nz + 1), r, wide), BF16),
            pltpu.VMEM((2, r, wide), BF16),
            pltpu.VMEM((2, r, wide), F32),
            pltpu.VMEM((n, 1, 128), F32),
            pltpu.VMEM((nz + 1, ns * r, rest), BF16),
            pltpu.VMEM((2 * r, rest), BF16),
            pltpu.VMEM((r, rest), BF16),
            pltpu.VMEM((ns * r, rest), F32),
        ] + [dma(k) for k in sems],
        compiler_params=pltpu.CompilerParams(
            collective_id=0, has_side_effects=True, vmem_limit_bytes=52_000_000),
    )(attn_out, out_grad, master, moment_one, moment_two)
    return pl.pallas_call(
        functools.partial(finish, din * dout),
        out_shape=(jax.ShapeDtypeStruct((tok, din), BF16),) + (jax.ShapeDtypeStruct(*flat),) * 3,
        in_specs=[vm] * 6,
        out_specs=(hbm,) * 4,
        scratch_shapes=[pltpu.VMEM(*flat)] * 3 + [dma(1), pltpu.SemaphoreType.DMA((3, r // 8))],
        compiler_params=pltpu.CompilerParams(vmem_limit_bytes=6_000_000),
    )(*(pltpu.with_memory_space_constraint(v, pltpu.VMEM) for v in held))


def plain(attn_out, out_grad, shard_weight):
    projected = lax.dot_general(
        out_grad,
        lax.all_gather(shard_weight, ("seq", "batch"), axis=0, tiled=True),
        (((1,), (1,)), ((), ())),
        preferred_element_type=F32,
    )
    width = out_grad.shape[1] // GRAD_BLOCKS
    parts = []
    for b in range(GRAD_BLOCKS):
        d = lax.dot_general(
            attn_out, out_grad[:, b * width:(b + 1) * width],
            (((0,), (0,)), ((), ())), preferred_element_type=F32).astype(BF16)
        d = lax.psum_scatter(d, "seq", scatter_dimension=0, tiled=True)
        parts.append(lax.psum_scatter(d, "batch", scatter_dimension=0, tiled=True).astype(F32))
    weight_grad = jnp.concatenate(parts, axis=1)
    squares = lax.psum(jnp.sum(weight_grad * weight_grad), ("seq", "batch"))
    return projected.astype(BF16), weight_grad, squares


def on_device(ns, nb, attn_out, out_grad, master, moment_one, moment_two):
    r, dout = master.shape
    din = attn_out.shape[1]
    if ns == 4 and nb == 8 and r % 16 == 0 and (nb * r) % 128 == 0 and dout % 256 == 0:
        return fused(attn_out, out_grad, master, moment_one, moment_two, ns, nb)
    input_grad, weight_grad, squares = plain(attn_out, out_grad, master.astype(BF16))
    return (input_grad,) + update(weight_grad, squares, master, moment_one, moment_two, din * dout)


def solution(mesh):
    spec = P(("seq", "batch"), None)
    return jax.shard_map(
        functools.partial(on_device, mesh.shape["seq"], mesh.shape["batch"]),
        mesh=mesh,
        in_specs=(spec,) * 5,
        out_specs=(spec,) * 4,
        check_vma=False,
    )
```

```python
import functools
import jax
import jax.numpy as jnp
from jax import lax
from jax.experimental import pallas as pl
from jax.experimental.pallas import tpu as pltpu
from jax.sharding import PartitionSpec as P

GRAD_BLOCKS = 4
STEP = 10
MESH = pl.DeviceIdType.MESH
F32 = jnp.float32
BF16 = jnp.bfloat16


def update(weight_grad, squares, master, moment_one, moment_two, size):
    grad_norm = jnp.sqrt(squares) + 1e-06
    limit = jnp.sqrt(jnp.float32(size))
    clipped = weight_grad * jnp.minimum(jnp.float32(1.0), limit / grad_norm)
    new_one = 0.9 * moment_one + 0.1 * clipped
    new_two = 0.999 * moment_two + 0.001 * clipped * clipped
    first_hat = new_one * (1.0 / (1.0 - 0.9**STEP))
    second_hat = new_two * (1.0 / (1.0 - 0.999**STEP))
    new_master = master - 0.01 * (first_hat / (jnp.sqrt(second_hat) + 1e-08) + 0.1 * master)
    return new_master, new_one, new_two


def widths(dout):
    tiles = dout // 128 - 1
    wide = (tiles + 1) // 2 * 128
    return wide, tiles * 128 - wide, tiles * 128


def kernel(nb, attn_hbm, og_hbm, master_hbm, m1_hbm, m2_hbm, ig, gw_ref, sq_ref, mst, m1, m2,
           attn_ref, og_ref, rx_og, tbuf, tx, at_own, at_rx, wg, g, rx1, rzb, rx3, fbuf, sqs,
           tz, ty, tl, tsum,
           e_s, e_r, c_s, c_r, q_s, q_r):
    l_s = x_s = x_r = p_s = p_r = z_s = z_r = r_s = r_r = y_s = y_r = f_s = f_r = None
    a_s = a_r = b_s = b_r = d_s = d_r = t_s = t_r = u_s = u_r = None
    ns = 4
    nz = nb // 2
    tok, din = attn_ref.shape
    dout = og_ref.shape[1]
    r = gw_ref.shape[0]
    block = nb * r
    seq = lax.axis_index("seq")
    batch = lax.axis_index("batch")
    z = batch // 2
    core = batch % 2
    hi = seq // 2
    lo = seq % 2
    sh = (1 - hi) * 2 + lo
    sl = hi * 2 + (1 - lo)
    sd = (1 - hi) * 2 + (1 - lo)
    first = (sl, sh)
    last = (sh, sl)
    wide, slim, both = widths(dout)
    gcols = (pl.ds(0, wide), pl.ds(wide, slim))
    rcols = (pl.ds(0, slim), pl.ds(slim, wide))
    rw = (pl.ds(0, slim), pl.ds(0, wide))
    bcols = pl.ds(0, both)
    tcols = pl.ds(both, dout - both)
    core_dev = (seq, z * 2 + 1 - core)
    edge = jnp.logical_or(z == 0, z == nz - 1)

    def other(i):
        b = batch
        for k in range((nb - 1).bit_length()):
            if i >> k & 1:
                b += (1 - batch // 2**k % 2 * 2) * 2**k
        return (seq, sl, sh, sd)[i // nb], b

    near = jnp.minimum(z, nz - 1 - z)

    def zk(t):
        if t == 0:
            return z
        both = t <= 2 * near
        dist = jnp.where(both, (t + 1) // 2, t - near)
        above = jnp.where(both, t % 2, jnp.where(z < nz - 1 - z, 1, 0))
        return z + dist * (2 * above - 1)

    def wrows(zz):
        return pl.ds(pl.multiple_of((zz * 2 + core) * r, 16), r)

    def grows(s, zz):
        return pl.ds(pl.multiple_of((zz * ns + s) * r, 16), r)

    def remote(s, d, ssem, rsem, dev):
        return pltpu.make_async_remote_copy(
            src_ref=s, dst_ref=d, send_sem=ssem, recv_sem=rsem,
            device_id=dev, device_id_type=MESH)

    def shard(s, zz, h):
        return wg.at[s, wrows(zz), gcols[h]]

    def p_copy(h):
        v = shard(seq, z, h)
        return remote(v, v, p_s.at[0], p_r.at[h], (first[h], batch))

    def z_copy(h, i, t, up):
        zz = zk(t)
        to = jnp.minimum(z + 1, nz - 1) if up else jnp.maximum(z - 1, 0)
        v = shard((seq, first[h])[i], zz, h)
        k = (h * 2 + i) * nz + zz
        return remote(v, v, z_s.at[up], z_r.at[k], (seq, to * 2 + core))

    def z_each(h, i, t, act):
        zz = zk(t)
        for up in (0, 1):
            ok = jnp.logical_and(zz <= z, z < nz - 1) if up else jnp.logical_and(zz >= z, z > 0)

            @pl.when(ok)
            def _():
                act(z_copy(h, i, t, up))

    def e_copy(h, i, t):
        v = shard((seq, first[h])[i], zk(t), h)
        return remote(v, v, e_s.at[0], e_r.at[e_group(t, i)], (last[h], batch))

    def c_copy(k, t):
        s, h = ((seq, None), (sl, 0), (sh, 1), (sh, 0), (sd, 0), (sl, 1), (sd, 1))[k]
        v = wg.at[s, wrows(zk(t)), bcols] if h is None else shard(s, zk(t), h)
        return remote(v, v, c_s.at[0], c_r.at[c_group(k, t)], core_dev)

    def c_group(k, t):
        if t < nz - 1:
            return 0
        return 3 if k in (4, 6) else 2 if k else 1

    def r_copy(h, i, j):
        k = (h * 2 + i) * nz + j
        v = g.at[grows((last[h], sd)[i], zk(nz - 1 - j)), rcols[h]]
        return remote(v, rx1.at[k, :, rw[h]], r_s.at[0], r_r.at[k], (last[h], batch))

    def y_copy(h, i, j):
        t = zk(nz - 1 - j)
        up = t > z
        to = jnp.where(up, jnp.minimum(z + 1, nz - 1), jnp.maximum(z - 1, 0))
        k = (h * 2 + i) * (nz + 1) + jnp.where(jnp.logical_and(jnp.logical_not(up), t == z - 1), nz, t)
        v = g.at[grows((seq, first[h])[i], t), rcols[h]]
        return remote(v, rzb.at[k, :, rw[h]], y_s.at[0], y_r.at[k], (seq, to * 2 + core))

    def y_slot(h, i, t):
        k = (h * 2 + i) * (nz + 1) + t
        v = rzb.at[k, :, rw[h]]
        return remote(v, v, y_s.at[0], y_r.at[k], core_dev), v

    def f_copy(h):
        v = g.at[grows(first[h], z), rcols[h]]
        return remote(v, rx3.at[h, :, rw[h]], f_s.at[0], f_r.at[h], (first[h], batch))

    def all_of(ref, ssem, rsem):
        return remote(ref, ref, ssem, rsem, core_dev)

    def c_wait(group):
        v = (wg.at[pl.ds(0, nz - 1), pl.ds(0, ns * r), bcols] if group == 0
             else wg.at[0, pl.ds(0, (1, 2, 1)[group - 1] * r), bcols])
        all_of(v, c_s.at[0], c_r.at[group]).wait_recv()

    def d_wait(group):
        v = wg.at[:, pl.ds(0, (nz - 1, 1)[group] * r), tcols]
        all_of(v, d_s.at[0], d_r.at[group]).wait_recv()

    def a_copy(k):
        s, to = ((seq, sh), (seq, sl), (sh, sl))[k]
        v = wg.at[s, wrows(z), tcols]
        return remote(v, v, a_s.at[0], a_r.at[k], (to, batch))

    def b_copy(t, up):
        to = jnp.minimum(z + 1, nz - 1) if up else jnp.maximum(z - 1, 0)
        v = wg.at[:, wrows(zk(t)), tcols]
        return remote(v, v, b_s.at[up], b_r.at[zk(t)], (seq, to * 2 + core))

    def b_each(t, act):
        zz = zk(t)
        for up in (0, 1):
            ok = jnp.logical_and(zz <= z, z < nz - 1) if up else jnp.logical_and(zz >= z, z > 0)

            @pl.when(ok)
            def _():
                act(b_copy(t, up))

    def d_copy(t):
        v = wg.at[:, wrows(zk(t)), tcols]
        return remote(v, v, d_s.at[0], d_r.at[t // (nz - 1)], core_dev)

    def ab(t):
        b_copy(t, 0).wait_recv()
        b_each(t, lambda c: c.start())
        d_copy(t).start()

    def trows(t):
        return pl.ds(pl.multiple_of(t * (ns * r), 16), ns * r)

    def t_copy(j):
        t = zk(nz - 1 - j)
        up = t > z
        to = jnp.where(up, jnp.minimum(z + 1, nz - 1), jnp.maximum(z - 1, 0))
        k = jnp.where(jnp.logical_and(jnp.logical_not(up), t == z - 1), nz, t)
        return remote(g.at[trows(t), tcols], tz.at[k], t_s.at[0], t_r.at[k], (seq, to * 2 + core))

    def tr(j):
        t = zk(nz - 1 - j)
        more = jnp.logical_or(jnp.logical_and(t > z, z > 0), jnp.logical_and(t < z, z < nz - 1))

        @pl.when(more)
        def _():
            all_of(tz.at[t], t_s.at[0], t_r.at[t]).wait_recv()
            g[trows(t), tcols] = (g[trows(t), tcols].astype(F32) + tz[t].astype(F32)).astype(BF16)
        t_copy(j).start()

    def u_copy(k):
        if k == 0:
            v = g.at[pl.ds(pl.multiple_of(z * (ns * r) + (1 - hi) * (2 * r), 16), 2 * r), tcols]
            return remote(v, ty, u_s.at[0], u_r.at[0], (sh, batch))
        return remote(g.at[grows(sl, z), tcols], tl, u_s.at[1], u_r.at[1], (sl, batch))

    def tl1():
        tsum[...] = g[trows(z), tcols].astype(F32)
        for ok, k in ((z > 0, z), (z < nz - 1, nz)):
            @pl.when(ok)
            def _():
                all_of(tz.at[k], t_s.at[0], t_r.at[k]).wait_recv()
                tsum[...] += tz[k].astype(F32)
        away = pl.ds(pl.multiple_of((1 - hi) * (2 * r), 16), 2 * r)
        g[pl.ds(pl.multiple_of(z * (ns * r) + (1 - hi) * (2 * r), 16), 2 * r), tcols] = tsum[away, :].astype(BF16)
        u_copy(0).start()

    def tl2():
        u_copy(0).wait_recv()
        mine = pl.ds(pl.multiple_of((hi * 2 + lo) * r, 16), r)
        his = pl.ds(pl.multiple_of((hi * 2 + 1 - lo) * r, 16), r)
        gw_ref[:, tcols] = tsum[mine, :] + ty[pl.ds(pl.multiple_of(lo * r, 16), r), :].astype(F32)
        v = tsum[his, :] + ty[pl.ds(pl.multiple_of((1 - lo) * r, 16), r), :].astype(F32)
        g[grows(sl, z), tcols] = v.astype(BF16)
        u_copy(1).start()

    def az(t, h, i):
        z_copy(h, i, t, 0).wait_recv()
        z_each(h, i, t, lambda c: c.start())
        if t < nz - 1 or i == 0:
            e_copy(h, i, t).start()
        if i == 1:
            c_copy(1 + h, t).start()
        elif h == 1:
            c_copy(0, t).start()

    def e_group(t, i):
        return (0, 0, 1, 2 + i)[t]

    def ae(group):
        members = [(t, h, i) for t in range(nz) for h in (0, 1) for i in (0, 1) if e_group(t, i) == group]
        v = wg.at[0, pl.ds(0, len(members) // 2 * r), bcols]
        all_of(v, e_s.at[0], e_r.at[group]).wait_recv()
        for t, h, i in members:
            c_copy(3 + 2 * h + i, t).start()

    def rs(j):
        for i in (1, 0):
            for h in (0, 1):
                r_copy(h, i, j).start()

    def rr(j, h, i):
        k = (h * 2 + i) * nz + j
        t = zk(nz - 1 - j)
        rows = grows((seq, first[h])[i], t)
        r_copy(h, i, j).wait_recv()
        more = jnp.logical_or(jnp.logical_and(t > z, z > 0), jnp.logical_and(t < z, z < nz - 1))

        @pl.when(more)
        def _():
            c, buf = y_slot(h, i, t)
            c.wait_recv()
            g[rows, rcols[h]] = (g[rows, rcols[h]].astype(F32) + rx1[k, :, rw[h]].astype(F32)
                                 + buf[...].astype(F32)).astype(BF16)

        @pl.when(jnp.logical_not(more))
        def _():
            g[rows, rcols[h]] = (g[rows, rcols[h]].astype(F32) + rx1[k, :, rw[h]].astype(F32)).astype(BF16)
        y_copy(h, i, j).start()

    def rl(h, i):
        j = nz - 1
        k = (h * 2 + i) * nz + j
        rows = grows((seq, first[h])[i], z)
        dst = gw_ref.at[:, rcols[h]] if i == 0 else fbuf.at[h, :, rw[h]]
        r_copy(h, i, j).wait_recv()
        dst[...] = g[rows, rcols[h]].astype(F32) + rx1[k, :, rw[h]].astype(F32)
        for ok, t in ((z > 0, z), (z < nz - 1, nz)):
            @pl.when(ok)
            def _():
                c, buf = y_slot(h, i, t)
                c.wait_recv()
                dst[...] += buf[...].astype(F32)
        if i == 1:
            g[rows, rcols[h]] = dst[...].astype(BF16)
            f_copy(h).start()

    tile = 256
    far_cols = (nz - 1) * 2 * r // 128 * 128
    near_cols = far_cols // (nz - 1)

    def grad(j):
        rows = pl.ds(pl.multiple_of(zk(nz - 1 - j) * (ns * r), 16), ns * r)

        def body(i, carry):
            c = pl.ds(pl.multiple_of(i * tile, tile), tile)
            acc = jnp.dot(at_own[rows, :], og_ref[:, c], preferred_element_type=F32)
            acc += jnp.dot(at_rx[rows, :], rx_og[:, c], preferred_element_type=F32)
            g[rows, c] = acc.astype(BF16)
            return carry
        lax.fori_loop(0, dout // tile, body, 0)

    def part(s, c, n):
        v = lax.dot_general(og_ref[...], wg[s, pl.ds(pl.multiple_of(c, 128), n), :], (((1,), (1,)), ((), ())),
                            preferred_element_type=F32)
        ig[:, pl.ds(pl.multiple_of(s * block + c, 128), n)] = v.astype(BF16)

    def early(s):
        part(s, jnp.where(zk(nz - 1) == 0, block - far_cols, 0), far_cols)

    def late(s):
        part(s, zk(nz - 1) * near_cols, block - far_cols)

    hs = (0, 1)

    def early_scope(*sems):
        nonlocal l_s, x_s, x_r, p_s, p_r, z_s, z_r, r_s, r_r, y_s, y_r, f_s, f_r
        nonlocal a_s, a_r, b_s, b_r, d_s, d_r, t_s, t_r, u_s, u_r
        (l_s, x_s, x_r, p_s, p_r, z_s, z_r, r_s, r_r, y_s, y_r, f_s, f_r,
         a_s, a_r, b_s, b_r, d_s, d_r, t_s, t_r, u_s, u_r) = sems
        lm = pltpu.make_async_copy(master_hbm, mst, l_s.at[2])
        lm.start()
        la = pltpu.make_async_copy(attn_hbm, attn_ref, l_s.at[0])
        lg = pltpu.make_async_copy(og_hbm, og_ref, l_s.at[1])
        l1 = pltpu.make_async_copy(m1_hbm, m1, l_s.at[3])
        l2 = pltpu.make_async_copy(m2_hbm, m2, l_s.at[4])
        barrier = pltpu.get_barrier_semaphore()

        def greet(s, b):
            pl.semaphore_signal(barrier, inc=1, device_id=(s, b), device_id_type=MESH)

        greet(sl, batch)
        greet(sh, batch)
        greet(*core_dev)
        for step, ok in ((-2, z > 0), (2, z < nz - 1)):
            @pl.when(ok)
            def _():
                greet(seq, batch + step)

        xo = remote(og_hbm, rx_og, x_s.at[0], x_r.at[0], core_dev)
        xt = remote(tx, at_rx, x_s.at[1], x_r.at[1], core_dev)

        lm.wait()
        la.start()
        wg[seq, wrows(z), :] = mst[...].astype(BF16)
        pl.semaphore_wait(barrier, 5 - edge.astype(jnp.int32))
        for k in (0, 1):
            a_copy(k).start()
        for h in (0, 1):
            p_copy(h).start()
        for h in (0, 1):
            z_each(h, 0, 0, lambda c: c.start())
        xo.start()
        lg.start()
        la.wait()
        for s in range(ns):
            tbuf[...] = attn_ref[:, s * block:(s + 1) * block].T
            for zz in range(nz):
                rows = pl.ds((zz * ns + s) * r, r)
                at_own[rows, :] = tbuf[pl.ds(pl.multiple_of((zz * 2 + core) * r, 16), r), :]
                tx[rows, :] = tbuf[pl.ds(pl.multiple_of((zz * 2 + 1 - core) * r, 16), r), :]
        xt.start()
        a_copy(0).wait_recv()
        a_copy(2).start()
        for h in (1, 0):
            e_copy(h, 0, 0).start()
        c_copy(0, 0).start()
        for h in (0, 1):
            p_copy(h).wait_recv()
            z_each(h, 1, 0, lambda c: c.start())
            e_copy(h, 1, 0).start()
            c_copy(1 + h, 0).start()
        for k in (1, 2):
            a_copy(k).wait_recv()
        b_each(0, lambda c: c.start())
        d_copy(0).start()
        lg.wait()
        xo.wait_recv()
        xt.wait_recv()

        def do(on_edge, inside):
            for ok, events in ((edge, on_edge), (jnp.logical_not(edge), inside)):
                if events:
                    @pl.when(ok)
                    def _():
                        for f, *a in events:
                            f(*a)

        ih = [(h, i) for i in (1, 0) for h in hs]
        grad(0)
        rs(0)
        do([(tr, 0)] + [(az, 1, h, 0) for h in hs],
           [(az, t, h, 0) for h in hs for t in (1, 2)])
        grad(1)
        do([(tr, 1), (az, 1, 0, 1)],
           [(az, t, 0, 1) for t in (1, 2)])
        grad(2)
        do([(tr, 2), (az, 1, 1, 1), (rs, 1)],
           [(az, t, 1, 1) for t in (1, 2)] + [(rs, 1), (rs, 2)])
        do([(rr, 0, h, i) for h, i in ih[:2]], [])
        grad(3)
        do([(rr, 0, h, i) for h, i in ih[2:]] + [(ab, 1)]
           + [(az, 2, h, 0) for h in hs] + [(rs, 2)] + [(az, 2, h, 1) for h in hs]
           + [(rr, 1, h, i) for h, i in ih] + [(ab, 2)]
           + [(ae, 0)]
           + [(az, 3, h, i) for i in hs for h in hs]
           + [(rs, 3)] + [(rr, 2, h, i) for h, i in ih]
           + [(ae, 1)],
           [(ab, 1), (ab, 2), (tr, 0)]
           + [e for n, (h, i) in enumerate(ih) for e in ((az, 3, n % 2, n // 2), (rr, 0, h, i))]
           + [(tr, 1), (tr, 2), (rs, 3)]
           + [(ae, 0), (ae, 1)]
           + [(ab, 3)]
           + [(rr, j, h, i) for h, i in ih[:2] for j in (1, 2)])
        do([], [(rr, j, h, i) for h, i in ih[2:] for j in (1, 2)])
        l1.start()
        l2.start()
        c_wait(0)
        d_wait(0)
        early(seq)
        early(sl)
        early(sh)
        early(sd)
        do([(ab, 3)], [])
        tl1()
        ae(2)
        c_wait(1)
        d_wait(1)
        late(seq)
        for h in hs:
            rl(h, 1)
        e_copy(0, 1, nz - 1).start()
        tl2()
        e_copy(1, 1, nz - 1).start()
        for h in hs:
            rl(h, 0)
        for h in hs:
            f_copy(h).wait_recv()
        u_copy(1).wait_recv()

        def close(i, acc):
            rows = pl.ds(pl.multiple_of(i * 16, 16), 16)
            for c, x in ((rcols[0], rx3[0, rows, rw[0]]), (rcols[1], rx3[1, rows, rw[1]]), (tcols, tl[rows, :])):
                v = gw_ref[rows, c] + x.astype(F32)
                gw_ref[rows, c] = v
                v = v * v
                for k in range(0, v.shape[1], 128):
                    acc += v[:8, k:k + 128] + v[8:, k:k + 128]
            return acc

        acc = lax.fori_loop(0, r // 16, close, jnp.zeros((8, 128), F32))
        sqs[0] = jnp.sum(acc, axis=0, keepdims=True)

        def q_copy(i):
            return remote(sqs.at[0], sqs.at[i], q_s.at[0], q_r.at[0], other(i))

        for i in range(ns * nb - 1, 0, -1):
            q_copy(i).start()
        c_wait(2)
        late(sl)
        late(sh)
        xo.wait_send()
        xt.wait_send()
        for n, sem in ((1, p_s), (1, f_s), (2 * nz, r_s), (2 * (nz - 1), y_s)):
            all_of(wg.at[0, pl.ds(0, n * r), bcols], sem.at[0], q_r.at[0]).wait_send()
        for k in range(nz):
            @pl.when(z == k)
            def _():
                for up, n in ((1, k + 1 if k < nz - 1 else 0), (0, nz - k if k else 0)):
                    if n:
                        all_of(wg.at[0, pl.ds(0, 2 * n * r), bcols], z_s.at[up], q_r.at[0]).wait_send()
                        all_of(wg.at[:, pl.ds(0, n * r), tcols], b_s.at[up], q_r.at[0]).wait_send()
        all_of(wg.at[:, pl.ds(0, nz * r), tcols], d_s.at[0], q_r.at[0]).wait_send()
        all_of(tz.at[pl.ds(0, nz - 1)], t_s.at[0], q_r.at[0]).wait_send()
        all_of(wg.at[pl.ds(0, 3), pl.ds(0, r), tcols], a_s.at[0], q_r.at[0]).wait_send()
        for k in (0, 1):
            u_copy(k).wait_send()
        l1.wait()
        l2.wait()

    sizes = [5, 2, 2, 1, 2, 2, 4 * nz, 1, 4 * nz, 1, 4 * (nz + 1), 1, 2,
             1, 3, 2, nz, 1, 2, 1, nz + 1, 2, 2]
    pl.run_scoped(early_scope, *(pltpu.SemaphoreType.DMA((n,)) for n in sizes))
    ae(3)
    c_wait(3)
    late(sd)
    all_of(wg.at[0, pl.ds(0, 2 * nz * r), bcols], e_s.at[0], q_r.at[0]).wait_send()
    all_of(wg.at[pl.ds(0, 2), :, bcols], c_s.at[0], q_r.at[0]).wait_send()
    all_of(sqs.at[pl.ds(1, ns * nb - 1)], q_s.at[0], q_r.at[0]).wait()
    total = sqs[0]
    for i in range(1, ns * nb):
        total += sqs[i]
    sq_ref[...] = total


def finish(size, ig, gw, sq, mst, m1, m2, ig_hbm, nm_hbm, n1_hbm, n2_hbm, nm, n1, n2, i_s, o_s):
    ci = pltpu.make_async_copy(ig, ig_hbm, i_s.at[0])
    ci.start()
    steps = gw.shape[0] // 8
    squares = jnp.sum(sq[...], axis=1, keepdims=True)

    def copies(i):
        rows = pl.ds(pl.multiple_of(i * 8, 8), 8)
        return [pltpu.make_async_copy(a.at[rows], b.at[rows], o_s.at[k, i])
                for k, (a, b) in enumerate(((nm, nm_hbm), (n1, n1_hbm), (n2, n2_hbm)))]

    def body(i, carry):
        rows = pl.ds(pl.multiple_of(i * 8, 8), 8)
        nm[rows, :], n1[rows, :], n2[rows, :] = update(
            gw[rows, :], squares, mst[rows, :], m1[rows, :], m2[rows, :], size)
        for c in copies(i):
            c.start()
        return carry

    def drain(i, carry):
        for c in copies(i):
            c.wait()
        return carry

    lax.fori_loop(0, steps, body, 0)
    lax.fori_loop(0, steps, drain, 0)
    ci.wait()


def fused(attn_out, out_grad, master, moment_one, moment_two, ns, nb):
    tok, din = attn_out.shape
    dout = out_grad.shape[1]
    r = master.shape[0]
    wide, _, both = widths(dout)
    rest = dout - both
    nz = nb // 2
    n = ns * nb
    dma = lambda k: pltpu.SemaphoreType.DMA((k,))
    vm = pl.BlockSpec(memory_space=pltpu.VMEM)
    hbm = pl.BlockSpec(memory_space=pl.ANY)
    sems = [1, 4, 1, 4, 1, 1]
    flat = (r, dout), F32
    held = pl.pallas_call(
        functools.partial(kernel, nb),
        out_shape=tuple(pltpu.VMEM(*o) for o in (((tok, din), BF16), flat, ((1, 128), F32), flat, flat, flat)),
        in_specs=[hbm] * 5,
        out_specs=(vm,) * 6,
        scratch_shapes=[
            pltpu.VMEM((tok, din), BF16),
            pltpu.VMEM((tok, dout), BF16),
            pltpu.VMEM((tok, dout), BF16),
            pltpu.VMEM((nb * r, tok), BF16),
            pltpu.VMEM((din // 2, tok), BF16),
            pltpu.VMEM((din // 2, tok), BF16),
            pltpu.VMEM((din // 2, tok), BF16),
            pltpu.VMEM((ns, nb * r, dout), BF16),
            pltpu.VMEM((din // 2, dout), BF16),
            pltpu.VMEM((4 * nz, r, wide), BF16),
            pltpu.VMEM((4 * (nz + 1), r, wide), BF16),
            pltpu.VMEM((2, r, wide), BF16),
            pltpu.VMEM((2, r, wide), F32),
            pltpu.VMEM((n, 1, 128), F32),
            pltpu.VMEM((nz + 1, ns * r, rest), BF16),
            pltpu.VMEM((2 * r, rest), BF16),
            pltpu.VMEM((r, rest), BF16),
            pltpu.VMEM((ns * r, rest), F32),
        ] + [dma(k) for k in sems],
        compiler_params=pltpu.CompilerParams(
            collective_id=0, has_side_effects=True, vmem_limit_bytes=52_000_000),
    )(attn_out, out_grad, master, moment_one, moment_two)
    return pl.pallas_call(
        functools.partial(finish, din * dout),
        out_shape=(jax.ShapeDtypeStruct((tok, din), BF16),) + (jax.ShapeDtypeStruct(*flat),) * 3,
        in_specs=[vm] * 6,
        out_specs=(hbm,) * 4,
        scratch_shapes=[pltpu.VMEM(*flat)] * 3 + [dma(1), pltpu.SemaphoreType.DMA((3, r // 8))],
        compiler_params=pltpu.CompilerParams(vmem_limit_bytes=6_000_000),
    )(*(pltpu.with_memory_space_constraint(v, pltpu.VMEM) for v in held))


def plain(attn_out, out_grad, shard_weight):
    projected = lax.dot_general(
        out_grad,
        lax.all_gather(shard_weight, ("seq", "batch"), axis=0, tiled=True),
        (((1,), (1,)), ((), ())),
        preferred_element_type=F32,
    )
    width = out_grad.shape[1] // GRAD_BLOCKS
    parts = []
    for b in range(GRAD_BLOCKS):
        d = lax.dot_general(
            attn_out, out_grad[:, b * width:(b + 1) * width],
            (((0,), (0,)), ((), ())), preferred_element_type=F32).astype(BF16)
        d = lax.psum_scatter(d, "seq", scatter_dimension=0, tiled=True)
        parts.append(lax.psum_scatter(d, "batch", scatter_dimension=0, tiled=True).astype(F32))
    weight_grad = jnp.concatenate(parts, axis=1)
    squares = lax.psum(jnp.sum(weight_grad * weight_grad), ("seq", "batch"))
    return projected.astype(BF16), weight_grad, squares


def on_device(ns, nb, attn_out, out_grad, master, moment_one, moment_two):
    r, dout = master.shape
    din = attn_out.shape[1]
    if ns == 4 and nb == 8 and r % 16 == 0 and (nb * r) % 128 == 0 and dout % 256 == 0:
        return fused(attn_out, out_grad, master, moment_one, moment_two, ns, nb)
    input_grad, weight_grad, squares = plain(attn_out, out_grad, master.astype(BF16))
    return (input_grad,) + update(weight_grad, squares, master, moment_one, moment_two, din * dout)


def solution(mesh):
    spec = P(("seq", "batch"), None)
    return jax.shard_map(
        functools.partial(on_device, mesh.shape["seq"], mesh.shape["batch"]),
        mesh=mesh,
        in_specs=(spec,) * 5,
        out_specs=(spec,) * 4,
        check_vma=False,
    )
```

```python
import functools
import jax
import jax.numpy as jnp
from jax import lax
from jax.experimental import pallas as pl
from jax.experimental.pallas import tpu as pltpu
from jax.sharding import PartitionSpec as P

GRAD_BLOCKS = 4
STEP = 10
MESH = pl.DeviceIdType.MESH
F32 = jnp.float32
BF16 = jnp.bfloat16


def update(weight_grad, squares, master, moment_one, moment_two, size):
    grad_norm = jnp.sqrt(squares) + 1e-06
    limit = jnp.sqrt(jnp.float32(size))
    clipped = weight_grad * jnp.minimum(jnp.float32(1.0), limit / grad_norm)
    new_one = 0.9 * moment_one + 0.1 * clipped
    new_two = 0.999 * moment_two + 0.001 * clipped * clipped
    first_hat = new_one * (1.0 / (1.0 - 0.9**STEP))
    second_hat = new_two * (1.0 / (1.0 - 0.999**STEP))
    new_master = master - 0.01 * (first_hat / (jnp.sqrt(second_hat) + 1e-08) + 0.1 * master)
    return new_master, new_one, new_two


def widths(dout):
    tiles = dout // 128 - 1
    wide = (tiles + 1) // 2 * 128
    return wide, tiles * 128 - wide, tiles * 128


def kernel(nb, attn_hbm, og_hbm, master_hbm, m1_hbm, m2_hbm, ig, gw_ref, sq_ref, mst, m1, m2,
           attn_ref, og_ref, rx_og, tbuf, tx, at_own, at_rx, wg, g, rx1, rzb, rx3, fbuf, sqs,
           tz, ty, tl, tsum,
           e_s, e_r, c_s, c_r, q_s, q_r):
    l_s = x_s = x_r = p_s = p_r = z_s = z_r = r_s = r_r = y_s = y_r = f_s = f_r = None
    a_s = a_r = b_s = b_r = d_s = d_r = t_s = t_r = u_s = u_r = None
    ns = 4
    nz = nb // 2
    tok, din = attn_ref.shape
    dout = og_ref.shape[1]
    r = gw_ref.shape[0]
    block = nb * r
    seq = lax.axis_index("seq")
    batch = lax.axis_index("batch")
    z = batch // 2
    core = batch % 2
    hi = seq // 2
    lo = seq % 2
    sh = (1 - hi) * 2 + lo
    sl = hi * 2 + (1 - lo)
    sd = (1 - hi) * 2 + (1 - lo)
    first = (sl, sh)
    last = (sh, sl)
    wide, slim, both = widths(dout)
    gcols = (pl.ds(0, wide), pl.ds(wide, slim))
    rcols = (pl.ds(0, slim), pl.ds(slim, wide))
    rw = (pl.ds(0, slim), pl.ds(0, wide))
    bcols = pl.ds(0, both)
    tcols = pl.ds(both, dout - both)
    core_dev = (seq, z * 2 + 1 - core)
    edge = jnp.logical_or(z == 0, z == nz - 1)

    def other(i):
        b = batch
        for k in range((nb - 1).bit_length()):
            if i >> k & 1:
                b += (1 - batch // 2**k % 2 * 2) * 2**k
        return (seq, sl, sh, sd)[i // nb], b

    near = jnp.minimum(z, nz - 1 - z)

    def zk(t):
        if t == 0:
            return z
        both = t <= 2 * near
        dist = jnp.where(both, (t + 1) // 2, t - near)
        above = jnp.where(both, t % 2, jnp.where(z < nz - 1 - z, 1, 0))
        return z + dist * (2 * above - 1)

    def wrows(zz):
        return pl.ds(pl.multiple_of((zz * 2 + core) * r, 16), r)

    def grows(s, zz):
        return pl.ds(pl.multiple_of((zz * ns + s) * r, 16), r)

    def remote(s, d, ssem, rsem, dev):
        return pltpu.make_async_remote_copy(
            src_ref=s, dst_ref=d, send_sem=ssem, recv_sem=rsem,
            device_id=dev, device_id_type=MESH)

    def shard(s, zz, h):
        return wg.at[s, wrows(zz), gcols[h]]

    def p_copy(h):
        v = shard(seq, z, h)
        return remote(v, v, p_s.at[0], p_r.at[h], (first[h], batch))

    def z_copy(h, i, t, up):
        zz = zk(t)
        to = jnp.minimum(z + 1, nz - 1) if up else jnp.maximum(z - 1, 0)
        v = shard((seq, first[h])[i], zz, h)
        k = (h * 2 + i) * nz + zz
        return remote(v, v, z_s.at[up], z_r.at[k], (seq, to * 2 + core))

    def z_each(h, i, t, act):
        zz = zk(t)
        for up in (0, 1):
            ok = jnp.logical_and(zz <= z, z < nz - 1) if up else jnp.logical_and(zz >= z, z > 0)

            @pl.when(ok)
            def _():
                act(z_copy(h, i, t, up))

    def e_copy(h, i, t):
        v = shard((seq, first[h])[i], zk(t), h)
        return remote(v, v, e_s.at[0], e_r.at[e_group(t, i)], (last[h], batch))

    def c_copy(k, t):
        s, h = ((seq, None), (sl, 0), (sh, 1), (sh, 0), (sd, 0), (sl, 1), (sd, 1))[k]
        v = wg.at[s, wrows(zk(t)), bcols] if h is None else shard(s, zk(t), h)
        return remote(v, v, c_s.at[0], c_r.at[c_group(k, t)], core_dev)

    def c_group(k, t):
        if t < nz - 1:
            return 0
        return 3 if k in (4, 6) else 2 if k else 1

    def r_copy(h, i, j):
        k = (h * 2 + i) * nz + j
        v = g.at[grows((last[h], sd)[i], zk(nz - 1 - j)), rcols[h]]
        return remote(v, rx1.at[k, :, rw[h]], r_s.at[0], r_r.at[k], (last[h], batch))

    def y_copy(h, i, j):
        t = zk(nz - 1 - j)
        up = t > z
        to = jnp.where(up, jnp.minimum(z + 1, nz - 1), jnp.maximum(z - 1, 0))
        k = (h * 2 + i) * (nz + 1) + jnp.where(jnp.logical_and(jnp.logical_not(up), t == z - 1), nz, t)
        v = g.at[grows((seq, first[h])[i], t), rcols[h]]
        return remote(v, rzb.at[k, :, rw[h]], y_s.at[0], y_r.at[k], (seq, to * 2 + core))

    def y_slot(h, i, t):
        k = (h * 2 + i) * (nz + 1) + t
        v = rzb.at[k, :, rw[h]]
        return remote(v, v, y_s.at[0], y_r.at[k], core_dev), v

    def f_copy(h):
        v = g.at[grows(first[h], z), rcols[h]]
        return remote(v, rx3.at[h, :, rw[h]], f_s.at[0], f_r.at[h], (first[h], batch))

    def all_of(ref, ssem, rsem):
        return remote(ref, ref, ssem, rsem, core_dev)

    def c_wait(group):
        v = (wg.at[pl.ds(0, nz - 1), pl.ds(0, ns * r), bcols] if group == 0
             else wg.at[0, pl.ds(0, (1, 2, 1)[group - 1] * r), bcols])
        all_of(v, c_s.at[0], c_r.at[group]).wait_recv()

    def d_wait(group):
        v = wg.at[:, pl.ds(0, (nz - 1, 1)[group] * r), tcols]
        all_of(v, d_s.at[0], d_r.at[group]).wait_recv()

    def a_copy(k):
        s, to = ((seq, sh), (seq, sl), (sh, sl))[k]
        v = wg.at[s, wrows(z), tcols]
        return remote(v, v, a_s.at[0], a_r.at[k], (to, batch))

    def b_copy(t, up):
        to = jnp.minimum(z + 1, nz - 1) if up else jnp.maximum(z - 1, 0)
        v = wg.at[:, wrows(zk(t)), tcols]
        return remote(v, v, b_s.at[up], b_r.at[zk(t)], (seq, to * 2 + core))

    def b_each(t, act):
        zz = zk(t)
        for up in (0, 1):
            ok = jnp.logical_and(zz <= z, z < nz - 1) if up else jnp.logical_and(zz >= z, z > 0)

            @pl.when(ok)
            def _():
                act(b_copy(t, up))

    def d_copy(t):
        v = wg.at[:, wrows(zk(t)), tcols]
        return remote(v, v, d_s.at[0], d_r.at[t // (nz - 1)], core_dev)

    def ab(t):
        b_copy(t, 0).wait_recv()
        b_each(t, lambda c: c.start())
        d_copy(t).start()

    def trows(t):
        return pl.ds(pl.multiple_of(t * (ns * r), 16), ns * r)

    def t_copy(j):
        t = zk(nz - 1 - j)
        up = t > z
        to = jnp.where(up, jnp.minimum(z + 1, nz - 1), jnp.maximum(z - 1, 0))
        k = jnp.where(jnp.logical_and(jnp.logical_not(up), t == z - 1), nz, t)
        return remote(g.at[trows(t), tcols], tz.at[k], t_s.at[0], t_r.at[k], (seq, to * 2 + core))

    def tr(j):
        t = zk(nz - 1 - j)
        more = jnp.logical_or(jnp.logical_and(t > z, z > 0), jnp.logical_and(t < z, z < nz - 1))

        @pl.when(more)
        def _():
            all_of(tz.at[t], t_s.at[0], t_r.at[t]).wait_recv()
            g[trows(t), tcols] = (g[trows(t), tcols].astype(F32) + tz[t].astype(F32)).astype(BF16)
        t_copy(j).start()

    def u_copy(k):
        if k == 0:
            v = g.at[pl.ds(pl.multiple_of(z * (ns * r) + (1 - hi) * (2 * r), 16), 2 * r), tcols]
            return remote(v, ty, u_s.at[0], u_r.at[0], (sh, batch))
        return remote(g.at[grows(sl, z), tcols], tl, u_s.at[1], u_r.at[1], (sl, batch))

    def tl1():
        tsum[...] = g[trows(z), tcols].astype(F32)
        for ok, k in ((z > 0, z), (z < nz - 1, nz)):
            @pl.when(ok)
            def _():
                all_of(tz.at[k], t_s.at[0], t_r.at[k]).wait_recv()
                tsum[...] += tz[k].astype(F32)
        away = pl.ds(pl.multiple_of((1 - hi) * (2 * r), 16), 2 * r)
        g[pl.ds(pl.multiple_of(z * (ns * r) + (1 - hi) * (2 * r), 16), 2 * r), tcols] = tsum[away, :].astype(BF16)
        u_copy(0).start()

    def tl2():
        u_copy(0).wait_recv()
        mine = pl.ds(pl.multiple_of((hi * 2 + lo) * r, 16), r)
        his = pl.ds(pl.multiple_of((hi * 2 + 1 - lo) * r, 16), r)
        gw_ref[:, tcols] = tsum[mine, :] + ty[pl.ds(pl.multiple_of(lo * r, 16), r), :].astype(F32)
        v = tsum[his, :] + ty[pl.ds(pl.multiple_of((1 - lo) * r, 16), r), :].astype(F32)
        g[grows(sl, z), tcols] = v.astype(BF16)
        u_copy(1).start()

    def az(t, h, i):
        z_copy(h, i, t, 0).wait_recv()
        z_each(h, i, t, lambda c: c.start())
        if t < nz - 1 or i == 0:
            e_copy(h, i, t).start()
        if i == 1:
            c_copy(1 + h, t).start()
        elif h == 1:
            c_copy(0, t).start()

    def e_group(t, i):
        return (0, 0, 1, 2 + i)[t]

    def ae(group):
        members = [(t, h, i) for t in range(nz) for h in (0, 1) for i in (0, 1) if e_group(t, i) == group]
        v = wg.at[0, pl.ds(0, len(members) // 2 * r), bcols]
        all_of(v, e_s.at[0], e_r.at[group]).wait_recv()
        for t, h, i in members:
            c_copy(3 + 2 * h + i, t).start()

    def rs(j):
        for i in (1, 0):
            for h in (0, 1):
                r_copy(h, i, j).start()

    def rr(j, h, i):
        k = (h * 2 + i) * nz + j
        t = zk(nz - 1 - j)
        rows = grows((seq, first[h])[i], t)
        r_copy(h, i, j).wait_recv()
        more = jnp.logical_or(jnp.logical_and(t > z, z > 0), jnp.logical_and(t < z, z < nz - 1))

        @pl.when(more)
        def _():
            c, buf = y_slot(h, i, t)
            c.wait_recv()
            g[rows, rcols[h]] = (g[rows, rcols[h]].astype(F32) + rx1[k, :, rw[h]].astype(F32)
                                 + buf[...].astype(F32)).astype(BF16)

        @pl.when(jnp.logical_not(more))
        def _():
            g[rows, rcols[h]] = (g[rows, rcols[h]].astype(F32) + rx1[k, :, rw[h]].astype(F32)).astype(BF16)
        y_copy(h, i, j).start()

    def rl(h, i):
        j = nz - 1
        k = (h * 2 + i) * nz + j
        rows = grows((seq, first[h])[i], z)
        dst = gw_ref.at[:, rcols[h]] if i == 0 else fbuf.at[h, :, rw[h]]
        r_copy(h, i, j).wait_recv()
        dst[...] = g[rows, rcols[h]].astype(F32) + rx1[k, :, rw[h]].astype(F32)
        for ok, t in ((z > 0, z), (z < nz - 1, nz)):
            @pl.when(ok)
            def _():
                c, buf = y_slot(h, i, t)
                c.wait_recv()
                dst[...] += buf[...].astype(F32)
        if i == 1:
            g[rows, rcols[h]] = dst[...].astype(BF16)
            f_copy(h).start()

    tile = 256
    far_cols = (nz - 1) * 2 * r // 128 * 128
    near_cols = far_cols // (nz - 1)

    def grad(j):
        rows = pl.ds(pl.multiple_of(zk(nz - 1 - j) * (ns * r), 16), ns * r)

        def body(i, carry):
            c = pl.ds(pl.multiple_of(i * tile, tile), tile)
            acc = jnp.dot(at_own[rows, :], og_ref[:, c], preferred_element_type=F32)
            acc += jnp.dot(at_rx[rows, :], rx_og[:, c], preferred_element_type=F32)
            g[rows, c] = acc.astype(BF16)
            return carry
        lax.fori_loop(0, dout // tile, body, 0)

    def part(s, c, n):
        v = lax.dot_general(og_ref[...], wg[s, pl.ds(pl.multiple_of(c, 128), n), :], (((1,), (1,)), ((), ())),
                            preferred_element_type=F32)
        ig[:, pl.ds(pl.multiple_of(s * block + c, 128), n)] = v.astype(BF16)

    def early(s):
        part(s, jnp.where(zk(nz - 1) == 0, block - far_cols, 0), far_cols)

    def late(s):
        part(s, zk(nz - 1) * near_cols, block - far_cols)

    hs = (0, 1)

    def early_scope(*sems):
        nonlocal l_s, x_s, x_r, p_s, p_r, z_s, z_r, r_s, r_r, y_s, y_r, f_s, f_r
        nonlocal a_s, a_r, b_s, b_r, d_s, d_r, t_s, t_r, u_s, u_r
        (l_s, x_s, x_r, p_s, p_r, z_s, z_r, r_s, r_r, y_s, y_r, f_s, f_r,
         a_s, a_r, b_s, b_r, d_s, d_r, t_s, t_r, u_s, u_r) = sems
        lm = pltpu.make_async_copy(master_hbm, mst, l_s.at[2])
        lm.start()
        la = pltpu.make_async_copy(attn_hbm, attn_ref, l_s.at[0])
        lg = pltpu.make_async_copy(og_hbm, og_ref, l_s.at[1])
        l1 = pltpu.make_async_copy(m1_hbm, m1, l_s.at[3])
        l2 = pltpu.make_async_copy(m2_hbm, m2, l_s.at[4])
        barrier = pltpu.get_barrier_semaphore()

        def greet(s, b):
            pl.semaphore_signal(barrier, inc=1, device_id=(s, b), device_id_type=MESH)

        greet(sl, batch)
        greet(sh, batch)
        greet(*core_dev)
        for step, ok in ((-2, z > 0), (2, z < nz - 1)):
            @pl.when(ok)
            def _():
                greet(seq, batch + step)

        xo = remote(og_hbm, rx_og, x_s.at[0], x_r.at[0], core_dev)
        xt = remote(tx, at_rx, x_s.at[1], x_r.at[1], core_dev)

        lm.wait()
        la.start()
        wg[seq, wrows(z), :] = mst[...].astype(BF16)
        pl.semaphore_wait(barrier, 5 - edge.astype(jnp.int32))
        for k in (0, 1):
            a_copy(k).start()
        for h in (0, 1):
            p_copy(h).start()
        for h in (0, 1):
            z_each(h, 0, 0, lambda c: c.start())
        xo.start()
        lg.start()
        la.wait()
        for s in range(ns):
            tbuf[...] = attn_ref[:, s * block:(s + 1) * block].T
            for zz in range(nz):
                rows = pl.ds((zz * ns + s) * r, r)
                at_own[rows, :] = tbuf[pl.ds(pl.multiple_of((zz * 2 + core) * r, 16), r), :]
                tx[rows, :] = tbuf[pl.ds(pl.multiple_of((zz * 2 + 1 - core) * r, 16), r), :]
        xt.start()
        a_copy(0).wait_recv()
        a_copy(2).start()
        for h in (1, 0):
            e_copy(h, 0, 0).start()
        c_copy(0, 0).start()
        for h in (0, 1):
            p_copy(h).wait_recv()
            z_each(h, 1, 0, lambda c: c.start())
            e_copy(h, 1, 0).start()
            c_copy(1 + h, 0).start()
        for k in (1, 2):
            a_copy(k).wait_recv()
        b_each(0, lambda c: c.start())
        d_copy(0).start()
        lg.wait()
        xo.wait_recv()
        xt.wait_recv()

        def do(on_edge, inside):
            for ok, events in ((edge, on_edge), (jnp.logical_not(edge), inside)):
                if events:
                    @pl.when(ok)
                    def _():
                        for f, *a in events:
                            f(*a)

        ih = [(h, i) for i in (1, 0) for h in hs]
        grad(0)
        rs(0)
        do([(tr, 0)] + [(az, 1, h, 0) for h in hs],
           [(az, t, h, 0) for h in hs for t in (1, 2)])
        grad(1)
        do([(tr, 1), (az, 1, 0, 1)],
           [(az, t, 0, 1) for t in (1, 2)])
        grad(2)
        do([(tr, 2), (az, 1, 1, 1), (rs, 1)],
           [(az, t, 1, 1) for t in (1, 2)] + [(rs, 1), (rs, 2)])
        do([(rr, 0, h, i) for h, i in ih[:2]], [])
        grad(3)
        do([(rr, 0, h, i) for h, i in ih[2:]] + [(ab, 1)]
           + [(az, 2, h, 0) for h in hs] + [(rs, 2)] + [(az, 2, h, 1) for h in hs]
           + [(rr, 1, h, i) for h, i in ih] + [(ab, 2)]
           + [(ae, 0)]
           + [(az, 3, h, i) for i in hs for h in hs]
           + [(rs, 3)] + [(rr, 2, h, i) for h, i in ih]
           + [(ae, 1)],
           [(ab, 1), (ab, 2), (tr, 0)]
           + [e for n, (h, i) in enumerate(ih) for e in ((az, 3, n % 2, n // 2), (rr, 0, h, i))]
           + [(tr, 1), (tr, 2), (rs, 3)]
           + [(ae, 0), (ae, 1)]
           + [(ab, 3)]
           + [(rr, j, h, i) for h, i in ih[:2] for j in (1, 2)])
        do([], [(rr, j, h, i) for h, i in ih[2:] for j in (1, 2)])
        l1.start()
        l2.start()
        c_wait(0)
        d_wait(0)
        early(seq)
        early(sl)
        early(sh)
        early(sd)
        do([(ab, 3)], [])
        tl1()
        for h in hs:
            rl(h, 1)
        e_copy(0, 1, nz - 1).start()
        ae(2)
        c_wait(1)
        d_wait(1)
        late(seq)
        tl2()
        e_copy(1, 1, nz - 1).start()
        for h in hs:
            rl(h, 0)
        for h in hs:
            f_copy(h).wait_recv()
        u_copy(1).wait_recv()

        def close(i, acc):
            rows = pl.ds(pl.multiple_of(i * 16, 16), 16)
            for c, x in ((rcols[0], rx3[0, rows, rw[0]]), (rcols[1], rx3[1, rows, rw[1]]), (tcols, tl[rows, :])):
                v = gw_ref[rows, c] + x.astype(F32)
                gw_ref[rows, c] = v
                v = v * v
                for k in range(0, v.shape[1], 128):
                    acc += v[:8, k:k + 128] + v[8:, k:k + 128]
            return acc

        acc = lax.fori_loop(0, r // 16, close, jnp.zeros((8, 128), F32))
        sqs[0] = jnp.sum(acc, axis=0, keepdims=True)

        def q_copy(i):
            return remote(sqs.at[0], sqs.at[i], q_s.at[0], q_r.at[0], other(i))

        for i in range(ns * nb - 1, 0, -1):
            q_copy(i).start()
        c_wait(2)
        late(sl)
        late(sh)
        xo.wait_send()
        xt.wait_send()
        for n, sem in ((1, p_s), (1, f_s), (2 * nz, r_s), (2 * (nz - 1), y_s)):
            all_of(wg.at[0, pl.ds(0, n * r), bcols], sem.at[0], q_r.at[0]).wait_send()
        for k in range(nz):
            @pl.when(z == k)
            def _():
                for up, n in ((1, k + 1 if k < nz - 1 else 0), (0, nz - k if k else 0)):
                    if n:
                        all_of(wg.at[0, pl.ds(0, 2 * n * r), bcols], z_s.at[up], q_r.at[0]).wait_send()
                        all_of(wg.at[:, pl.ds(0, n * r), tcols], b_s.at[up], q_r.at[0]).wait_send()
        all_of(wg.at[:, pl.ds(0, nz * r), tcols], d_s.at[0], q_r.at[0]).wait_send()
        all_of(tz.at[pl.ds(0, nz - 1)], t_s.at[0], q_r.at[0]).wait_send()
        all_of(wg.at[pl.ds(0, 3), pl.ds(0, r), tcols], a_s.at[0], q_r.at[0]).wait_send()
        for k in (0, 1):
            u_copy(k).wait_send()
        l1.wait()
        l2.wait()

    sizes = [5, 2, 2, 1, 2, 2, 4 * nz, 1, 4 * nz, 1, 4 * (nz + 1), 1, 2,
             1, 3, 2, nz, 1, 2, 1, nz + 1, 2, 2]
    pl.run_scoped(early_scope, *(pltpu.SemaphoreType.DMA((n,)) for n in sizes))
    ae(3)
    c_wait(3)
    late(sd)
    all_of(wg.at[0, pl.ds(0, 2 * nz * r), bcols], e_s.at[0], q_r.at[0]).wait_send()
    all_of(wg.at[pl.ds(0, 2), :, bcols], c_s.at[0], q_r.at[0]).wait_send()
    all_of(sqs.at[pl.ds(1, ns * nb - 1)], q_s.at[0], q_r.at[0]).wait()
    total = sqs[0]
    for i in range(1, ns * nb):
        total += sqs[i]
    sq_ref[...] = total


def finish(size, ig, gw, sq, mst, m1, m2, ig_hbm, nm_hbm, n1_hbm, n2_hbm, nm, n1, n2, i_s, o_s):
    ci = pltpu.make_async_copy(ig, ig_hbm, i_s.at[0])
    ci.start()
    steps = gw.shape[0] // 8
    squares = jnp.sum(sq[...], axis=1, keepdims=True)

    def copies(i):
        rows = pl.ds(pl.multiple_of(i * 8, 8), 8)
        return [pltpu.make_async_copy(a.at[rows], b.at[rows], o_s.at[k, i])
                for k, (a, b) in enumerate(((nm, nm_hbm), (n1, n1_hbm), (n2, n2_hbm)))]

    def body(i, carry):
        rows = pl.ds(pl.multiple_of(i * 8, 8), 8)
        nm[rows, :], n1[rows, :], n2[rows, :] = update(
            gw[rows, :], squares, mst[rows, :], m1[rows, :], m2[rows, :], size)
        for c in copies(i):
            c.start()
        return carry

    def drain(i, carry):
        for c in copies(i):
            c.wait()
        return carry

    lax.fori_loop(0, steps, body, 0)
    lax.fori_loop(0, steps, drain, 0)
    ci.wait()


def fused(attn_out, out_grad, master, moment_one, moment_two, ns, nb):
    tok, din = attn_out.shape
    dout = out_grad.shape[1]
    r = master.shape[0]
    wide, _, both = widths(dout)
    rest = dout - both
    nz = nb // 2
    n = ns * nb
    dma = lambda k: pltpu.SemaphoreType.DMA((k,))
    vm = pl.BlockSpec(memory_space=pltpu.VMEM)
    hbm = pl.BlockSpec(memory_space=pl.ANY)
    sems = [1, 4, 1, 4, 1, 1]
    flat = (r, dout), F32
    held = pl.pallas_call(
        functools.partial(kernel, nb),
        out_shape=tuple(pltpu.VMEM(*o) for o in (((tok, din), BF16), flat, ((1, 128), F32), flat, flat, flat)),
        in_specs=[hbm] * 5,
        out_specs=(vm,) * 6,
        scratch_shapes=[
            pltpu.VMEM((tok, din), BF16),
            pltpu.VMEM((tok, dout), BF16),
            pltpu.VMEM((tok, dout), BF16),
            pltpu.VMEM((nb * r, tok), BF16),
            pltpu.VMEM((din // 2, tok), BF16),
            pltpu.VMEM((din // 2, tok), BF16),
            pltpu.VMEM((din // 2, tok), BF16),
            pltpu.VMEM((ns, nb * r, dout), BF16),
            pltpu.VMEM((din // 2, dout), BF16),
            pltpu.VMEM((4 * nz, r, wide), BF16),
            pltpu.VMEM((4 * (nz + 1), r, wide), BF16),
            pltpu.VMEM((2, r, wide), BF16),
            pltpu.VMEM((2, r, wide), F32),
            pltpu.VMEM((n, 1, 128), F32),
            pltpu.VMEM((nz + 1, ns * r, rest), BF16),
            pltpu.VMEM((2 * r, rest), BF16),
            pltpu.VMEM((r, rest), BF16),
            pltpu.VMEM((ns * r, rest), F32),
        ] + [dma(k) for k in sems],
        compiler_params=pltpu.CompilerParams(
            collective_id=0, has_side_effects=True, vmem_limit_bytes=52_000_000),
    )(attn_out, out_grad, master, moment_one, moment_two)
    return pl.pallas_call(
        functools.partial(finish, din * dout),
        out_shape=(jax.ShapeDtypeStruct((tok, din), BF16),) + (jax.ShapeDtypeStruct(*flat),) * 3,
        in_specs=[vm] * 6,
        out_specs=(hbm,) * 4,
        scratch_shapes=[pltpu.VMEM(*flat)] * 3 + [dma(1), pltpu.SemaphoreType.DMA((3, r // 8))],
        compiler_params=pltpu.CompilerParams(vmem_limit_bytes=6_000_000),
    )(*(pltpu.with_memory_space_constraint(v, pltpu.VMEM) for v in held))


def plain(attn_out, out_grad, shard_weight):
    projected = lax.dot_general(
        out_grad,
        lax.all_gather(shard_weight, ("seq", "batch"), axis=0, tiled=True),
        (((1,), (1,)), ((), ())),
        preferred_element_type=F32,
    )
    width = out_grad.shape[1] // GRAD_BLOCKS
    parts = []
    for b in range(GRAD_BLOCKS):
        d = lax.dot_general(
            attn_out, out_grad[:, b * width:(b + 1) * width],
            (((0,), (0,)), ((), ())), preferred_element_type=F32).astype(BF16)
        d = lax.psum_scatter(d, "seq", scatter_dimension=0, tiled=True)
        parts.append(lax.psum_scatter(d, "batch", scatter_dimension=0, tiled=True).astype(F32))
    weight_grad = jnp.concatenate(parts, axis=1)
    squares = lax.psum(jnp.sum(weight_grad * weight_grad), ("seq", "batch"))
    return projected.astype(BF16), weight_grad, squares


def on_device(ns, nb, attn_out, out_grad, master, moment_one, moment_two):
    r, dout = master.shape
    din = attn_out.shape[1]
    if ns == 4 and nb == 8 and r % 16 == 0 and (nb * r) % 128 == 0 and dout % 256 == 0:
        return fused(attn_out, out_grad, master, moment_one, moment_two, ns, nb)
    input_grad, weight_grad, squares = plain(attn_out, out_grad, master.astype(BF16))
    return (input_grad,) + update(weight_grad, squares, master, moment_one, moment_two, din * dout)


def solution(mesh):
    spec = P(("seq", "batch"), None)
    return jax.shard_map(
        functools.partial(on_device, mesh.shape["seq"], mesh.shape["batch"]),
        mesh=mesh,
        in_specs=(spec,) * 5,
        out_specs=(spec,) * 4,
        check_vma=False,
    )
```

```python
import functools
import jax
import jax.numpy as jnp
from jax import lax
from jax.experimental import pallas as pl
from jax.experimental.pallas import tpu as pltpu
from jax.sharding import PartitionSpec as P

GRAD_BLOCKS = 4
STEP = 10
MESH = pl.DeviceIdType.MESH
F32 = jnp.float32
BF16 = jnp.bfloat16


def clip_factor(squares, size):
    grad_norm = jnp.sqrt(squares) + 1e-06
    limit = jnp.sqrt(jnp.float32(size))
    return jnp.minimum(jnp.float32(1.0), limit / grad_norm)


def update(weight_grad, clip, master, moment_one, moment_two):
    clipped = weight_grad * clip
    new_one = 0.9 * moment_one + 0.1 * clipped
    new_two = 0.999 * moment_two + 0.001 * clipped * clipped
    first_hat = new_one * (1.0 / (1.0 - 0.9**STEP))
    second_hat = new_two * (1.0 / (1.0 - 0.999**STEP))
    new_master = master - 0.01 * (first_hat / (jnp.sqrt(second_hat) + 1e-08) + 0.1 * master)
    return new_master, new_one, new_two


def widths(dout):
    tiles = dout // 128 - 1
    wide = (tiles + 1) // 2 * 128
    return wide, tiles * 128 - wide, tiles * 128


def kernel(nb, attn_hbm, og_hbm, master_hbm, m1_hbm, m2_hbm, ig, gw_ref, sq_ref, mst, m1, m2,
           attn_ref, og_ref, rx_og, tbuf, tx, at_own, at_rx, wg, g, rx1, rzb, rx3, fbuf, sqs,
           tz, ty, tl, tsum,
           e_s, e_r, c_s, c_r, q_s, q_r):
    l_s = x_s = x_r = p_s = p_r = z_s = z_r = r_s = r_r = y_s = y_r = f_s = f_r = None
    a_s = a_r = b_s = b_r = d_s = d_r = t_s = t_r = u_s = u_r = None
    ns = 4
    nz = nb // 2
    tok, din = attn_ref.shape
    dout = og_ref.shape[1]
    r = gw_ref.shape[0]
    block = nb * r
    seq = lax.axis_index("seq")
    batch = lax.axis_index("batch")
    z = batch // 2
    core = batch % 2
    hi = seq // 2
    lo = seq % 2
    sh = (1 - hi) * 2 + lo
    sl = hi * 2 + (1 - lo)
    sd = (1 - hi) * 2 + (1 - lo)
    first = (sl, sh)
    last = (sh, sl)
    wide, slim, both = widths(dout)
    gcols = (pl.ds(0, wide), pl.ds(wide, slim))
    rcols = (pl.ds(0, slim), pl.ds(slim, wide))
    rw = (pl.ds(0, slim), pl.ds(0, wide))
    bcols = pl.ds(0, both)
    tcols = pl.ds(both, dout - both)
    core_dev = (seq, z * 2 + 1 - core)
    edge = jnp.logical_or(z == 0, z == nz - 1)

    def other(i):
        b = batch
        for k in range((nb - 1).bit_length()):
            if i >> k & 1:
                b += (1 - batch // 2**k % 2 * 2) * 2**k
        return (seq, sl, sh, sd)[i // nb], b

    near = jnp.minimum(z, nz - 1 - z)

    def zk(t):
        if t == 0:
            return z
        both = t <= 2 * near
        dist = jnp.where(both, (t + 1) // 2, t - near)
        above = jnp.where(both, t % 2, jnp.where(z < nz - 1 - z, 1, 0))
        return z + dist * (2 * above - 1)

    def wrows(zz):
        return pl.ds(pl.multiple_of((zz * 2 + core) * r, 16), r)

    def grows(s, zz):
        return pl.ds(pl.multiple_of((zz * ns + s) * r, 16), r)

    def remote(s, d, ssem, rsem, dev):
        return pltpu.make_async_remote_copy(
            src_ref=s, dst_ref=d, send_sem=ssem, recv_sem=rsem,
            device_id=dev, device_id_type=MESH)

    def shard(s, zz, h):
        return wg.at[s, wrows(zz), gcols[h]]

    def p_copy(h):
        v = shard(seq, z, h)
        return remote(v, v, p_s.at[0], p_r.at[h], (first[h], batch))

    def z_copy(h, i, t, up):
        zz = zk(t)
        to = jnp.minimum(z + 1, nz - 1) if up else jnp.maximum(z - 1, 0)
        v = shard((seq, first[h])[i], zz, h)
        k = (h * 2 + i) * nz + zz
        return remote(v, v, z_s.at[up], z_r.at[k], (seq, to * 2 + core))

    def z_each(h, i, t, act):
        zz = zk(t)
        for up in (0, 1):
            ok = jnp.logical_and(zz <= z, z < nz - 1) if up else jnp.logical_and(zz >= z, z > 0)

            @pl.when(ok)
            def _():
                act(z_copy(h, i, t, up))

    def e_copy(h, i, t):
        v = shard((seq, first[h])[i], zk(t), h)
        return remote(v, v, e_s.at[0], e_r.at[e_group(t, i)], (last[h], batch))

    def c_copy(k, t):
        s, h = ((seq, None), (sl, 0), (sh, 1), (sh, 0), (sd, 0), (sl, 1), (sd, 1))[k]
        v = wg.at[s, wrows(zk(t)), bcols] if h is None else shard(s, zk(t), h)
        return remote(v, v, c_s.at[0], c_r.at[c_group(k, t)], core_dev)

    def c_group(k, t):
        if t < nz - 1:
            return 0
        return 3 if k in (4, 6) else 2 if k else 1

    def r_copy(h, i, j):
        k = (h * 2 + i) * nz + j
        v = g.at[grows((last[h], sd)[i], zk(nz - 1 - j)), rcols[h]]
        return remote(v, rx1.at[k, :, rw[h]], r_s.at[0], r_r.at[k], (last[h], batch))

    def y_copy(h, i, j):
        t = zk(nz - 1 - j)
        up = t > z
        to = jnp.where(up, jnp.minimum(z + 1, nz - 1), jnp.maximum(z - 1, 0))
        k = (h * 2 + i) * (nz + 1) + jnp.where(jnp.logical_and(jnp.logical_not(up), t == z - 1), nz, t)
        v = g.at[grows((seq, first[h])[i], t), rcols[h]]
        return remote(v, rzb.at[k, :, rw[h]], y_s.at[0], y_r.at[k], (seq, to * 2 + core))

    def y_slot(h, i, t):
        k = (h * 2 + i) * (nz + 1) + t
        v = rzb.at[k, :, rw[h]]
        return remote(v, v, y_s.at[0], y_r.at[k], core_dev), v

    def f_copy(h):
        v = g.at[grows(first[h], z), rcols[h]]
        return remote(v, rx3.at[h, :, rw[h]], f_s.at[0], f_r.at[h], (first[h], batch))

    def all_of(ref, ssem, rsem):
        return remote(ref, ref, ssem, rsem, core_dev)

    def c_wait(group):
        v = (wg.at[pl.ds(0, nz - 1), pl.ds(0, ns * r), bcols] if group == 0
             else wg.at[0, pl.ds(0, (1, 2, 1)[group - 1] * r), bcols])
        all_of(v, c_s.at[0], c_r.at[group]).wait_recv()

    def d_wait(group):
        v = wg.at[:, pl.ds(0, (nz - 1, 1)[group] * r), tcols]
        all_of(v, d_s.at[0], d_r.at[group]).wait_recv()

    def a_copy(k):
        s, to = ((seq, sh), (seq, sl), (sh, sl))[k]
        v = wg.at[s, wrows(z), tcols]
        return remote(v, v, a_s.at[0], a_r.at[k], (to, batch))

    def b_copy(t, up):
        to = jnp.minimum(z + 1, nz - 1) if up else jnp.maximum(z - 1, 0)
        v = wg.at[:, wrows(zk(t)), tcols]
        return remote(v, v, b_s.at[up], b_r.at[zk(t)], (seq, to * 2 + core))

    def b_each(t, act):
        zz = zk(t)
        for up in (0, 1):
            ok = jnp.logical_and(zz <= z, z < nz - 1) if up else jnp.logical_and(zz >= z, z > 0)

            @pl.when(ok)
            def _():
                act(b_copy(t, up))

    def d_copy(t):
        v = wg.at[:, wrows(zk(t)), tcols]
        return remote(v, v, d_s.at[0], d_r.at[t // (nz - 1)], core_dev)

    def ab(t):
        b_copy(t, 0).wait_recv()
        b_each(t, lambda c: c.start())
        d_copy(t).start()

    def trows(t):
        return pl.ds(pl.multiple_of(t * (ns * r), 16), ns * r)

    def t_copy(j):
        t = zk(nz - 1 - j)
        up = t > z
        to = jnp.where(up, jnp.minimum(z + 1, nz - 1), jnp.maximum(z - 1, 0))
        k = jnp.where(jnp.logical_and(jnp.logical_not(up), t == z - 1), nz, t)
        return remote(g.at[trows(t), tcols], tz.at[k], t_s.at[0], t_r.at[k], (seq, to * 2 + core))

    def tr(j):
        t = zk(nz - 1 - j)
        more = jnp.logical_or(jnp.logical_and(t > z, z > 0), jnp.logical_and(t < z, z < nz - 1))

        @pl.when(more)
        def _():
            all_of(tz.at[t], t_s.at[0], t_r.at[t]).wait_recv()
            g[trows(t), tcols] = (g[trows(t), tcols].astype(F32) + tz[t].astype(F32)).astype(BF16)
        t_copy(j).start()

    def u_copy(k):
        if k == 0:
            v = g.at[pl.ds(pl.multiple_of(z * (ns * r) + (1 - hi) * (2 * r), 16), 2 * r), tcols]
            return remote(v, ty, u_s.at[0], u_r.at[0], (sh, batch))
        return remote(g.at[grows(sl, z), tcols], tl, u_s.at[1], u_r.at[1], (sl, batch))

    def tl1():
        tsum[...] = g[trows(z), tcols].astype(F32)
        for ok, k in ((z > 0, z), (z < nz - 1, nz)):
            @pl.when(ok)
            def _():
                all_of(tz.at[k], t_s.at[0], t_r.at[k]).wait_recv()
                tsum[...] += tz[k].astype(F32)
        away = pl.ds(pl.multiple_of((1 - hi) * (2 * r), 16), 2 * r)
        g[pl.ds(pl.multiple_of(z * (ns * r) + (1 - hi) * (2 * r), 16), 2 * r), tcols] = tsum[away, :].astype(BF16)
        u_copy(0).start()

    def tl2():
        u_copy(0).wait_recv()
        mine = pl.ds(pl.multiple_of((hi * 2 + lo) * r, 16), r)
        his = pl.ds(pl.multiple_of((hi * 2 + 1 - lo) * r, 16), r)
        gw_ref[:, tcols] = tsum[mine, :] + ty[pl.ds(pl.multiple_of(lo * r, 16), r), :].astype(F32)
        v = tsum[his, :] + ty[pl.ds(pl.multiple_of((1 - lo) * r, 16), r), :].astype(F32)
        g[grows(sl, z), tcols] = v.astype(BF16)
        u_copy(1).start()

    def az(t, h, i):
        z_copy(h, i, t, 0).wait_recv()
        z_each(h, i, t, lambda c: c.start())
        if t < nz - 1 or i == 0:
            e_copy(h, i, t).start()
        if i == 1:
            c_copy(1 + h, t).start()
        elif h == 1:
            c_copy(0, t).start()

    def e_group(t, i):
        return (0, 0, 1, 2 + i)[t]

    def ae(group):
        members = [(t, h, i) for t in range(nz) for h in (0, 1) for i in (0, 1) if e_group(t, i) == group]
        v = wg.at[0, pl.ds(0, len(members) // 2 * r), bcols]
        all_of(v, e_s.at[0], e_r.at[group]).wait_recv()
        for t, h, i in members:
            c_copy(3 + 2 * h + i, t).start()

    def rs(j):
        for i in (1, 0):
            for h in (0, 1):
                r_copy(h, i, j).start()

    def rr(j, h, i):
        k = (h * 2 + i) * nz + j
        t = zk(nz - 1 - j)
        rows = grows((seq, first[h])[i], t)
        r_copy(h, i, j).wait_recv()
        more = jnp.logical_or(jnp.logical_and(t > z, z > 0), jnp.logical_and(t < z, z < nz - 1))

        @pl.when(more)
        def _():
            c, buf = y_slot(h, i, t)
            c.wait_recv()
            g[rows, rcols[h]] = (g[rows, rcols[h]].astype(F32) + rx1[k, :, rw[h]].astype(F32)
                                 + buf[...].astype(F32)).astype(BF16)

        @pl.when(jnp.logical_not(more))
        def _():
            g[rows, rcols[h]] = (g[rows, rcols[h]].astype(F32) + rx1[k, :, rw[h]].astype(F32)).astype(BF16)
        y_copy(h, i, j).start()

    def rl(h, i):
        j = nz - 1
        k = (h * 2 + i) * nz + j
        rows = grows((seq, first[h])[i], z)
        dst = gw_ref.at[:, rcols[h]] if i == 0 else fbuf.at[h, :, rw[h]]
        r_copy(h, i, j).wait_recv()
        dst[...] = g[rows, rcols[h]].astype(F32) + rx1[k, :, rw[h]].astype(F32)
        for ok, t in ((z > 0, z), (z < nz - 1, nz)):
            @pl.when(ok)
            def _():
                c, buf = y_slot(h, i, t)
                c.wait_recv()
                dst[...] += buf[...].astype(F32)
        if i == 1:
            g[rows, rcols[h]] = dst[...].astype(BF16)
            f_copy(h).start()

    tile = 256
    far_cols = (nz - 1) * 2 * r // 128 * 128
    near_cols = far_cols // (nz - 1)

    def grad(j):
        rows = pl.ds(pl.multiple_of(zk(nz - 1 - j) * (ns * r), 16), ns * r)

        def body(i, carry):
            c = pl.ds(pl.multiple_of(i * tile, tile), tile)
            acc = jnp.dot(at_own[rows, :], og_ref[:, c], preferred_element_type=F32)
            acc += jnp.dot(at_rx[rows, :], rx_og[:, c], preferred_element_type=F32)
            g[rows, c] = acc.astype(BF16)
            return carry
        lax.fori_loop(0, dout // tile, body, 0)

    def part(s, c, n):
        v = lax.dot_general(og_ref[...], wg[s, pl.ds(pl.multiple_of(c, 128), n), :], (((1,), (1,)), ((), ())),
                            preferred_element_type=F32)
        ig[:, pl.ds(pl.multiple_of(s * block + c, 128), n)] = v.astype(BF16)

    def early(s):
        part(s, jnp.where(zk(nz - 1) == 0, block - far_cols, 0), far_cols)

    def late(s):
        part(s, zk(nz - 1) * near_cols, block - far_cols)

    hs = (0, 1)

    def early_scope(*sems):
        nonlocal l_s, x_s, x_r, p_s, p_r, z_s, z_r, r_s, r_r, y_s, y_r, f_s, f_r
        nonlocal a_s, a_r, b_s, b_r, d_s, d_r, t_s, t_r, u_s, u_r
        (l_s, x_s, x_r, p_s, p_r, z_s, z_r, r_s, r_r, y_s, y_r, f_s, f_r,
         a_s, a_r, b_s, b_r, d_s, d_r, t_s, t_r, u_s, u_r) = sems
        lm = pltpu.make_async_copy(master_hbm, mst, l_s.at[2])
        lm.start()
        la = pltpu.make_async_copy(attn_hbm, attn_ref, l_s.at[0])
        lg = pltpu.make_async_copy(og_hbm, og_ref, l_s.at[1])
        l1 = pltpu.make_async_copy(m1_hbm, m1, l_s.at[3])
        l2 = pltpu.make_async_copy(m2_hbm, m2, l_s.at[4])
        barrier = pltpu.get_barrier_semaphore()

        def greet(s, b):
            pl.semaphore_signal(barrier, inc=1, device_id=(s, b), device_id_type=MESH)

        greet(sl, batch)
        greet(sh, batch)
        greet(*core_dev)
        for step, ok in ((-2, z > 0), (2, z < nz - 1)):
            @pl.when(ok)
            def _():
                greet(seq, batch + step)

        xo = remote(og_hbm, rx_og, x_s.at[0], x_r.at[0], core_dev)
        xt = remote(tx, at_rx, x_s.at[1], x_r.at[1], core_dev)

        lm.wait()
        la.start()
        wg[seq, wrows(z), :] = mst[...].astype(BF16)
        pl.semaphore_wait(barrier, 5 - edge.astype(jnp.int32))
        for k in (0, 1):
            a_copy(k).start()
        for h in (0, 1):
            p_copy(h).start()
        for h in (0, 1):
            z_each(h, 0, 0, lambda c: c.start())
        xo.start()
        lg.start()
        la.wait()
        for s in range(ns):
            tbuf[...] = attn_ref[:, s * block:(s + 1) * block].T
            for zz in range(nz):
                rows = pl.ds((zz * ns + s) * r, r)
                at_own[rows, :] = tbuf[pl.ds(pl.multiple_of((zz * 2 + core) * r, 16), r), :]
                tx[rows, :] = tbuf[pl.ds(pl.multiple_of((zz * 2 + 1 - core) * r, 16), r), :]
        xt.start()
        a_copy(0).wait_recv()
        a_copy(2).start()
        for h in (1, 0):
            e_copy(h, 0, 0).start()
        c_copy(0, 0).start()
        for h in (0, 1):
            p_copy(h).wait_recv()
            z_each(h, 1, 0, lambda c: c.start())
            e_copy(h, 1, 0).start()
            c_copy(1 + h, 0).start()
        for k in (1, 2):
            a_copy(k).wait_recv()
        b_each(0, lambda c: c.start())
        d_copy(0).start()
        lg.wait()
        xo.wait_recv()
        xt.wait_recv()

        def do(on_edge, inside):
            for ok, events in ((edge, on_edge), (jnp.logical_not(edge), inside)):
                if events:
                    @pl.when(ok)
                    def _():
                        for f, *a in events:
                            f(*a)

        ih = [(h, i) for i in (1, 0) for h in hs]
        grad(0)
        rs(0)
        do([(tr, 0)] + [(az, 1, h, 0) for h in hs],
           [(az, t, h, 0) for h in hs for t in (1, 2)])
        grad(1)
        do([(tr, 1), (az, 1, 0, 1)],
           [(az, t, 0, 1) for t in (1, 2)])
        grad(2)
        do([(tr, 2), (az, 1, 1, 1), (rs, 1)],
           [(az, t, 1, 1) for t in (1, 2)] + [(rs, 1), (rs, 2)])
        do([(rr, 0, h, i) for h, i in ih[:2]], [])
        grad(3)
        do([(rr, 0, h, i) for h, i in ih[2:]] + [(ab, 1)]
           + [(az, 2, h, 0) for h in hs] + [(rs, 2)] + [(az, 2, h, 1) for h in hs]
           + [(rr, 1, h, i) for h, i in ih] + [(ab, 2)]
           + [(ae, 0)]
           + [(az, 3, h, i) for i in hs for h in hs]
           + [(rs, 3)] + [(rr, 2, h, i) for h, i in ih]
           + [(ae, 1)],
           [(ab, 1), (ab, 2), (tr, 0)]
           + [e for n, (h, i) in enumerate(ih) for e in ((az, 3, n % 2, n // 2), (rr, 0, h, i))]
           + [(tr, 1), (tr, 2), (rs, 3)]
           + [(ae, 0), (ae, 1)]
           + [(ab, 3)]
           + [(rr, j, h, i) for h, i in ih[:2] for j in (1, 2)])
        do([], [(rr, j, h, i) for h, i in ih[2:] for j in (1, 2)])
        l1.start()
        l2.start()
        c_wait(0)
        d_wait(0)
        early(seq)
        early(sl)
        early(sh)
        early(sd)
        do([(ab, 3)], [])
        tl1()
        for h in hs:
            rl(h, 1)
        e_copy(0, 1, nz - 1).start()
        ae(2)
        c_wait(1)
        d_wait(1)
        late(seq)
        tl2()
        e_copy(1, 1, nz - 1).start()
        for h in hs:
            rl(h, 0)
        for h in hs:
            f_copy(h).wait_recv()
        u_copy(1).wait_recv()

        def close(i, acc):
            rows = pl.ds(pl.multiple_of(i * 16, 16), 16)
            for c, x in ((rcols[0], rx3[0, rows, rw[0]]), (rcols[1], rx3[1, rows, rw[1]]), (tcols, tl[rows, :])):
                v = gw_ref[rows, c] + x.astype(F32)
                gw_ref[rows, c] = v
                v = v * v
                for k in range(0, v.shape[1], 128):
                    acc += v[:8, k:k + 128] + v[8:, k:k + 128]
            return acc

        acc = lax.fori_loop(0, r // 16, close, jnp.zeros((8, 128), F32))
        sqs[0] = jnp.sum(acc, axis=0, keepdims=True)

        def q_copy(i):
            return remote(sqs.at[0], sqs.at[i], q_s.at[0], q_r.at[0], other(i))

        for i in range(ns * nb - 1, 0, -1):
            q_copy(i).start()
        c_wait(2)
        late(sl)
        late(sh)
        xo.wait_send()
        xt.wait_send()
        for n, sem in ((1, p_s), (1, f_s), (2 * nz, r_s), (2 * (nz - 1), y_s)):
            all_of(wg.at[0, pl.ds(0, n * r), bcols], sem.at[0], q_r.at[0]).wait_send()
        for k in range(nz):
            @pl.when(z == k)
            def _():
                for up, n in ((1, k + 1 if k < nz - 1 else 0), (0, nz - k if k else 0)):
                    if n:
                        all_of(wg.at[0, pl.ds(0, 2 * n * r), bcols], z_s.at[up], q_r.at[0]).wait_send()
                        all_of(wg.at[:, pl.ds(0, n * r), tcols], b_s.at[up], q_r.at[0]).wait_send()
        all_of(wg.at[:, pl.ds(0, nz * r), tcols], d_s.at[0], q_r.at[0]).wait_send()
        all_of(tz.at[pl.ds(0, nz - 1)], t_s.at[0], q_r.at[0]).wait_send()
        all_of(wg.at[pl.ds(0, 3), pl.ds(0, r), tcols], a_s.at[0], q_r.at[0]).wait_send()
        for k in (0, 1):
            u_copy(k).wait_send()
        l1.wait()
        l2.wait()

    sizes = [5, 2, 2, 1, 2, 2, 4 * nz, 1, 4 * nz, 1, 4 * (nz + 1), 1, 2,
             1, 3, 2, nz, 1, 2, 1, nz + 1, 2, 2]
    pl.run_scoped(early_scope, *(pltpu.SemaphoreType.DMA((n,)) for n in sizes))
    ae(3)
    c_wait(3)
    late(sd)
    all_of(wg.at[0, pl.ds(0, 2 * nz * r), bcols], e_s.at[0], q_r.at[0]).wait_send()
    all_of(wg.at[pl.ds(0, 2), :, bcols], c_s.at[0], q_r.at[0]).wait_send()
    all_of(sqs.at[pl.ds(1, ns * nb - 1)], q_s.at[0], q_r.at[0]).wait()
    total = sqs[0]
    for i in range(1, ns * nb):
        total += sqs[i]
    sq_ref[...] = total


def finish(size, ig, gw, sq, mst, m1, m2, ig_hbm, nm_hbm, n1_hbm, n2_hbm, nm, n1, n2, i_s, o_s):
    ci = pltpu.make_async_copy(ig, ig_hbm, i_s.at[0])
    ci.start()
    steps = gw.shape[0] // 16
    clip = clip_factor(jnp.sum(sq[...], axis=1, keepdims=True), size)

    def copies(i):
        rows = pl.ds(pl.multiple_of(i * 16, 16), 16)
        return [pltpu.make_async_copy(a.at[rows], b.at[rows], o_s.at[k, i])
                for k, (a, b) in enumerate(((nm, nm_hbm), (n1, n1_hbm), (n2, n2_hbm)))]

    def body(i, carry):
        rows = pl.ds(pl.multiple_of(i * 16, 16), 16)
        nm[rows, :], n1[rows, :], n2[rows, :] = update(
            gw[rows, :], clip, mst[rows, :], m1[rows, :], m2[rows, :])
        for c in copies(i):
            c.start()
        return carry

    def drain(i, carry):
        for c in copies(i):
            c.wait()
        return carry

    lax.fori_loop(0, steps, body, 0)
    lax.fori_loop(0, steps, drain, 0)
    ci.wait()


def fused(attn_out, out_grad, master, moment_one, moment_two, ns, nb):
    tok, din = attn_out.shape
    dout = out_grad.shape[1]
    r = master.shape[0]
    wide, _, both = widths(dout)
    rest = dout - both
    nz = nb // 2
    n = ns * nb
    dma = lambda k: pltpu.SemaphoreType.DMA((k,))
    vm = pl.BlockSpec(memory_space=pltpu.VMEM)
    hbm = pl.BlockSpec(memory_space=pl.ANY)
    sems = [1, 4, 1, 4, 1, 1]
    flat = (r, dout), F32
    held = pl.pallas_call(
        functools.partial(kernel, nb),
        out_shape=tuple(pltpu.VMEM(*o) for o in (((tok, din), BF16), flat, ((1, 128), F32), flat, flat, flat)),
        in_specs=[hbm] * 5,
        out_specs=(vm,) * 6,
        scratch_shapes=[
            pltpu.VMEM((tok, din), BF16),
            pltpu.VMEM((tok, dout), BF16),
            pltpu.VMEM((tok, dout), BF16),
            pltpu.VMEM((nb * r, tok), BF16),
            pltpu.VMEM((din // 2, tok), BF16),
            pltpu.VMEM((din // 2, tok), BF16),
            pltpu.VMEM((din // 2, tok), BF16),
            pltpu.VMEM((ns, nb * r, dout), BF16),
            pltpu.VMEM((din // 2, dout), BF16),
            pltpu.VMEM((4 * nz, r, wide), BF16),
            pltpu.VMEM((4 * (nz + 1), r, wide), BF16),
            pltpu.VMEM((2, r, wide), BF16),
            pltpu.VMEM((2, r, wide), F32),
            pltpu.VMEM((n, 1, 128), F32),
            pltpu.VMEM((nz + 1, ns * r, rest), BF16),
            pltpu.VMEM((2 * r, rest), BF16),
            pltpu.VMEM((r, rest), BF16),
            pltpu.VMEM((ns * r, rest), F32),
        ] + [dma(k) for k in sems],
        compiler_params=pltpu.CompilerParams(
            collective_id=0, has_side_effects=True, vmem_limit_bytes=52_000_000),
    )(attn_out, out_grad, master, moment_one, moment_two)
    return pl.pallas_call(
        functools.partial(finish, din * dout),
        out_shape=(jax.ShapeDtypeStruct((tok, din), BF16),) + (jax.ShapeDtypeStruct(*flat),) * 3,
        in_specs=[vm] * 6,
        out_specs=(hbm,) * 4,
        scratch_shapes=[pltpu.VMEM(*flat)] * 3 + [dma(1), pltpu.SemaphoreType.DMA((3, r // 16))],
        compiler_params=pltpu.CompilerParams(vmem_limit_bytes=6_000_000),
    )(*(pltpu.with_memory_space_constraint(v, pltpu.VMEM) for v in held))


def plain(attn_out, out_grad, shard_weight):
    projected = lax.dot_general(
        out_grad,
        lax.all_gather(shard_weight, ("seq", "batch"), axis=0, tiled=True),
        (((1,), (1,)), ((), ())),
        preferred_element_type=F32,
    )
    width = out_grad.shape[1] // GRAD_BLOCKS
    parts = []
    for b in range(GRAD_BLOCKS):
        d = lax.dot_general(
            attn_out, out_grad[:, b * width:(b + 1) * width],
            (((0,), (0,)), ((), ())), preferred_element_type=F32).astype(BF16)
        d = lax.psum_scatter(d, "seq", scatter_dimension=0, tiled=True)
        parts.append(lax.psum_scatter(d, "batch", scatter_dimension=0, tiled=True).astype(F32))
    weight_grad = jnp.concatenate(parts, axis=1)
    squares = lax.psum(jnp.sum(weight_grad * weight_grad), ("seq", "batch"))
    return projected.astype(BF16), weight_grad, squares


def on_device(ns, nb, attn_out, out_grad, master, moment_one, moment_two):
    r, dout = master.shape
    din = attn_out.shape[1]
    if ns == 4 and nb == 8 and r % 16 == 0 and (nb * r) % 128 == 0 and dout % 256 == 0:
        return fused(attn_out, out_grad, master, moment_one, moment_two, ns, nb)
    input_grad, weight_grad, squares = plain(attn_out, out_grad, master.astype(BF16))
    return (input_grad,) + update(
        weight_grad, clip_factor(squares, din * dout), master, moment_one, moment_two)


def solution(mesh):
    spec = P(("seq", "batch"), None)
    return jax.shard_map(
        functools.partial(on_device, mesh.shape["seq"], mesh.shape["batch"]),
        mesh=mesh,
        in_specs=(spec,) * 5,
        out_specs=(spec,) * 4,
        check_vma=False,
    )
```

```python
import functools
import jax
import jax.numpy as jnp
from jax import lax
from jax.experimental import pallas as pl
from jax.experimental.pallas import tpu as pltpu
from jax.sharding import PartitionSpec as P

GRAD_BLOCKS = 4
STEP = 10
MESH = pl.DeviceIdType.MESH
F32 = jnp.float32
BF16 = jnp.bfloat16


def clip_factor(squares, size):
    grad_norm = jnp.sqrt(squares) + 1e-06
    limit = jnp.sqrt(jnp.float32(size))
    return jnp.minimum(jnp.float32(1.0), limit / grad_norm)


def update(weight_grad, clip, master, moment_one, moment_two):
    clipped = weight_grad * clip
    new_one = 0.9 * moment_one + 0.1 * clipped
    new_two = 0.999 * moment_two + 0.001 * clipped * clipped
    first_hat = new_one * (1.0 / (1.0 - 0.9**STEP))
    second_hat = new_two * (1.0 / (1.0 - 0.999**STEP))
    new_master = master - 0.01 * (first_hat / (jnp.sqrt(second_hat) + 1e-08) + 0.1 * master)
    return new_master, new_one, new_two


def widths(dout):
    tiles = dout // 128 - 1
    wide = (tiles + 1) // 2 * 128
    return wide, tiles * 128 - wide, tiles * 128


def kernel(nb, attn_hbm, og_hbm, master_hbm, m1_hbm, m2_hbm, ig, gw_ref, sq_ref, mst, m1, m2,
           attn_ref, og_ref, rx_og, tbuf, tx, at_own, at_rx, wg, g, rx1, rzb, rx3, fbuf, sqs,
           tz, ty, tl, tsum,
           e_s, e_r, c_s, c_r, q_s, q_r):
    l_s = x_s = x_r = p_s = p_r = z_s = z_r = r_s = r_r = y_s = y_r = f_s = f_r = None
    a_s = a_r = b_s = b_r = d_s = d_r = t_s = t_r = u_s = u_r = None
    ns = 4
    nz = nb // 2
    tok, din = attn_ref.shape
    dout = og_ref.shape[1]
    r = gw_ref.shape[0]
    block = nb * r
    seq = lax.axis_index("seq")
    batch = lax.axis_index("batch")
    z = batch // 2
    core = batch % 2
    hi = seq // 2
    lo = seq % 2
    sh = (1 - hi) * 2 + lo
    sl = hi * 2 + (1 - lo)
    sd = (1 - hi) * 2 + (1 - lo)
    first = (sl, sh)
    last = (sh, sl)
    wide, slim, both = widths(dout)
    gcols = (pl.ds(0, wide), pl.ds(wide, slim))
    rcols = (pl.ds(0, slim), pl.ds(slim, wide))
    rw = (pl.ds(0, slim), pl.ds(0, wide))
    bcols = pl.ds(0, both)
    tcols = pl.ds(both, dout - both)
    core_dev = (seq, z * 2 + 1 - core)
    edge = jnp.logical_or(z == 0, z == nz - 1)

    def other(i):
        b = batch
        for k in range((nb - 1).bit_length()):
            if i >> k & 1:
                b += (1 - batch // 2**k % 2 * 2) * 2**k
        return (seq, sl, sh, sd)[i // nb], b

    near = jnp.minimum(z, nz - 1 - z)

    def zk(t):
        if t == 0:
            return z
        both = t <= 2 * near
        dist = jnp.where(both, (t + 1) // 2, t - near)
        above = jnp.where(both, t % 2, jnp.where(z < nz - 1 - z, 1, 0))
        return z + dist * (2 * above - 1)

    def wrows(zz):
        return pl.ds(pl.multiple_of((zz * 2 + core) * r, 16), r)

    def grows(s, zz):
        return pl.ds(pl.multiple_of((zz * ns + s) * r, 16), r)

    def remote(s, d, ssem, rsem, dev):
        return pltpu.make_async_remote_copy(
            src_ref=s, dst_ref=d, send_sem=ssem, recv_sem=rsem,
            device_id=dev, device_id_type=MESH)

    def shard(s, zz, h):
        return wg.at[s, wrows(zz), gcols[h]]

    def p_copy(h):
        v = shard(seq, z, h)
        return remote(v, v, p_s.at[0], p_r.at[h], (first[h], batch))

    def z_copy(h, i, t, up):
        zz = zk(t)
        to = jnp.minimum(z + 1, nz - 1) if up else jnp.maximum(z - 1, 0)
        v = shard((seq, first[h])[i], zz, h)
        k = (h * 2 + i) * nz + zz
        return remote(v, v, z_s.at[up], z_r.at[k], (seq, to * 2 + core))

    def z_each(h, i, t, act):
        zz = zk(t)
        for up in (0, 1):
            ok = jnp.logical_and(zz <= z, z < nz - 1) if up else jnp.logical_and(zz >= z, z > 0)

            @pl.when(ok)
            def _():
                act(z_copy(h, i, t, up))

    def e_copy(h, i, t):
        v = shard((seq, first[h])[i], zk(t), h)
        return remote(v, v, e_s.at[0], e_r.at[e_group(t, i)], (last[h], batch))

    def c_copy(k, t):
        s, h = ((seq, None), (sl, 0), (sh, 1), (sh, 0), (sd, 0), (sl, 1), (sd, 1))[k]
        v = wg.at[s, wrows(zk(t)), bcols] if h is None else shard(s, zk(t), h)
        return remote(v, v, c_s.at[0], c_r.at[c_group(k, t)], core_dev)

    def c_group(k, t):
        if t < nz - 1:
            return 0
        return 3 if k in (4, 6) else 2 if k else 1

    def r_copy(h, i, j):
        k = (h * 2 + i) * nz + j
        v = g.at[grows((last[h], sd)[i], zk(nz - 1 - j)), rcols[h]]
        return remote(v, rx1.at[k, :, rw[h]], r_s.at[0], r_r.at[k], (last[h], batch))

    def y_copy(h, i, j):
        t = zk(nz - 1 - j)
        up = t > z
        to = jnp.where(up, jnp.minimum(z + 1, nz - 1), jnp.maximum(z - 1, 0))
        k = (h * 2 + i) * (nz + 1) + jnp.where(jnp.logical_and(jnp.logical_not(up), t == z - 1), nz, t)
        v = g.at[grows((seq, first[h])[i], t), rcols[h]]
        return remote(v, rzb.at[k, :, rw[h]], y_s.at[0], y_r.at[k], (seq, to * 2 + core))

    def y_slot(h, i, t):
        k = (h * 2 + i) * (nz + 1) + t
        v = rzb.at[k, :, rw[h]]
        return remote(v, v, y_s.at[0], y_r.at[k], core_dev), v

    def f_copy(h):
        v = g.at[grows(first[h], z), rcols[h]]
        return remote(v, rx3.at[h, :, rw[h]], f_s.at[0], f_r.at[h], (first[h], batch))

    def all_of(ref, ssem, rsem):
        return remote(ref, ref, ssem, rsem, core_dev)

    def c_wait(group):
        v = (wg.at[pl.ds(0, nz - 1), pl.ds(0, ns * r), bcols] if group == 0
             else wg.at[0, pl.ds(0, (1, 2, 1)[group - 1] * r), bcols])
        all_of(v, c_s.at[0], c_r.at[group]).wait_recv()

    def d_wait(group):
        v = wg.at[:, pl.ds(0, (nz - 1, 1)[group] * r), tcols]
        all_of(v, d_s.at[0], d_r.at[group]).wait_recv()

    def a_copy(k):
        s, to = ((seq, sh), (seq, sl), (sh, sl))[k]
        v = wg.at[s, wrows(z), tcols]
        return remote(v, v, a_s.at[0], a_r.at[k], (to, batch))

    def b_copy(t, up):
        to = jnp.minimum(z + 1, nz - 1) if up else jnp.maximum(z - 1, 0)
        v = wg.at[:, wrows(zk(t)), tcols]
        return remote(v, v, b_s.at[up], b_r.at[zk(t)], (seq, to * 2 + core))

    def b_each(t, act):
        zz = zk(t)
        for up in (0, 1):
            ok = jnp.logical_and(zz <= z, z < nz - 1) if up else jnp.logical_and(zz >= z, z > 0)

            @pl.when(ok)
            def _():
                act(b_copy(t, up))

    def d_copy(t):
        v = wg.at[:, wrows(zk(t)), tcols]
        return remote(v, v, d_s.at[0], d_r.at[t // (nz - 1)], core_dev)

    def ab(t):
        b_copy(t, 0).wait_recv()
        b_each(t, lambda c: c.start())
        d_copy(t).start()

    def trows(t):
        return pl.ds(pl.multiple_of(t * (ns * r), 16), ns * r)

    def t_copy(j):
        t = zk(nz - 1 - j)
        up = t > z
        to = jnp.where(up, jnp.minimum(z + 1, nz - 1), jnp.maximum(z - 1, 0))
        k = jnp.where(jnp.logical_and(jnp.logical_not(up), t == z - 1), nz, t)
        return remote(g.at[trows(t), tcols], tz.at[k], t_s.at[0], t_r.at[k], (seq, to * 2 + core))

    def tr(j):
        t = zk(nz - 1 - j)
        more = jnp.logical_or(jnp.logical_and(t > z, z > 0), jnp.logical_and(t < z, z < nz - 1))

        @pl.when(more)
        def _():
            all_of(tz.at[t], t_s.at[0], t_r.at[t]).wait_recv()
            g[trows(t), tcols] = (g[trows(t), tcols].astype(F32) + tz[t].astype(F32)).astype(BF16)
        t_copy(j).start()

    def u_copy(k):
        if k == 0:
            v = g.at[pl.ds(pl.multiple_of(z * (ns * r) + (1 - hi) * (2 * r), 16), 2 * r), tcols]
            return remote(v, ty, u_s.at[0], u_r.at[0], (sh, batch))
        return remote(g.at[grows(sl, z), tcols], tl, u_s.at[1], u_r.at[1], (sl, batch))

    def tl1():
        tsum[...] = g[trows(z), tcols].astype(F32)
        for ok, k in ((z > 0, z), (z < nz - 1, nz)):
            @pl.when(ok)
            def _():
                all_of(tz.at[k], t_s.at[0], t_r.at[k]).wait_recv()
                tsum[...] += tz[k].astype(F32)
        away = pl.ds(pl.multiple_of((1 - hi) * (2 * r), 16), 2 * r)
        g[pl.ds(pl.multiple_of(z * (ns * r) + (1 - hi) * (2 * r), 16), 2 * r), tcols] = tsum[away, :].astype(BF16)
        u_copy(0).start()

    def tl2():
        u_copy(0).wait_recv()
        mine = pl.ds(pl.multiple_of((hi * 2 + lo) * r, 16), r)
        his = pl.ds(pl.multiple_of((hi * 2 + 1 - lo) * r, 16), r)
        gw_ref[:, tcols] = tsum[mine, :] + ty[pl.ds(pl.multiple_of(lo * r, 16), r), :].astype(F32)
        v = tsum[his, :] + ty[pl.ds(pl.multiple_of((1 - lo) * r, 16), r), :].astype(F32)
        g[grows(sl, z), tcols] = v.astype(BF16)
        u_copy(1).start()

    def az(t, h, i):
        z_copy(h, i, t, 0).wait_recv()
        z_each(h, i, t, lambda c: c.start())
        if t < nz - 1 or i == 0:
            e_copy(h, i, t).start()
        if i == 1:
            c_copy(1 + h, t).start()
        elif h == 1:
            c_copy(0, t).start()

    def e_group(t, i):
        return (0, 0, 1, 2 + i)[t]

    def ae(group):
        members = [(t, h, i) for t in range(nz) for h in (0, 1) for i in (0, 1) if e_group(t, i) == group]
        v = wg.at[0, pl.ds(0, len(members) // 2 * r), bcols]
        all_of(v, e_s.at[0], e_r.at[group]).wait_recv()
        for t, h, i in members:
            c_copy(3 + 2 * h + i, t).start()

    def rs(j):
        for i in (1, 0):
            for h in (0, 1):
                r_copy(h, i, j).start()

    def rr(j, h, i):
        k = (h * 2 + i) * nz + j
        t = zk(nz - 1 - j)
        rows = grows((seq, first[h])[i], t)
        r_copy(h, i, j).wait_recv()
        more = jnp.logical_or(jnp.logical_and(t > z, z > 0), jnp.logical_and(t < z, z < nz - 1))

        @pl.when(more)
        def _():
            c, buf = y_slot(h, i, t)
            c.wait_recv()
            g[rows, rcols[h]] = (g[rows, rcols[h]].astype(F32) + rx1[k, :, rw[h]].astype(F32)
                                 + buf[...].astype(F32)).astype(BF16)

        @pl.when(jnp.logical_not(more))
        def _():
            g[rows, rcols[h]] = (g[rows, rcols[h]].astype(F32) + rx1[k, :, rw[h]].astype(F32)).astype(BF16)
        y_copy(h, i, j).start()

    def rl(h, i):
        j = nz - 1
        k = (h * 2 + i) * nz + j
        rows = grows((seq, first[h])[i], z)
        dst = gw_ref.at[:, rcols[h]] if i == 0 else fbuf.at[h, :, rw[h]]
        r_copy(h, i, j).wait_recv()
        dst[...] = g[rows, rcols[h]].astype(F32) + rx1[k, :, rw[h]].astype(F32)
        for ok, t in ((z > 0, z), (z < nz - 1, nz)):
            @pl.when(ok)
            def _():
                c, buf = y_slot(h, i, t)
                c.wait_recv()
                dst[...] += buf[...].astype(F32)
        if i == 1:
            g[rows, rcols[h]] = dst[...].astype(BF16)
            f_copy(h).start()

    tile = 256
    far_cols = (nz - 1) * 2 * r // 128 * 128
    near_cols = far_cols // (nz - 1)

    def grad(j):
        rows = pl.ds(pl.multiple_of(zk(nz - 1 - j) * (ns * r), 16), ns * r)

        def body(i, carry):
            c = pl.ds(pl.multiple_of(i * tile, tile), tile)
            acc = jnp.dot(at_own[rows, :], og_ref[:, c], preferred_element_type=F32)
            acc += jnp.dot(at_rx[rows, :], rx_og[:, c], preferred_element_type=F32)
            g[rows, c] = acc.astype(BF16)
            return carry
        lax.fori_loop(0, dout // tile, body, 0)

    def part(s, c, n):
        v = lax.dot_general(og_ref[...], wg[s, pl.ds(pl.multiple_of(c, 128), n), :], (((1,), (1,)), ((), ())),
                            preferred_element_type=F32)
        ig[:, pl.ds(pl.multiple_of(s * block + c, 128), n)] = v.astype(BF16)

    def early(s):
        part(s, jnp.where(zk(nz - 1) == 0, block - far_cols, 0), far_cols)

    def late(s):
        part(s, zk(nz - 1) * near_cols, block - far_cols)

    hs = (0, 1)

    def early_scope(*sems):
        nonlocal l_s, x_s, x_r, p_s, p_r, z_s, z_r, r_s, r_r, y_s, y_r, f_s, f_r
        nonlocal a_s, a_r, b_s, b_r, d_s, d_r, t_s, t_r, u_s, u_r
        (l_s, x_s, x_r, p_s, p_r, z_s, z_r, r_s, r_r, y_s, y_r, f_s, f_r,
         a_s, a_r, b_s, b_r, d_s, d_r, t_s, t_r, u_s, u_r) = sems
        lm = pltpu.make_async_copy(master_hbm, mst, l_s.at[2])
        lm.start()
        la = pltpu.make_async_copy(attn_hbm, attn_ref, l_s.at[0])
        lg = pltpu.make_async_copy(og_hbm, og_ref, l_s.at[1])
        l1 = pltpu.make_async_copy(m1_hbm, m1, l_s.at[3])
        l2 = pltpu.make_async_copy(m2_hbm, m2, l_s.at[4])
        barrier = pltpu.get_barrier_semaphore()

        def greet(s, b):
            pl.semaphore_signal(barrier, inc=1, device_id=(s, b), device_id_type=MESH)

        greet(sl, batch)
        greet(sh, batch)
        greet(*core_dev)
        for step, ok in ((-2, z > 0), (2, z < nz - 1)):
            @pl.when(ok)
            def _():
                greet(seq, batch + step)

        xo = remote(og_hbm, rx_og, x_s.at[0], x_r.at[0], core_dev)
        xt = remote(tx, at_rx, x_s.at[1], x_r.at[1], core_dev)

        lm.wait()
        la.start()
        wg[seq, wrows(z), :] = mst[...].astype(BF16)
        pl.semaphore_wait(barrier, 5 - edge.astype(jnp.int32))
        for k in (0, 1):
            a_copy(k).start()
        for h in (0, 1):
            p_copy(h).start()
        for h in (0, 1):
            z_each(h, 0, 0, lambda c: c.start())
        xo.start()
        lg.start()
        la.wait()
        for s in range(ns):
            tbuf[...] = attn_ref[:, s * block:(s + 1) * block].T
            for zz in range(nz):
                rows = pl.ds((zz * ns + s) * r, r)
                at_own[rows, :] = tbuf[pl.ds(pl.multiple_of((zz * 2 + core) * r, 16), r), :]
                tx[rows, :] = tbuf[pl.ds(pl.multiple_of((zz * 2 + 1 - core) * r, 16), r), :]
        xt.start()
        a_copy(0).wait_recv()
        a_copy(2).start()
        for h in (1, 0):
            e_copy(h, 0, 0).start()
        c_copy(0, 0).start()
        for h in (0, 1):
            p_copy(h).wait_recv()
            z_each(h, 1, 0, lambda c: c.start())
            e_copy(h, 1, 0).start()
            c_copy(1 + h, 0).start()
        for k in (1, 2):
            a_copy(k).wait_recv()
        b_each(0, lambda c: c.start())
        d_copy(0).start()
        lg.wait()
        xo.wait_recv()
        xt.wait_recv()

        def do(on_edge, inside):
            for ok, events in ((edge, on_edge), (jnp.logical_not(edge), inside)):
                if events:
                    @pl.when(ok)
                    def _():
                        for f, *a in events:
                            f(*a)

        ih = [(h, i) for i in (1, 0) for h in hs]
        grad(0)
        rs(0)
        do([(tr, 0)] + [(az, 1, h, 0) for h in hs],
           [(az, t, h, 0) for h in hs for t in (1, 2)])
        grad(1)
        do([(tr, 1), (az, 1, 0, 1)],
           [(az, t, 0, 1) for t in (1, 2)])
        grad(2)
        do([(tr, 2), (az, 1, 1, 1), (rs, 1)],
           [(az, t, 1, 1) for t in (1, 2)] + [(rs, 1), (rs, 2)])
        do([(rr, 0, h, i) for h, i in ih[:2]], [])
        grad(3)
        do([(rr, 0, h, i) for h, i in ih[2:]] + [(ab, 1)]
           + [(az, 2, h, 0) for h in hs] + [(rs, 2)] + [(az, 2, h, 1) for h in hs]
           + [(rr, 1, h, i) for h, i in ih] + [(ab, 2)]
           + [(ae, 0)]
           + [(az, 3, h, i) for i in hs for h in hs]
           + [(rs, 3)] + [(rr, 2, h, i) for h, i in ih]
           + [(ae, 1)],
           [(ab, 1), (ab, 2), (tr, 0)]
           + [e for n, (h, i) in enumerate(ih) for e in ((az, 3, n % 2, n // 2), (rr, 0, h, i))]
           + [(tr, 1), (tr, 2), (rs, 3)]
           + [(ae, 0), (ae, 1)]
           + [(ab, 3)]
           + [(rr, j, h, i) for h, i in ih[:2] for j in (1, 2)])
        do([], [(rr, j, h, i) for h, i in ih[2:] for j in (1, 2)])
        l1.start()
        l2.start()
        c_wait(0)
        d_wait(0)
        early(seq)
        early(sl)
        early(sh)
        early(sd)
        tl1()
        do([(ab, 3)], [])
        for h in hs:
            rl(h, 1)
        e_copy(0, 1, nz - 1).start()
        ae(2)
        tl2()
        e_copy(1, 1, nz - 1).start()
        c_wait(1)
        d_wait(1)
        late(seq)
        for h in hs:
            rl(h, 0)
        for h in hs:
            f_copy(h).wait_recv()
        u_copy(1).wait_recv()

        def close(i, acc):
            rows = pl.ds(pl.multiple_of(i * 16, 16), 16)
            for c, x in ((rcols[0], rx3[0, rows, rw[0]]), (rcols[1], rx3[1, rows, rw[1]]), (tcols, tl[rows, :])):
                v = gw_ref[rows, c] + x.astype(F32)
                gw_ref[rows, c] = v
                v = v * v
                for k in range(0, v.shape[1], 128):
                    acc += v[:8, k:k + 128] + v[8:, k:k + 128]
            return acc

        acc = lax.fori_loop(0, r // 16, close, jnp.zeros((8, 128), F32))
        sqs[0] = jnp.sum(acc, axis=0, keepdims=True)

        def q_copy(i):
            return remote(sqs.at[0], sqs.at[i], q_s.at[0], q_r.at[0], other(i))

        for i in range(ns * nb - 1, 0, -1):
            q_copy(i).start()
        c_wait(2)
        late(sl)
        late(sh)
        xo.wait_send()
        xt.wait_send()
        for n, sem in ((1, p_s), (1, f_s), (2 * nz, r_s), (2 * (nz - 1), y_s)):
            all_of(wg.at[0, pl.ds(0, n * r), bcols], sem.at[0], q_r.at[0]).wait_send()
        for k in range(nz):
            @pl.when(z == k)
            def _():
                for up, n in ((1, k + 1 if k < nz - 1 else 0), (0, nz - k if k else 0)):
                    if n:
                        all_of(wg.at[0, pl.ds(0, 2 * n * r), bcols], z_s.at[up], q_r.at[0]).wait_send()
                        all_of(wg.at[:, pl.ds(0, n * r), tcols], b_s.at[up], q_r.at[0]).wait_send()
        all_of(wg.at[:, pl.ds(0, nz * r), tcols], d_s.at[0], q_r.at[0]).wait_send()
        all_of(tz.at[pl.ds(0, nz - 1)], t_s.at[0], q_r.at[0]).wait_send()
        all_of(wg.at[pl.ds(0, 3), pl.ds(0, r), tcols], a_s.at[0], q_r.at[0]).wait_send()
        for k in (0, 1):
            u_copy(k).wait_send()
        l1.wait()
        l2.wait()

    sizes = [5, 2, 2, 1, 2, 2, 4 * nz, 1, 4 * nz, 1, 4 * (nz + 1), 1, 2,
             1, 3, 2, nz, 1, 2, 1, nz + 1, 2, 2]
    pl.run_scoped(early_scope, *(pltpu.SemaphoreType.DMA((n,)) for n in sizes))
    ae(3)
    c_wait(3)
    late(sd)
    all_of(wg.at[0, pl.ds(0, 2 * nz * r), bcols], e_s.at[0], q_r.at[0]).wait_send()
    all_of(wg.at[pl.ds(0, 2), :, bcols], c_s.at[0], q_r.at[0]).wait_send()
    all_of(sqs.at[pl.ds(1, ns * nb - 1)], q_s.at[0], q_r.at[0]).wait()
    total = sqs[0]
    for i in range(1, ns * nb):
        total += sqs[i]
    sq_ref[...] = total


def finish(size, ig, gw, sq, mst, m1, m2, ig_hbm, nm_hbm, n1_hbm, n2_hbm, nm, n1, n2, i_s, o_s):
    ci = pltpu.make_async_copy(ig, ig_hbm, i_s.at[0])
    ci.start()
    steps = gw.shape[0] // 16
    clip = clip_factor(jnp.sum(sq[...], axis=1, keepdims=True), size)

    def copies(i):
        rows = pl.ds(pl.multiple_of(i * 16, 16), 16)
        return [pltpu.make_async_copy(a.at[rows], b.at[rows], o_s.at[k, i])
                for k, (a, b) in enumerate(((nm, nm_hbm), (n1, n1_hbm), (n2, n2_hbm)))]

    def body(i, carry):
        rows = pl.ds(pl.multiple_of(i * 16, 16), 16)
        nm[rows, :], n1[rows, :], n2[rows, :] = update(
            gw[rows, :], clip, mst[rows, :], m1[rows, :], m2[rows, :])
        for c in copies(i):
            c.start()
        return carry

    def drain(i, carry):
        for c in copies(i):
            c.wait()
        return carry

    lax.fori_loop(0, steps, body, 0)
    lax.fori_loop(0, steps, drain, 0)
    ci.wait()


def fused(attn_out, out_grad, master, moment_one, moment_two, ns, nb):
    tok, din = attn_out.shape
    dout = out_grad.shape[1]
    r = master.shape[0]
    wide, _, both = widths(dout)
    rest = dout - both
    nz = nb // 2
    n = ns * nb
    dma = lambda k: pltpu.SemaphoreType.DMA((k,))
    vm = pl.BlockSpec(memory_space=pltpu.VMEM)
    hbm = pl.BlockSpec(memory_space=pl.ANY)
    sems = [1, 4, 1, 4, 1, 1]
    flat = (r, dout), F32
    held = pl.pallas_call(
        functools.partial(kernel, nb),
        out_shape=tuple(pltpu.VMEM(*o) for o in (((tok, din), BF16), flat, ((1, 128), F32), flat, flat, flat)),
        in_specs=[hbm] * 5,
        out_specs=(vm,) * 6,
        scratch_shapes=[
            pltpu.VMEM((tok, din), BF16),
            pltpu.VMEM((tok, dout), BF16),
            pltpu.VMEM((tok, dout), BF16),
            pltpu.VMEM((nb * r, tok), BF16),
            pltpu.VMEM((din // 2, tok), BF16),
            pltpu.VMEM((din // 2, tok), BF16),
            pltpu.VMEM((din // 2, tok), BF16),
            pltpu.VMEM((ns, nb * r, dout), BF16),
            pltpu.VMEM((din // 2, dout), BF16),
            pltpu.VMEM((4 * nz, r, wide), BF16),
            pltpu.VMEM((4 * (nz + 1), r, wide), BF16),
            pltpu.VMEM((2, r, wide), BF16),
            pltpu.VMEM((2, r, wide), F32),
            pltpu.VMEM((n, 1, 128), F32),
            pltpu.VMEM((nz + 1, ns * r, rest), BF16),
            pltpu.VMEM((2 * r, rest), BF16),
            pltpu.VMEM((r, rest), BF16),
            pltpu.VMEM((ns * r, rest), F32),
        ] + [dma(k) for k in sems],
        compiler_params=pltpu.CompilerParams(
            collective_id=0, has_side_effects=True, vmem_limit_bytes=52_000_000),
    )(attn_out, out_grad, master, moment_one, moment_two)
    return pl.pallas_call(
        functools.partial(finish, din * dout),
        out_shape=(jax.ShapeDtypeStruct((tok, din), BF16),) + (jax.ShapeDtypeStruct(*flat),) * 3,
        in_specs=[vm] * 6,
        out_specs=(hbm,) * 4,
        scratch_shapes=[pltpu.VMEM(*flat)] * 3 + [dma(1), pltpu.SemaphoreType.DMA((3, r // 16))],
        compiler_params=pltpu.CompilerParams(vmem_limit_bytes=6_000_000),
    )(*(pltpu.with_memory_space_constraint(v, pltpu.VMEM) for v in held))


def plain(attn_out, out_grad, shard_weight):
    projected = lax.dot_general(
        out_grad,
        lax.all_gather(shard_weight, ("seq", "batch"), axis=0, tiled=True),
        (((1,), (1,)), ((), ())),
        preferred_element_type=F32,
    )
    width = out_grad.shape[1] // GRAD_BLOCKS
    parts = []
    for b in range(GRAD_BLOCKS):
        d = lax.dot_general(
            attn_out, out_grad[:, b * width:(b + 1) * width],
            (((0,), (0,)), ((), ())), preferred_element_type=F32).astype(BF16)
        d = lax.psum_scatter(d, "seq", scatter_dimension=0, tiled=True)
        parts.append(lax.psum_scatter(d, "batch", scatter_dimension=0, tiled=True).astype(F32))
    weight_grad = jnp.concatenate(parts, axis=1)
    squares = lax.psum(jnp.sum(weight_grad * weight_grad), ("seq", "batch"))
    return projected.astype(BF16), weight_grad, squares


def on_device(ns, nb, attn_out, out_grad, master, moment_one, moment_two):
    r, dout = master.shape
    din = attn_out.shape[1]
    if ns == 4 and nb == 8 and r % 16 == 0 and (nb * r) % 128 == 0 and dout % 256 == 0:
        return fused(attn_out, out_grad, master, moment_one, moment_two, ns, nb)
    input_grad, weight_grad, squares = plain(attn_out, out_grad, master.astype(BF16))
    return (input_grad,) + update(
        weight_grad, clip_factor(squares, din * dout), master, moment_one, moment_two)


def solution(mesh):
    spec = P(("seq", "batch"), None)
    return jax.shard_map(
        functools.partial(on_device, mesh.shape["seq"], mesh.shape["batch"]),
        mesh=mesh,
        in_specs=(spec,) * 5,
        out_specs=(spec,) * 4,
        check_vma=False,
    )
```
